16 devices in a mesh: dp: 2 (over z), tp: 8 (over y, x, core).
Axes of the slice: x: 2, y: 2, z: 2, core: 2. Of those that a mesh axis runs over, the one named last changes fastest.
Arguments:
- x: bfloat16 [8192, 3072], P('dp'), parts along dimension 0
- pos: int32 [8192], P('dp'), parts along dimension 0
- g1: bfloat16 [3072], replicated
- g2: bfloat16 [3072], replicated
- wq: bfloat16 [3072, 3072], P(None, 'tp')
- wk: bfloat16 [3072, 1024], replicated
- wv: bfloat16 [3072, 1024], replicated
- wo: bfloat16 [3072, 3072], P('tp')
- wg: bfloat16 [3072, 8192], P(None, 'tp')
- wu: bfloat16 [3072, 8192], P(None, 'tp')
- wd: bfloat16 [8192, 3072], P('tp')
Outputs:
- output 1: bfloat16 [8192, 3072], P('dp'), parts along dimension 0
- output 2: bfloat16 [8192, 8, 128], P('dp', 'tp'), parts along dimension 0
- output 3: bfloat16 [8192, 8, 128], P('dp', 'tp'), parts along dimension 0
There are 2 independent parts. The reference program is written for one: setup_inputs(seed, part) draws one part's arguments, and reference() takes and returns one part's arrays. A program takes and returns all parts, laid end to end along the dimension named above; an argument that names none is the same for every part.
All inputs are finite; a program needn't handle non-finite values.
Results may differ from the reference program's by a relative error of at most 0.0160802.
Values are sent between devices in bfloat16 or wider.
A program may use at most 1 GiB of HBM per device.

```python
import jax
import jax.numpy as jnp
from jax import lax
import numpy as np

D = 3072
HEADS = 24
KV_HEADS = 8
HEAD = 128
FF = 8192
T = 4096
SLOTS = 8

EPS = 1e-5
ROPE_BASE = 500000.0
R = HEADS // KV_HEADS
QB = min(T, 256)


def setup_inputs(seed: int = 0, part: int = 0) -> dict:
    base = jax.random.PRNGKey(seed)
    kw = jax.random.split(jax.random.fold_in(base, 0), 9)
    kx, kp = jax.random.split(jax.random.fold_in(jax.random.fold_in(base, 1), part))

    def w(k, shape, scale):
        return (jax.random.normal(k, shape, jnp.float32) * scale).astype(jnp.bfloat16)

    def gain(k):
        return (1.0 + 0.2 * jax.random.normal(k, (D,), jnp.float32)).astype(jnp.bfloat16)

    x = jax.random.normal(kx, (T, D), jnp.float32).astype(jnp.bfloat16)
    pos = jax.random.randint(kp, (), 0, 4096, dtype=jnp.int32) + jnp.arange(T, dtype=jnp.int32)
    return {
        "x": x,
        "pos": pos,
        "g1": gain(kw[0]),
        "g2": gain(kw[1]),
        "wq": w(kw[2], (D, HEADS * HEAD), 1.5 * D ** -0.5),
        "wk": w(kw[3], (D, KV_HEADS * HEAD), 1.5 * D ** -0.5),
        "wv": w(kw[4], (D, KV_HEADS * HEAD), D ** -0.5),
        "wo": w(kw[5], (HEADS * HEAD, D), 2.0 * (HEADS * HEAD) ** -0.5),
        "wg": w(kw[6], (D, FF), D ** -0.5),
        "wu": w(kw[7], (D, FF), D ** -0.5),
        "wd": w(kw[8], (FF, D), 2.0 * FF ** -0.5),
    }


def _rms(x, g):
    x32 = x.astype(jnp.float32)
    inv = lax.rsqrt(jnp.mean(x32 * x32, axis=-1, keepdims=True) + EPS)
    return (x32 * inv * g.astype(jnp.float32)).astype(jnp.bfloat16)


def _rope(t, pos):
    half = HEAD // 2
    inv = ROPE_BASE ** (-2.0 * jnp.arange(half, dtype=jnp.float32) / HEAD)
    ang = pos.astype(jnp.float32)[:, None] * inv[None, :]
    c = jnp.cos(ang)[:, None, :]
    s = jnp.sin(ang)[:, None, :]
    t1, t2 = t[..., :half], t[..., half:]
    return jnp.concatenate([t1 * c - t2 * s, t2 * c + t1 * s], axis=-1)


def reference(x, pos, g1, g2, wq, wk, wv, wo, wg, wu, wd):
    a = _rms(x, g1)
    q = _rope(jnp.dot(a, wq, preferred_element_type=jnp.float32).reshape(T, HEADS, HEAD), pos).astype(jnp.bfloat16)
    k = _rope(jnp.dot(a, wk, preferred_element_type=jnp.float32).reshape(T, KV_HEADS, HEAD), pos).astype(jnp.bfloat16)
    v = jnp.dot(a, wv, preferred_element_type=jnp.float32).astype(jnp.bfloat16).reshape(T, KV_HEADS, HEAD)
    qg = q.reshape(T // QB, QB, KV_HEADS, R, HEAD)
    pq = pos.reshape(T // QB, QB)
    scale = HEAD ** -0.5

    def one_head(g):
        kg = k[:, g].astype(jnp.float32)
        vg = v[:, g].astype(jnp.float32)

        def one_block(blk):
            qq, pb = blk
            sc = jnp.einsum("qrd,kd->rqk", qq.astype(jnp.float32), kg) * scale
            sc = jnp.where((pos[None, :] <= pb[:, None])[None], sc, -jnp.inf)
            e = jnp.exp(sc - jnp.max(sc, axis=-1, keepdims=True))
            pr = (e / jnp.sum(e, axis=-1, keepdims=True)).astype(jnp.bfloat16)
            return jnp.einsum("rqk,kd->qrd", pr.astype(jnp.float32), vg).astype(jnp.bfloat16)

        return lax.map(one_block, (qg[:, :, g], pq))

    o = lax.map(one_head, jnp.arange(KV_HEADS))
    o = o.transpose(1, 2, 0, 3, 4).reshape(T, HEADS * HEAD)
    h = (x.astype(jnp.float32) + jnp.dot(o, wo, preferred_element_type=jnp.float32)).astype(jnp.bfloat16)
    b = _rms(h, g2)
    gt = jnp.dot(b, wg, preferred_element_type=jnp.float32)
    up = jnp.dot(b, wu, preferred_element_type=jnp.float32)
    u = (jax.nn.silu(gt) * up).astype(jnp.bfloat16)
    y = (h.astype(jnp.float32) + jnp.dot(u, wd, preferred_element_type=jnp.float32)).astype(jnp.bfloat16)
    sl = np.arange(SLOTS) * KV_HEADS // SLOTS
    return (y, k[:, sl], v[:, sl])
```

```python
import functools

import jax
import jax.numpy as jnp
from jax import lax
from jax.experimental import pallas as pl
from jax.experimental.pallas import tpu as pltpu
from jax.sharding import PartitionSpec as P

HEAD = 128
EPS = 1e-5
ROPE_BASE = 500000.0
LOG2E = 1.4426950408889634
NCHUNK = 4
MESH = pl.DeviceIdType.MESH
F32, BF = jnp.float32, jnp.bfloat16
ANY = pl.BlockSpec(memory_space=pl.ANY)


def _pos_of(r):
    return (r % 2) * 4 + r // 2


def _qkv_kernel(nb, x_ref, g_ref, c_ref, s_ref, wq_ref, wk_ref, wv_ref, q_ref, k_ref, v_ref, w, a, sems):
    i = pl.program_id(0)
    r = lax.axis_index("tp")
    tm = x_ref.shape[0]
    nq = wq_ref.shape[1]

    @pl.when(i == 0)
    def _():
        col = pl.ds(pl.multiple_of(r * HEAD, HEAD), HEAD)
        cps = [
            pltpu.make_async_copy(wq_ref, w.at[:, pl.ds(0, nq)], sems.at[0]),
            pltpu.make_async_copy(wk_ref.at[:, col], w.at[:, pl.ds(nq, HEAD)], sems.at[1]),
            pltpu.make_async_copy(wv_ref.at[:, col], w.at[:, pl.ds(nq + HEAD, HEAD)], sems.at[2]),
        ]
        for cp in cps:
            cp.start()
        for cp in cps:
            cp.wait()

    _norm_rows(x_ref, g_ref, a, tm)
    first = i < nb // 2
    lane = lax.broadcasted_iota(jnp.int32, (tm, HEAD), 1)
    low = lane < HEAD // 2
    keep = jnp.logical_xor(low, jnp.logical_not(first))
    cb, sb = c_ref[...], s_ref[...]
    c = jnp.where(keep, cb, pltpu.roll(cb, HEAD // 2, 1))
    s = jnp.where(keep, sb, pltpu.roll(sb, HEAD // 2, 1))
    s = jnp.where(low, -s, s)
    z = jnp.dot(a[...], w[...], preferred_element_type=F32)
    for h in range(nq // HEAD + 1):
        t = z[:, h * HEAD:(h + 1) * HEAD]
        t = (t * c + pltpu.roll(t, HEAD // 2, 1) * s).astype(BF)
        if h < nq // HEAD:
            q_ref[:, h * HEAD:(h + 1) * HEAD] = t
        else:
            k_ref[...] = t
    v_ref[...] = z[:, nq + HEAD:].astype(BF)


def _norm_rows(src, g_ref, dst, rows, step=16):
    @pl.loop(0, rows // step, unroll=2)
    def _(n):
        sl = pl.ds(pl.multiple_of(n * step, step), step)
        t = src[sl, :].astype(F32)
        inv = lax.rsqrt(jnp.mean(t * t, axis=-1, keepdims=True) + EPS)
        dst[sl, :] = (t * inv * g_ref[...].astype(F32)).astype(BF)


def _big_kernel(J, R, QB, x_ref, q_ref, k_ref, v_ref, wo_ref, g2_ref, wg_ref, wu_ref, wd_ref,
                y_ref, oland, bland, rs1land,
                wg, wu, wd, rs2x, rs2y, rs3a, rs3b, hk, own,
                a2s, a2r, abs_, abr, ays, ayr, rss, rsr, lsem, wsem):
    me = lax.axis_index("tp")
    c, s = me // 2, me % 2
    D = x_ref.shape[1]
    H = D // 2
    T = x_ref.shape[0]
    C = 8 * R
    R4 = 4 * R
    hq = q_ref.shape[1]
    cx = c + 1 - 2 * (c % 2)
    cy = (c + 2) % 4
    cd = 3 - c
    dev = lambda chip, core: chip * 2 + core
    X, Y, PT = dev(cx, s), dev(cy, s), dev(c, 1 - s)
    mypos = s * 4 + c
    px, py, pd = s * 4 + cx, s * 4 + cy, s * 4 + cd

    def rcopy(src, dst, ss, rs, to):
        return pltpu.make_async_remote_copy(src_ref=src, dst_ref=dst, send_sem=ss, recv_sem=rs,
                                            device_id={"tp": to}, device_id_type=MESH)

    wcp = [pltpu.make_async_copy(wg_ref, wg, wsem.at[0]), pltpu.make_async_copy(wu_ref, wu, wsem.at[1]),
           pltpu.make_async_copy(wd_ref, wd, wsem.at[2])]

    bar = pltpu.get_barrier_semaphore()
    for m in range(1, 8):
        pl.semaphore_signal(bar, inc=1, device_id={"tp": (me + m) % 8}, device_id_type=MESH)
    pl.semaphore_wait(bar, 7)

    def peer(m):
        return (me + m) % 8

    def frm(m):
        return (me + 8 - m) % 8

    def a2a(j, m, o):
        to = peer(m)
        return rcopy(o.at[pl.ds(pl.multiple_of(j * C + _pos_of(to) * R, R), R), :],
                     oland.at[pl.ds(pl.multiple_of(j * R, R), R), pl.ds(pl.multiple_of(me * hq, HEAD), hq)],
                     a2s.at[j, m], a2r.at[j, m], to)

    def a2a_land(j, m):
        return oland.at[pl.ds(pl.multiple_of(j * R, R), R), pl.ds(pl.multiple_of(frm(m) * hq, HEAD), hq)]

    def attention(q, k, v, o, acc, mm, ll, asem):
        cps = [pltpu.make_async_copy(q_ref, q, asem.at[0]), pltpu.make_async_copy(k_ref, k, asem.at[1]),
               pltpu.make_async_copy(v_ref, v, asem.at[2])]
        for cp in cps:
            cp.start()
        for cp in wcp:
            cp.start()
        for cp in cps:
            cp.wait()
        nh = hq // HEAD
        sc = (HEAD ** -0.5) * LOG2E

        def block(row, kb, masked):
            kv = pl.ds(pl.multiple_of(kb * QB, QB), QB)
            kk, vv = k[kv, :], v[kv, :]
            for h in range(nh):
                qq = q[row, h * HEAD:(h + 1) * HEAD]
                sco = lax.dot_general(qq, kk, (((1,), (1,)), ((), ())), preferred_element_type=F32) * sc
                if masked:
                    ri = lax.broadcasted_iota(jnp.int32, (QB, QB), 0)
                    ci = lax.broadcasted_iota(jnp.int32, (QB, QB), 1)
                    sco = jnp.where(ci <= ri, sco, -jnp.inf)
                mo = mm[h, :, :1]
                mn = jnp.maximum(mo, jnp.max(sco, axis=-1, keepdims=True))
                al = jnp.exp2(mo - mn)
                p = jnp.exp2(sco - mn)
                ll[h] = ll[h] * al + jnp.sum(p, axis=-1, keepdims=True)
                acc[h] = acc[h] * al + jnp.dot(p.astype(BF), vv, preferred_element_type=F32)
                mm[h] = jnp.broadcast_to(mn, (QB, HEAD))

        @pl.loop(0, T // QB)
        def _(i):
            row = pl.ds(pl.multiple_of(i * QB, QB), QB)
            acc[...] = jnp.zeros_like(acc)
            ll[...] = jnp.zeros_like(ll)
            mm[...] = jnp.full_like(mm, -jnp.inf)

            @pl.loop(0, i)
            def _(kb):
                block(row, kb, False)

            block(row, i, True)
            for h in range(nh):
                o[row, h * HEAD:(h + 1) * HEAD] = (acc[h] / ll[h]).astype(BF)

            per = C // QB

            @pl.when(i % per == per - 1)
            def _():
                j = i // per
                for m in range(1, 8):
                    a2a(j, m, o).start()
                pltpu.make_async_copy(
                    o.at[pl.ds(pl.multiple_of(j * C + mypos * R, R), R), :],
                    oland.at[pl.ds(pl.multiple_of(j * R, R), R), pl.ds(pl.multiple_of(me * hq, HEAD), hq)],
                    a2s.at[j, 0]).start()

        @pl.loop(0, J)
        def _(j):
            pltpu.make_async_copy(
                o.at[pl.ds(pl.multiple_of(j * C + mypos * R, R), R), :],
                oland.at[pl.ds(pl.multiple_of(j * R, R), R), pl.ds(pl.multiple_of(me * hq, HEAD), hq)],
                a2s.at[j, 0]).wait()
            for m in range(1, 8):
                a2a(j, m, o).wait_send()

    pl.run_scoped(attention, pltpu.VMEM((T, hq), BF), pltpu.VMEM((T, HEAD), BF), pltpu.VMEM((T, HEAD), BF),
                  pltpu.VMEM((T, hq), BF), pltpu.VMEM((hq // HEAD, QB, HEAD), F32),
                  pltpu.VMEM((hq // HEAD, QB, HEAD), F32), pltpu.VMEM((hq // HEAD, QB, HEAD), F32),
                  pltpu.SemaphoreType.DMA((3,)))

    NT = min(512, D)

    def oproj(oo, wt, osem, tsem):
        for j in range(J):
            pltpu.make_async_copy(x_ref.at[pl.ds(pl.multiple_of(j * C + mypos * R, R), R), :],
                                  hk.at[pl.ds(j * R, R), :], osem.at[1 + j]).start()

        def tile(n, slot):
            return pltpu.make_async_copy(wo_ref.at[:, pl.ds(pl.multiple_of(n * NT, NT), NT)], wt.at[slot],
                                         tsem.at[slot])

        tile(0, 0).start()

        @pl.loop(0, J)
        def _(j):
            for m in range(1, 8):
                pltpu.make_async_remote_copy(src_ref=a2a_land(j, m), dst_ref=a2a_land(j, m), send_sem=a2s.at[j, m],
                                             recv_sem=a2r.at[j, m], device_id={"tp": frm(m)},
                                             device_id_type=MESH).wait_recv()

        cp = pltpu.make_async_copy(oland, oo, osem.at[0])
        cp.start()
        cp.wait()
        for j in range(J):
            pltpu.make_async_copy(x_ref.at[pl.ds(pl.multiple_of(j * C + mypos * R, R), R), :],
                                  hk.at[pl.ds(j * R, R), :], osem.at[1 + j]).wait()
        nt = D // NT

        @pl.loop(0, nt)
        def _(n):
            slot = n % 2

            @pl.when(n + 1 < nt)
            def _():
                tile(n + 1, 1 - slot).start()

            tile(n, slot).wait()
            col = pl.ds(pl.multiple_of(n * NT, NT), NT)
            hk[:, col] = (hk[:, col].astype(F32)
                          + jnp.dot(oo[...], wt[slot], preferred_element_type=F32)).astype(BF)

        _norm_rows(hk, g2_ref, own, J * R)

    pl.run_scoped(oproj, pltpu.VMEM((J * R, 8 * hq), BF), pltpu.VMEM((2, 8 * hq, NT), BF), pltpu.SemaphoreType.DMA((1 + J,)),
                  pltpu.SemaphoreType.DMA((2,)))

    R2 = R // 2

    def rows(land, j, pos, off=0, n=R):
        return land.at[pl.ds(pl.multiple_of(j * C + pos * R + off, R2), n), :]

    def ownrows(j):
        return own.at[pl.ds(pl.multiple_of(j * R, R), R), :]

    def g_copy(land, ss, rs, j, i):
        k = dict(ss=ss.at[j, i], rs=rs.at[j, i])
        if i < 3:
            return rcopy(ownrows(j), rows(land, j, mypos), to=(X, Y, PT)[i], **k)
        if i == 3:
            return rcopy(rows(land, j, px, 0, R2), rows(land, j, px, 0, R2), to=Y, **k)
        if i == 4:
            return rcopy(rows(land, j, py, R2, R2), rows(land, j, py, R2, R2), to=X, **k)
        if i == 5:
            return rcopy(rows(land, j, px), rows(land, j, px), to=PT, **k)
        if i == 6:
            return rcopy(rows(land, j, py), rows(land, j, py), to=PT, **k)
        off = 0 if i == 7 else R2
        return rcopy(rows(land, j, pd, off, R2), rows(land, j, pd, off, R2), to=PT, **k)

    def g_recv(land, ss, rs, j, i):
        o4 = (1 - s) * 4
        src = [(px, 0, R), (py, 0, R), (o4 + c, 0, R), (pd, 0, R2), (pd, R2, R2), (o4 + cx, 0, R), (o4 + cy, 0, R),
               (o4 + cd, 0, R2), (o4 + cd, R2, R2)][i]
        d = rows(land, j, *src)
        rcopy(d, d, ss.at[j, i], rs.at[j, i], PT).wait_recv()

    def g_local(land, j, kind):
        return pltpu.make_async_copy(ownrows(j), rows(land, j, mypos), lsem.at[kind, j])

    def g_own(land, ss, rs, j, kind):
        for i in range(3):
            g_copy(land, ss, rs, j, i).start()
        g_local(land, j, kind).start()

    def g_fwd(land, ss, rs, j):
        g_recv(land, ss, rs, j, 0)
        g_copy(land, ss, rs, j, 3).start()
        g_recv(land, ss, rs, j, 1)
        g_copy(land, ss, rs, j, 4).start()
        g_copy(land, ss, rs, j, 5).start()
        g_copy(land, ss, rs, j, 6).start()

    def g_fwd2(land, ss, rs, j):
        for i in (3, 4):
            g_recv(land, ss, rs, j, i)
            g_copy(land, ss, rs, j, i + 4).start()

    def g_finish(land, ss, rs, j):
        for i in (2, 5, 6, 7, 8):
            g_recv(land, ss, rs, j, i)

    gb = (bland, abs_, abr)
    gy = (y_ref, ays, ayr)

    def ew(n, f):
        @pl.loop(0, n // 16)
        def _(i):
            f(pl.ds(pl.multiple_of(i * 16, 16), 16))

    def mlp(bt, us, pb, rt, sums, bsem):
        def sumsl(j, chip, col):
            return sums.at[j % 2, pl.ds(pl.multiple_of(chip * R, R), R), col]

        lo, hi = pl.ds(0, H), pl.ds(H, H)

        def rs_copy(j, i):
            k = dict(ss=rss.at[j, i], rs=rsr.at[j, i])
            if i == 0:
                return rcopy(pb.at[0], rs1land.at[j], to=PT, **k)
            if i == 1:
                return rcopy(sumsl(j, cx, lo), rs2x.at[j, 0], to=X, **k)
            if i == 2:
                return rcopy(sumsl(j, cd, lo), rs2x.at[j, 1], to=X, **k)
            if i == 3:
                return rcopy(sumsl(j, cy, hi), rs2y.at[j, 0], to=Y, **k)
            if i == 4:
                return rcopy(sumsl(j, cd, hi), rs2y.at[j, 1], to=Y, **k)
            if i == 5:
                return rcopy(sumsl(j, cy, lo), rs3a.at[j], to=Y, **k)
            return rcopy(sumsl(j, cx, hi), rs3b.at[j], to=X, **k)

        def load_b(j, half):
            pos = jnp.where(half == 0, 1 - s, s) * 4 if not isinstance(half, int) else ((1 - s) if half == 0 else s) * 4
            return pltpu.make_async_copy(bland.at[pl.ds(pl.multiple_of(j * C + pos * R, R4), R4), :], bt.at[half],
                                         bsem.at[half])

        def compute(j):
            for half in range(2):
                load_b(j, half).start()
            for half in range(2):
                load_b(j, half).wait()
                if half == 0:
                    @pl.when(j >= 1)
                    def _():
                        rs_copy(j - 1, 0).wait_send()

                @pl.loop(0, us.shape[1] // 256)
                def _(n):
                    col = pl.ds(pl.multiple_of(n * 256, 256), 256)
                    g = jnp.dot(bt[half], wg[:, col], preferred_element_type=F32)
                    u = jnp.dot(bt[half], wu[:, col], preferred_element_type=F32)
                    us[:, col] = (g * jax.nn.sigmoid(g) * u).astype(BF)

                @pl.loop(0, D // 512)
                def _(n):
                    col = pl.ds(pl.multiple_of(n * 512, 512), 512)
                    pb[half, :, col] = jnp.dot(us[...], wd[:, col], preferred_element_type=F32).astype(BF)

                if half == 0:
                    rs_copy(j, 0).start()

            rs_copy(j, 0).wait_recv()
            cp = pltpu.make_async_copy(rs1land.at[j], rt, bsem.at[0])
            cp.start()
            cp.wait()

            @pl.when(j >= 2)
            def _():
                for i in range(1, 7):
                    rs_copy(j - 2, i).wait_send()

            def add(sl):
                sums[j % 2, sl, :] = (pb[1, sl, :].astype(F32) + rt[sl, :].astype(F32)).astype(BF)

            ew(R4, add)
            for i in (1, 3, 2, 4):
                rs_copy(j, i).start()

        def rs3(j):
            for i in (1, 3, 2, 4):
                rs_copy(j, i).wait_recv()

            def addy(sl):
                b = pl.ds(pl.multiple_of(cy * R + sl.start, 16), 16)
                sums[j % 2, b, lo] = (sums[j % 2, b, lo].astype(F32) + rs2x[j, 1, sl, :].astype(F32)).astype(BF)
                b = pl.ds(pl.multiple_of(cx * R + sl.start, 16), 16)
                sums[j % 2, b, hi] = (sums[j % 2, b, hi].astype(F32) + rs2y[j, 1, sl, :].astype(F32)).astype(BF)

            ew(R, addy)
            rs_copy(j, 5).start()
            rs_copy(j, 6).start()

        def final(j):
            rs_copy(j, 5).wait_recv()
            rs_copy(j, 6).wait_recv()
            for i in range(3):
                g_copy(*gb, j, i).wait_send()

            def fin(sl):
                b = pl.ds(pl.multiple_of(c * R + sl.start, 16), 16)
                o = pl.ds(pl.multiple_of(j * R + sl.start, 16), 16)
                for col, r2, r3 in ((lo, rs2x, rs3a), (hi, rs2y, rs3b)):
                    t = (sums[j % 2, b, col].astype(F32) + r2[j, 0, sl, :].astype(F32)) + r3[j, sl, :].astype(F32)
                    own[o, col] = (hk[o, col].astype(F32) + t).astype(BF)

            ew(R, fin)
            g_own(*gy, j, 1)

        g_own(*gb, 0, 0)
        for cp in wcp:
            cp.wait()

        @pl.loop(0, J + 2)
        def _(t):
            @pl.when(t < J)
            def _():
                g_fwd(*gb, t)

            @pl.when(jnp.logical_and(t >= 1, t <= J))
            def _():
                rs3(t - 1)

            @pl.when(t >= 2)
            def _():
                g_fwd(*gy, t - 2)

            @pl.when(t + 1 < J)
            def _():
                g_own(*gb, t + 1, 0)

            @pl.when(t < J)
            def _():
                g_fwd2(*gb, t)

            @pl.when(jnp.logical_and(t >= 1, t <= J))
            def _():
                final(t - 1)

            @pl.when(t < J)
            def _():
                g_finish(*gb, t)
                g_local(bland, t, 0).wait()
                compute(t)

            @pl.when(t >= 2)
            def _():
                g_fwd2(*gy, t - 2)

        rs_copy(J - 1, 0).wait_send()
        for j in range(max(J - 2, 0), J):
            for i in range(1, 7):
                rs_copy(j, i).wait_send()

    pl.run_scoped(mlp, pltpu.VMEM((2, R4, D), BF), pltpu.VMEM((R4, wg.shape[1]), BF), pltpu.VMEM((2, R4, D), BF),
                  pltpu.VMEM((R4, D), BF), pltpu.VMEM((2, R4, D), BF), pltpu.SemaphoreType.DMA((2,)))

    @pl.loop(0, J)
    def _(j):
        g_finish(*gy, j)
        for i in range(3, 9):
            g_copy(*gb, j, i).wait_send()
        for i in range(9):
            g_copy(*gy, j, i).wait_send()
        g_local(y_ref, j, 1).wait()


def _tables(pos):
    half = HEAD // 2
    inv = ROPE_BASE ** (-2.0 * jnp.arange(half, dtype=F32) / HEAD)
    t = pos.shape[0]
    p = pos.astype(F32)
    lane = lax.broadcasted_iota(jnp.int32, (t // 2, HEAD), 1)
    pp = jnp.where(lane < half, p[:t // 2, None], p[t // 2:, None])
    ang = pp * jnp.concatenate([inv, inv])[None, :]
    return jnp.cos(ang), jnp.sin(ang)


def solution(mesh):
    def local(x, pos, g1, g2, wq, wk, wv, wo, wg, wu, wd):
        t, d = x.shape
        hq = wq.shape[1]
        ff = wg.shape[1]
        wo_full = lax.all_gather(wo, "tp", axis=0, tiled=True)
        cs, sn = _tables(pos)
        tm = min(512, t // 2)
        nb = t // tm
        row = lambda i: (i, 0)
        q, k, v = pl.pallas_call(
            functools.partial(_qkv_kernel, nb),
            grid=(nb,),
            in_specs=[pl.BlockSpec((tm, d), row), pl.BlockSpec((1, d), lambda i: (0, 0)),
                      pl.BlockSpec((tm, HEAD), lambda i: (i % (nb // 2), 0)),
                      pl.BlockSpec((tm, HEAD), lambda i: (i % (nb // 2), 0)), ANY, ANY, ANY],
            out_specs=[pl.BlockSpec((tm, hq), row), pl.BlockSpec((tm, HEAD), row), pl.BlockSpec((tm, HEAD), row)],
            out_shape=[jax.ShapeDtypeStruct((t, hq), BF), jax.ShapeDtypeStruct((t, HEAD), BF),
                       jax.ShapeDtypeStruct((t, HEAD), BF)],
            scratch_shapes=[pltpu.VMEM((d, hq + 2 * HEAD), BF), pltpu.VMEM((tm, d), BF),
                            pltpu.SemaphoreType.DMA((3,))],
            compiler_params=pltpu.CompilerParams(dimension_semantics=("arbitrary",), vmem_limit_bytes=40 << 20),
            cost_estimate=pl.CostEstimate(flops=2 * t * d * (hq + 2 * HEAD), bytes_accessed=2 * t * d,
                                          transcendentals=0),
            name="qkv",
        )(x, g1.reshape(1, d), cs, sn, wq, wk, wv)

        J = NCHUNK
        R = t // 8 // J
        QB = min(512, 8 * R)
        dma = pltpu.SemaphoreType.DMA
        y, _, _, _ = pl.pallas_call(
            functools.partial(_big_kernel, J, R, QB),
            in_specs=[ANY] * 5 + [pl.BlockSpec(memory_space=pltpu.VMEM)] + [ANY] * 3,
            out_specs=[ANY] * 4,
            out_shape=[jax.ShapeDtypeStruct((t, d), BF), jax.ShapeDtypeStruct((J * R, 8 * hq), BF),
                       jax.ShapeDtypeStruct((t, d), BF), jax.ShapeDtypeStruct((J, 4 * R, d), BF)],
            scratch_shapes=[pltpu.VMEM((d, ff), BF), pltpu.VMEM((d, ff), BF), pltpu.VMEM((ff, d), BF),
                            pltpu.VMEM((J, 2, R, d // 2), BF), pltpu.VMEM((J, 2, R, d // 2), BF),
                            pltpu.VMEM((J, R, d // 2), BF), pltpu.VMEM((J, R, d // 2), BF),
                            pltpu.VMEM((J * R, d), BF), pltpu.VMEM((J * R, d), BF),
                            dma((J, 8)), dma((J, 8)), dma((J, 9)), dma((J, 9)), dma((J, 9)), dma((J, 9)),
                            dma((J, 7)), dma((J, 7)), dma((2, J)), dma((3,))],
            compiler_params=pltpu.CompilerParams(collective_id=0, has_side_effects=True,
                                                 vmem_limit_bytes=67043328),
            cost_estimate=pl.CostEstimate(flops=2 * t * d * ff * 3, bytes_accessed=2 * t * d * 6, transcendentals=0),
            name="layer",
        )(x, q, k, v, wo_full, g2.reshape(1, d), wg, wu, wd)
        return y, k.reshape(t, 1, HEAD), v.reshape(t, 1, HEAD)

    return jax.shard_map(
        local,
        mesh=mesh,
        in_specs=(P("dp", None), P("dp"), P(), P(), P(None, "tp"), P(), P(), P("tp", None),
                  P(None, "tp"), P(None, "tp"), P("tp", None)),
        out_specs=(P("dp", None), P("dp", "tp", None), P("dp", "tp", None)),
        check_vma=False,
    )
```

```python
import functools

import jax
import jax.numpy as jnp
from jax import lax
from jax.experimental import pallas as pl
from jax.experimental.pallas import tpu as pltpu
from jax.sharding import PartitionSpec as P

HEAD = 128
EPS = 1e-5
ROPE_BASE = 500000.0
LOG2E = 1.4426950408889634
NCHUNK = 4
MESH = pl.DeviceIdType.MESH
F32, BF = jnp.float32, jnp.bfloat16
ANY = pl.BlockSpec(memory_space=pl.ANY)


def _pos_of(r):
    return (r % 2) * 4 + r // 2


def _norm_rows(src, g_ref, dst, rows, step=16):
    @pl.loop(0, rows // step, unroll=2)
    def _(n):
        sl = pl.ds(pl.multiple_of(n * step, step), step)
        t = src[sl, :].astype(F32)
        inv = lax.rsqrt(jnp.mean(t * t, axis=-1, keepdims=True) + EPS)
        dst[sl, :] = (t * inv * g_ref[...].astype(F32)).astype(BF)


def _big_kernel(J, R, QB, x_ref, g1_ref, g2_ref, cos_ref, sin_ref, wq_ref, wk_ref, wv_ref, wo_ref, wg_ref, wu_ref,
                wd_ref, y_ref, kout, vout, oland, bland, rs1land, woland,
                wg, wu, wd, rs2x, rs2y, rs3a, rs3b, hk, own,
                a2s, a2r, abs_, abr, ays, ayr, rss, rsr, wos, wor, lsem, wsem):
    me = lax.axis_index("tp")
    c, s = me // 2, me % 2
    T, D = x_ref.shape
    H = D // 2
    C = 8 * R
    R4 = 4 * R
    hq = wq_ref.shape[1]
    nh = hq // HEAD
    cx = c + 1 - 2 * (c % 2)
    cy = (c + 2) % 4
    cd = 3 - c
    dev = lambda chip, core: chip * 2 + core
    X, Y, DG, PT = dev(cx, s), dev(cy, s), dev(cd, s), dev(c, 1 - s)
    mypos = s * 4 + c
    px, py, pd = s * 4 + cx, s * 4 + cy, s * 4 + cd

    def rcopy(src, dst, ss, rs, to):
        return pltpu.make_async_remote_copy(src_ref=src, dst_ref=dst, send_sem=ss, recv_sem=rs,
                                            device_id={"tp": to}, device_id_type=MESH)

    wcp = [pltpu.make_async_copy(wg_ref, wg, wsem.at[0]), pltpu.make_async_copy(wu_ref, wu, wsem.at[1]),
           pltpu.make_async_copy(wd_ref, wd, wsem.at[2])]

    bar = pltpu.get_barrier_semaphore()
    for m in range(1, 8):
        pl.semaphore_signal(bar, inc=1, device_id={"tp": (me + m) % 8}, device_id_type=MESH)
    pl.semaphore_wait(bar, 7)

    W2 = hq // 2

    def worows(d, off=0, n=hq):
        return woland.at[pl.ds(pl.multiple_of(d * hq + off, W2), n), :]

    def wo_copy(i):
        k = dict(ss=wos.at[i], rs=wor.at[i])
        if i < 3:
            return rcopy(wo_ref, worows(me), to=(X, Y, PT)[i], **k)
        d, off, n, to = ((X, 0, W2, Y), (Y, W2, W2, X), (X, 0, hq, PT), (Y, 0, hq, PT), (DG, 0, W2, PT),
                         (DG, W2, W2, PT))[i - 3]
        return rcopy(worows(d, off, n), worows(d, off, n), to=to, **k)

    def wo_recv(i):
        d = worows(*((X,), (Y,), (PT,), (DG, 0, W2), (DG, W2, W2), (dev(cx, 1 - s),), (dev(cy, 1 - s),),
                     (dev(cd, 1 - s), 0, W2), (dev(cd, 1 - s), W2, W2))[i])
        rcopy(d, d, wos.at[i], wor.at[i], PT).wait_recv()

    wo_in = pltpu.make_async_copy(wo_ref, hk.at[pl.ds(0, hq), :], lsem.at[0, 0])
    wo_out = pltpu.make_async_copy(hk.at[pl.ds(0, hq), :], worows(me), lsem.at[0, 0])

    def peer(m):
        return (me + m) % 8

    def frm(m):
        return (me + 8 - m) % 8

    def a2a(j, m, o):
        to = peer(m)
        return rcopy(o.at[pl.ds(pl.multiple_of(j * C + _pos_of(to) * R, R), R), :],
                     oland.at[pl.ds(pl.multiple_of(j * R, R), R), pl.ds(pl.multiple_of(me * hq, HEAD), hq)],
                     a2s.at[j, m], a2r.at[j, m], to)

    def a2a_land(j, m):
        return oland.at[pl.ds(pl.multiple_of(j * R, R), R), pl.ds(pl.multiple_of(frm(m) * hq, HEAD), hq)]

    def a2a_own(j, o):
        return pltpu.make_async_copy(o.at[pl.ds(pl.multiple_of(j * C + mypos * R, R), R), :], a2a_land(j, 0),
                                     a2s.at[j, 0])

    TM = min(512, T // 2)

    def qkv(q, k, v, vt):
        def run(w, xt, ct, st, tsem, msem):
            nb = T // TM
            col = pl.ds(pl.multiple_of(me * HEAD, HEAD), HEAD)
            cps = [pltpu.make_async_copy(wq_ref, w.at[:, pl.ds(0, hq)], msem.at[0]),
                   pltpu.make_async_copy(wk_ref.at[:, col], w.at[:, pl.ds(hq, HEAD)], msem.at[1]),
                   pltpu.make_async_copy(wv_ref.at[:, col], w.at[:, pl.ds(hq + HEAD, HEAD)], msem.at[2])]

            def tile(i, slot):
                r = pl.ds(pl.multiple_of(i * TM, TM), TM)
                t = pl.ds(pl.multiple_of((i % (nb // 2)) * TM, TM), TM)
                return [pltpu.make_async_copy(x_ref.at[r, :], xt.at[slot], tsem.at[slot, 0]),
                        pltpu.make_async_copy(cos_ref.at[t, :], ct.at[slot], tsem.at[slot, 1]),
                        pltpu.make_async_copy(sin_ref.at[t, :], st.at[slot], tsem.at[slot, 2])]

            for cp in tile(0, 0) + cps:
                cp.start()
            for i in range(3):
                wo_copy(i).start()
            wo_in.start()

            @pl.loop(0, nb)
            def _(i):
                slot = i % 2

                @pl.when(i + 1 < nb)
                def _():
                    for cp in tile(i + 1, 1 - slot):
                        cp.start()

                for cp in tile(i, slot):
                    cp.wait()
                _norm_rows(xt.at[slot], g1_ref, xt.at[slot], TM)

                @pl.when(i == 0)
                def _():
                    for cp in cps:
                        cp.wait()

                row = pl.ds(pl.multiple_of(i * TM, TM), TM)
                low = lax.broadcasted_iota(jnp.int32, (TM, HEAD), 1) < HEAD // 2
                keep = jnp.logical_xor(low, i >= nb // 2)
                cb, sb = ct[slot], st[slot]
                cc = jnp.where(keep, cb, pltpu.roll(cb, HEAD // 2, 1))
                ss = jnp.where(keep, sb, pltpu.roll(sb, HEAD // 2, 1))
                ss = jnp.where(low, -ss, ss)
                z = jnp.dot(xt[slot], w[...], preferred_element_type=F32)
                for h in range(nh + 1):
                    t = z[:, h * HEAD:(h + 1) * HEAD]
                    t = (t * cc + pltpu.roll(t, HEAD // 2, 1) * ss).astype(BF)
                    if h < nh:
                        q[row, h * HEAD:(h + 1) * HEAD] = t
                    else:
                        k[row, :] = t
                zv = z[:, hq + HEAD:]
                v[row, :] = zv.astype(BF)
                vt[:, row] = zv.T.astype(BF)

        pl.run_scoped(run, pltpu.VMEM((D, hq + 2 * HEAD), BF), pltpu.VMEM((2, TM, D), BF),
                      pltpu.VMEM((2, TM, HEAD), F32), pltpu.VMEM((2, TM, HEAD), F32),
                      pltpu.SemaphoreType.DMA((2, 3)), pltpu.SemaphoreType.DMA((3,)))

    def attention(q, k, v, vt, acc, mm, ll, mx, sb, asem):
        qkv(q, k, v, vt)
        kv_out = [pltpu.make_async_copy(k, kout, asem.at[0]), pltpu.make_async_copy(v, vout, asem.at[1])]
        for cp in kv_out + wcp:
            cp.start()
        wo_in.wait()
        wo_out.start()
        sc = (HEAD ** -0.5) * LOG2E
        nq = T // QB
        ki = lax.broadcasted_iota(jnp.int32, (QB, QB), 0)
        qi = lax.broadcasted_iota(jnp.int32, (QB, QB), 1)

        @pl.loop(0, nq)
        def _(i):
            row = pl.ds(pl.multiple_of(i * QB, QB), QB)

            def qk(kb, h, masked=False):
                kk = k[pl.ds(pl.multiple_of(kb * QB, QB), QB), :]
                t = lax.dot_general(kk, q[row, h * HEAD:(h + 1) * HEAD], (((1,), (1,)), ((), ())),
                                    preferred_element_type=F32)
                if masked:
                    t = jnp.where(ki <= qi, t, -jnp.inf)
                sb[h] = t
                mx[h] = jnp.max(t, axis=0, keepdims=True)

            def soft(kb, h):
                mo = mm[h]
                mn = jnp.maximum(mo, mx[h])
                mm[h] = mn
                al = jnp.exp2((mo - mn) * sc)
                p = jnp.exp2((sb[h] - mn) * sc)
                ll[h] = ll[h] * al + jnp.sum(p, axis=0, keepdims=True)
                acc[h] = acc[h] * al + jnp.dot(vt[:, pl.ds(pl.multiple_of(kb * QB, QB), QB)], p.astype(BF),
                                               preferred_element_type=F32)

            acc[...] = jnp.zeros_like(acc)
            ll[...] = jnp.zeros_like(ll)
            mm[...] = jnp.full_like(mm, -jnp.inf)

            def phases(kb, nxt, masked):
                for h in range(nh):
                    ahead = h + nh - 1
                    if ahead < nh:
                        qk(kb, ahead, masked)
                    else:
                        qk(nxt, ahead - nh)
                    soft(kb, h)

            for h in range(nh - 1):
                qk(i, h, True)
            phases(i, 0, True)

            @pl.loop(0, i)
            def _(kb):
                phases(kb, kb + 1, False)

            for h in range(nh):
                q[row, h * HEAD:(h + 1) * HEAD] = (acc[h] / ll[h]).T.astype(BF)

            per = C // QB

            @pl.when(i % per == per - 1)
            def _():
                j = i // per
                for m in range(1, 8):
                    a2a(j, m, q).start()
                a2a_own(j, q).start()

            @pl.when(i == nq // 2)
            def _():
                for n in (0, 1):
                    wo_recv(n)
                    wo_copy(n + 3).start()
                for n in (5, 6):
                    wo_copy(n).start()

        for n in (3, 4):
            wo_recv(n)
            wo_copy(n + 4).start()
        for cp in kv_out:
            cp.wait()

        @pl.loop(0, J)
        def _(j):
            a2a_own(j, q).wait()
            for m in range(1, 8):
                a2a(j, m, q).wait_send()

    pl.run_scoped(attention, pltpu.VMEM((T, hq), BF), pltpu.VMEM((T, HEAD), BF), pltpu.VMEM((T, HEAD), BF),
                  pltpu.VMEM((HEAD, T), BF), pltpu.VMEM((nh, HEAD, QB), F32),
                  pltpu.VMEM((nh, 1, QB), F32), pltpu.VMEM((nh, 1, QB), F32), pltpu.VMEM((nh, 1, QB), F32),
                  pltpu.VMEM((nh, QB, QB), F32), pltpu.SemaphoreType.DMA((2,)))
    wo_out.wait()
    for n in (2, 5, 6, 7, 8):
        wo_recv(n)
    for n in range(9):
        wo_copy(n).wait_send()

    NT = min(512, D)

    def oproj(oo, wt, osem, tsem):
        for j in range(J):
            pltpu.make_async_copy(x_ref.at[pl.ds(pl.multiple_of(j * C + mypos * R, R), R), :],
                                  hk.at[pl.ds(j * R, R), :], osem.at[1 + j]).start()

        def tile(n, slot):
            return pltpu.make_async_copy(woland.at[:, pl.ds(pl.multiple_of(n * NT, NT), NT)], wt.at[slot],
                                         tsem.at[slot])

        tile(0, 0).start()

        @pl.loop(0, J)
        def _(j):
            for m in range(1, 8):
                pltpu.make_async_remote_copy(src_ref=a2a_land(j, m), dst_ref=a2a_land(j, m), send_sem=a2s.at[j, m],
                                             recv_sem=a2r.at[j, m], device_id={"tp": frm(m)},
                                             device_id_type=MESH).wait_recv()

        cp = pltpu.make_async_copy(oland, oo, osem.at[0])
        cp.start()
        cp.wait()
        for j in range(J):
            pltpu.make_async_copy(x_ref.at[pl.ds(pl.multiple_of(j * C + mypos * R, R), R), :],
                                  hk.at[pl.ds(j * R, R), :], osem.at[1 + j]).wait()
        nt = D // NT

        @pl.loop(0, nt)
        def _(n):
            slot = n % 2

            @pl.when(n + 1 < nt)
            def _():
                tile(n + 1, 1 - slot).start()

            tile(n, slot).wait()
            col = pl.ds(pl.multiple_of(n * NT, NT), NT)
            hk[:, col] = (hk[:, col].astype(F32)
                          + jnp.dot(oo[...], wt[slot], preferred_element_type=F32)).astype(BF)

        _norm_rows(hk, g2_ref, own, J * R)

    pl.run_scoped(oproj, pltpu.VMEM((J * R, 8 * hq), BF), pltpu.VMEM((2, 8 * hq, NT), BF), pltpu.SemaphoreType.DMA((1 + J,)),
                  pltpu.SemaphoreType.DMA((2,)))

    R2 = R // 2

    def rows(land, j, pos, off=0, n=R):
        return land.at[pl.ds(pl.multiple_of(j * C + pos * R + off, R2), n), :]

    def ownrows(j):
        return own.at[pl.ds(pl.multiple_of(j * R, R), R), :]

    def g_copy(land, ss, rs, j, i):
        k = dict(ss=ss.at[j, i], rs=rs.at[j, i])
        if i < 3:
            return rcopy(ownrows(j), rows(land, j, mypos), to=(X, Y, PT)[i], **k)
        if i == 3:
            return rcopy(rows(land, j, px, 0, R2), rows(land, j, px, 0, R2), to=Y, **k)
        if i == 4:
            return rcopy(rows(land, j, py, R2, R2), rows(land, j, py, R2, R2), to=X, **k)
        if i == 5:
            return rcopy(rows(land, j, px), rows(land, j, px), to=PT, **k)
        if i == 6:
            return rcopy(rows(land, j, py), rows(land, j, py), to=PT, **k)
        off = 0 if i == 7 else R2
        return rcopy(rows(land, j, pd, off, R2), rows(land, j, pd, off, R2), to=PT, **k)

    def g_recv(land, ss, rs, j, i):
        o4 = (1 - s) * 4
        src = [(px, 0, R), (py, 0, R), (o4 + c, 0, R), (pd, 0, R2), (pd, R2, R2), (o4 + cx, 0, R), (o4 + cy, 0, R),
               (o4 + cd, 0, R2), (o4 + cd, R2, R2)][i]
        d = rows(land, j, *src)
        rcopy(d, d, ss.at[j, i], rs.at[j, i], PT).wait_recv()

    def g_local(land, j, kind):
        return pltpu.make_async_copy(ownrows(j), rows(land, j, mypos), lsem.at[kind, j])

    def g_own(land, ss, rs, j, kind):
        for i in range(3):
            g_copy(land, ss, rs, j, i).start()
        g_local(land, j, kind).start()

    def g_fwd(land, ss, rs, j):
        g_recv(land, ss, rs, j, 0)
        g_copy(land, ss, rs, j, 3).start()
        g_recv(land, ss, rs, j, 1)
        g_copy(land, ss, rs, j, 4).start()
        g_copy(land, ss, rs, j, 5).start()
        g_copy(land, ss, rs, j, 6).start()

    def g_fwd2(land, ss, rs, j):
        for i in (3, 4):
            g_recv(land, ss, rs, j, i)
            g_copy(land, ss, rs, j, i + 4).start()

    def g_finish(land, ss, rs, j):
        for i in (2, 5, 6, 7, 8):
            g_recv(land, ss, rs, j, i)

    gb = (bland, abs_, abr)
    gy = (y_ref, ays, ayr)

    def ew(n, f):
        @pl.loop(0, n // 16)
        def _(i):
            f(pl.ds(pl.multiple_of(i * 16, 16), 16))

    def mlp(bt, us, pb, rt, sums, bsem):
        def sumsl(j, chip, col):
            return sums.at[j % 2, pl.ds(pl.multiple_of(chip * R, R), R), col]

        lo, hi = pl.ds(0, H), pl.ds(H, H)

        def rs_copy(j, i):
            k = dict(ss=rss.at[j, i], rs=rsr.at[j, i])
            if i == 0:
                return rcopy(pb.at[0], rs1land.at[j], to=PT, **k)
            if i == 1:
                return rcopy(sumsl(j, cx, lo), rs2x.at[j, 0], to=X, **k)
            if i == 2:
                return rcopy(sumsl(j, cd, lo), rs2x.at[j, 1], to=X, **k)
            if i == 3:
                return rcopy(sumsl(j, cy, hi), rs2y.at[j, 0], to=Y, **k)
            if i == 4:
                return rcopy(sumsl(j, cd, hi), rs2y.at[j, 1], to=Y, **k)
            if i == 5:
                return rcopy(sumsl(j, cy, lo), rs3a.at[j], to=Y, **k)
            return rcopy(sumsl(j, cx, hi), rs3b.at[j], to=X, **k)

        def load_b(j, half):
            pos = jnp.where(half == 0, 1 - s, s) * 4 if not isinstance(half, int) else ((1 - s) if half == 0 else s) * 4
            return pltpu.make_async_copy(bland.at[pl.ds(pl.multiple_of(j * C + pos * R, R4), R4), :], bt.at[half],
                                         bsem.at[half])

        def compute(j):
            for half in range(2):
                load_b(j, half).start()
            for half in range(2):
                load_b(j, half).wait()
                if half == 0:
                    @pl.when(j >= 1)
                    def _():
                        rs_copy(j - 1, 0).wait_send()

                @pl.loop(0, us.shape[1] // 256)
                def _(n):
                    col = pl.ds(pl.multiple_of(n * 256, 256), 256)
                    g = jnp.dot(bt[half], wg[:, col], preferred_element_type=F32)
                    u = jnp.dot(bt[half], wu[:, col], preferred_element_type=F32)
                    us[:, col] = (g * jax.nn.sigmoid(g) * u).astype(BF)

                @pl.loop(0, D // 512)
                def _(n):
                    col = pl.ds(pl.multiple_of(n * 512, 512), 512)
                    pb[half, :, col] = jnp.dot(us[...], wd[:, col], preferred_element_type=F32).astype(BF)

                if half == 0:
                    rs_copy(j, 0).start()

            rs_copy(j, 0).wait_recv()
            cp = pltpu.make_async_copy(rs1land.at[j], rt, bsem.at[0])
            cp.start()
            cp.wait()

            @pl.when(j >= 2)
            def _():
                for i in range(1, 7):
                    rs_copy(j - 2, i).wait_send()

            def add(sl):
                sums[j % 2, sl, :] = (pb[1, sl, :].astype(F32) + rt[sl, :].astype(F32)).astype(BF)

            ew(R4, add)
            for i in (1, 3, 2, 4):
                rs_copy(j, i).start()

        def rs3(j):
            for i in (1, 3, 2, 4):
                rs_copy(j, i).wait_recv()

            def addy(sl):
                b = pl.ds(pl.multiple_of(cy * R + sl.start, 16), 16)
                sums[j % 2, b, lo] = (sums[j % 2, b, lo].astype(F32) + rs2x[j, 1, sl, :].astype(F32)).astype(BF)
                b = pl.ds(pl.multiple_of(cx * R + sl.start, 16), 16)
                sums[j % 2, b, hi] = (sums[j % 2, b, hi].astype(F32) + rs2y[j, 1, sl, :].astype(F32)).astype(BF)

            ew(R, addy)
            rs_copy(j, 5).start()
            rs_copy(j, 6).start()

        def final(j):
            rs_copy(j, 5).wait_recv()
            rs_copy(j, 6).wait_recv()
            for i in range(3):
                g_copy(*gb, j, i).wait_send()

            def fin(sl):
                b = pl.ds(pl.multiple_of(c * R + sl.start, 16), 16)
                o = pl.ds(pl.multiple_of(j * R + sl.start, 16), 16)
                for col, r2, r3 in ((lo, rs2x, rs3a), (hi, rs2y, rs3b)):
                    t = (sums[j % 2, b, col].astype(F32) + r2[j, 0, sl, :].astype(F32)) + r3[j, sl, :].astype(F32)
                    own[o, col] = (hk[o, col].astype(F32) + t).astype(BF)

            ew(R, fin)
            g_own(*gy, j, 1)

        g_own(*gb, 0, 0)
        for cp in wcp:
            cp.wait()

        @pl.loop(0, J + 2)
        def _(t):
            @pl.when(t < J)
            def _():
                g_fwd(*gb, t)

            @pl.when(jnp.logical_and(t >= 1, t <= J))
            def _():
                rs3(t - 1)

            @pl.when(t >= 2)
            def _():
                g_fwd(*gy, t - 2)

            @pl.when(t + 1 < J)
            def _():
                g_own(*gb, t + 1, 0)

            @pl.when(t < J)
            def _():
                g_fwd2(*gb, t)

            @pl.when(jnp.logical_and(t >= 1, t <= J))
            def _():
                final(t - 1)

            @pl.when(t < J)
            def _():
                g_finish(*gb, t)
                g_local(bland, t, 0).wait()
                compute(t)

            @pl.when(t >= 2)
            def _():
                g_fwd2(*gy, t - 2)

        rs_copy(J - 1, 0).wait_send()
        for j in range(max(J - 2, 0), J):
            for i in range(1, 7):
                rs_copy(j, i).wait_send()

    pl.run_scoped(mlp, pltpu.VMEM((2, R4, D), BF), pltpu.VMEM((R4, wg.shape[1]), BF), pltpu.VMEM((2, R4, D), BF),
                  pltpu.VMEM((R4, D), BF), pltpu.VMEM((2, R4, D), BF), pltpu.SemaphoreType.DMA((2,)))

    @pl.loop(0, J)
    def _(j):
        g_finish(*gy, j)
        for i in range(3, 9):
            g_copy(*gb, j, i).wait_send()
        for i in range(9):
            g_copy(*gy, j, i).wait_send()
        g_local(y_ref, j, 1).wait()


def _tables(pos):
    half = HEAD // 2
    inv = ROPE_BASE ** (-2.0 * jnp.arange(half, dtype=F32) / HEAD)
    t = pos.shape[0]
    p = pos.astype(F32)
    lane = lax.broadcasted_iota(jnp.int32, (t // 2, HEAD), 1)
    pp = jnp.where(lane < half, p[:t // 2, None], p[t // 2:, None])
    ang = pp * jnp.concatenate([inv, inv])[None, :]
    return jnp.cos(ang), jnp.sin(ang)


def solution(mesh):
    def local(x, pos, g1, g2, wq, wk, wv, wo, wg, wu, wd):
        t, d = x.shape
        hq = wq.shape[1]
        ff = wg.shape[1]
        cs, sn = _tables(pos)
        J = NCHUNK
        R = t // 8 // J
        QB = min(512, 8 * R)
        dma = pltpu.SemaphoreType.DMA
        vm = pl.BlockSpec(memory_space=pltpu.VMEM)
        big = lambda *sh: jax.ShapeDtypeStruct(sh, BF)
        y, k, v, *_ = pl.pallas_call(
            functools.partial(_big_kernel, J, R, QB),
            in_specs=[ANY, vm, vm] + [ANY] * 9,
            out_specs=[ANY] * 7,
            out_shape=[big(t, d), big(t, HEAD), big(t, HEAD), big(J * R, 8 * hq), big(t, d), big(J, 4 * R, d),
                       big(8 * hq, d)],
            scratch_shapes=[pltpu.VMEM((d, ff), BF), pltpu.VMEM((d, ff), BF), pltpu.VMEM((ff, d), BF),
                            pltpu.VMEM((J, 2, R, d // 2), BF), pltpu.VMEM((J, 2, R, d // 2), BF),
                            pltpu.VMEM((J, R, d // 2), BF), pltpu.VMEM((J, R, d // 2), BF),
                            pltpu.VMEM((J * R, d), BF), pltpu.VMEM((J * R, d), BF),
                            dma((J, 8)), dma((J, 8)), dma((J, 9)), dma((J, 9)), dma((J, 9)), dma((J, 9)),
                            dma((J, 7)), dma((J, 7)), dma((9,)), dma((9,)), dma((2, J)), dma((3,))],
            compiler_params=pltpu.CompilerParams(collective_id=0, has_side_effects=True,
                                                 vmem_limit_bytes=67043328),
            cost_estimate=pl.CostEstimate(flops=2 * t * d * ff * 4, bytes_accessed=2 * t * d * 6, transcendentals=0),
            name="layer",
        )(x, g1.reshape(1, d), g2.reshape(1, d), cs, sn, wq, wk, wv, wo, wg, wu, wd)
        return y, k.reshape(t, 1, HEAD), v.reshape(t, 1, HEAD)

    return jax.shard_map(
        local,
        mesh=mesh,
        in_specs=(P("dp", None), P("dp"), P(), P(), P(None, "tp"), P(), P(), P("tp", None),
                  P(None, "tp"), P(None, "tp"), P("tp", None)),
        out_specs=(P("dp", None), P("dp", "tp", None), P("dp", "tp", None)),
        check_vma=False,
    )
```

```python
import functools

import jax
import jax.numpy as jnp
from jax import lax
from jax.experimental import pallas as pl
from jax.experimental.pallas import tpu as pltpu
from jax.sharding import PartitionSpec as P

HEAD = 128
EPS = 1e-5
ROPE_BASE = 500000.0
LOG2E = 1.4426950408889634
NCHUNK = 8
MESH = pl.DeviceIdType.MESH
F32, BF = jnp.float32, jnp.bfloat16
ANY = pl.BlockSpec(memory_space=pl.ANY)


def _pos_of(r):
    return (r % 2) * 4 + r // 2


def _norm_rows(src, g_ref, dst, rows, step=16):
    @pl.loop(0, rows // step, unroll=2)
    def _(n):
        sl = pl.ds(pl.multiple_of(n * step, step), step)
        t = src[sl, :].astype(F32)
        inv = lax.rsqrt(jnp.mean(t * t, axis=-1, keepdims=True) + EPS)
        dst[sl, :] = (t * inv * g_ref[...].astype(F32)).astype(BF)


def _big_kernel(J, R, QB, x_ref, g1_ref, g2_ref, cos_ref, sin_ref, wq_ref, wk_ref, wv_ref, wo_ref, wg_ref, wu_ref,
                wd_ref, y_ref, kout, vout, oland, bland, rs1land, woland,
                wg, wu, wd, rs2x, rs2y, rs3a, rs3b, hk, own,
                a2s, a2r, abs_, abr, ays, ayr, rss, rsr, wos, wor, lsem, wsem):
    me = lax.axis_index("tp")
    c, s = me // 2, me % 2
    T, D = x_ref.shape
    H = D // 2
    C = 8 * R
    R4 = 4 * R
    hq = wq_ref.shape[1]
    nh = hq // HEAD
    cx = c + 1 - 2 * (c % 2)
    cy = (c + 2) % 4
    cd = 3 - c
    dev = lambda chip, core: chip * 2 + core
    X, Y, DG, PT = dev(cx, s), dev(cy, s), dev(cd, s), dev(c, 1 - s)
    mypos = s * 4 + c
    px, py, pd = s * 4 + cx, s * 4 + cy, s * 4 + cd

    def rcopy(src, dst, ss, rs, to):
        return pltpu.make_async_remote_copy(src_ref=src, dst_ref=dst, send_sem=ss, recv_sem=rs,
                                            device_id={"tp": to}, device_id_type=MESH)

    wcp = [pltpu.make_async_copy(wg_ref, wg, wsem.at[0]), pltpu.make_async_copy(wu_ref, wu, wsem.at[1]),
           pltpu.make_async_copy(wd_ref, wd, wsem.at[2])]

    bar = pltpu.get_barrier_semaphore()
    for m in range(1, 8):
        pl.semaphore_signal(bar, inc=1, device_id={"tp": (me + m) % 8}, device_id_type=MESH)
    pl.semaphore_wait(bar, 7)

    W2 = hq // 2

    def worows(d, off=0, n=hq):
        return woland.at[pl.ds(pl.multiple_of(d * hq + off, W2), n), :]

    def wo_copy(i):
        k = dict(ss=wos.at[i], rs=wor.at[i])
        if i < 3:
            return rcopy(wo_ref, worows(me), to=(X, Y, PT)[i], **k)
        d, off, n, to = ((X, 0, W2, Y), (Y, W2, W2, X), (X, 0, hq, PT), (Y, 0, hq, PT), (DG, 0, W2, PT),
                         (DG, W2, W2, PT))[i - 3]
        return rcopy(worows(d, off, n), worows(d, off, n), to=to, **k)

    def wo_recv(i):
        d = worows(*((X,), (Y,), (PT,), (DG, 0, W2), (DG, W2, W2), (dev(cx, 1 - s),), (dev(cy, 1 - s),),
                     (dev(cd, 1 - s), 0, W2), (dev(cd, 1 - s), W2, W2))[i])
        rcopy(d, d, wos.at[i], wor.at[i], PT).wait_recv()

    wo_in = pltpu.make_async_copy(wo_ref, hk.at[pl.ds(0, hq), :], lsem.at[0, 0])
    wo_out = pltpu.make_async_copy(hk.at[pl.ds(0, hq), :], worows(me), lsem.at[0, 0])

    def peer(m):
        return (me + m) % 8

    def frm(m):
        return (me + 8 - m) % 8

    def a2a(j, m, o):
        to = peer(m)
        return rcopy(o.at[pl.ds(pl.multiple_of(j * C + _pos_of(to) * R, R), R), :],
                     oland.at[pl.ds(pl.multiple_of(j * R, R), R), pl.ds(pl.multiple_of(me * hq, HEAD), hq)],
                     a2s.at[j, m], a2r.at[j, m], to)

    def a2a_land(j, m):
        return oland.at[pl.ds(pl.multiple_of(j * R, R), R), pl.ds(pl.multiple_of(frm(m) * hq, HEAD), hq)]

    def a2a_own(j, o):
        return pltpu.make_async_copy(o.at[pl.ds(pl.multiple_of(j * C + mypos * R, R), R), :], a2a_land(j, 0),
                                     a2s.at[j, 0])

    TM = min(512, T // 2)

    def qkv(q, k, v, vt):
        def run(w, xt, ct, st, tsem, msem):
            nb = T // TM
            col = pl.ds(pl.multiple_of(me * HEAD, HEAD), HEAD)
            cps = [pltpu.make_async_copy(wq_ref, w.at[:, pl.ds(0, hq)], msem.at[0]),
                   pltpu.make_async_copy(wk_ref.at[:, col], w.at[:, pl.ds(hq, HEAD)], msem.at[1]),
                   pltpu.make_async_copy(wv_ref.at[:, col], w.at[:, pl.ds(hq + HEAD, HEAD)], msem.at[2])]

            def tile(i, slot):
                r = pl.ds(pl.multiple_of(i * TM, TM), TM)
                t = pl.ds(pl.multiple_of((i % (nb // 2)) * TM, TM), TM)
                return [pltpu.make_async_copy(x_ref.at[r, :], xt.at[slot], tsem.at[slot, 0]),
                        pltpu.make_async_copy(cos_ref.at[t, :], ct.at[slot], tsem.at[slot, 1]),
                        pltpu.make_async_copy(sin_ref.at[t, :], st.at[slot], tsem.at[slot, 2])]

            for cp in tile(0, 0) + cps:
                cp.start()
            for i in range(3):
                wo_copy(i).start()
            wo_in.start()

            @pl.loop(0, nb)
            def _(i):
                slot = i % 2

                @pl.when(i + 1 < nb)
                def _():
                    for cp in tile(i + 1, 1 - slot):
                        cp.start()

                for cp in tile(i, slot):
                    cp.wait()
                _norm_rows(xt.at[slot], g1_ref, xt.at[slot], TM)

                @pl.when(i == 0)
                def _():
                    for cp in cps:
                        cp.wait()

                row = pl.ds(pl.multiple_of(i * TM, TM), TM)
                low = lax.broadcasted_iota(jnp.int32, (TM, HEAD), 1) < HEAD // 2
                keep = jnp.logical_xor(low, i >= nb // 2)
                cb, sb = ct[slot], st[slot]
                cc = jnp.where(keep, cb, pltpu.roll(cb, HEAD // 2, 1))
                ss = jnp.where(keep, sb, pltpu.roll(sb, HEAD // 2, 1))
                ss = jnp.where(low, -ss, ss)
                z = jnp.dot(xt[slot], w[...], preferred_element_type=F32)
                for h in range(nh + 1):
                    t = z[:, h * HEAD:(h + 1) * HEAD]
                    t = (t * cc + pltpu.roll(t, HEAD // 2, 1) * ss).astype(BF)
                    if h < nh:
                        q[row, h * HEAD:(h + 1) * HEAD] = t
                    else:
                        k[row, :] = t
                zv = z[:, hq + HEAD:]
                v[row, :] = zv.astype(BF)
                vt[:, row] = zv.T.astype(BF)

        pl.run_scoped(run, pltpu.VMEM((D, hq + 2 * HEAD), BF), pltpu.VMEM((2, TM, D), BF),
                      pltpu.VMEM((2, TM, HEAD), F32), pltpu.VMEM((2, TM, HEAD), F32),
                      pltpu.SemaphoreType.DMA((2, 3)), pltpu.SemaphoreType.DMA((3,)))

    def attention(q, k, v, vt, acc, mm, ll, mx, sb, asem):
        qkv(q, k, v, vt)
        kv_out = [pltpu.make_async_copy(k, kout, asem.at[0]), pltpu.make_async_copy(v, vout, asem.at[1])]
        for cp in kv_out + wcp:
            cp.start()
        wo_in.wait()
        wo_out.start()
        sc = (HEAD ** -0.5) * LOG2E
        nq = T // QB
        ki = lax.broadcasted_iota(jnp.int32, (QB, QB), 0)
        qi = lax.broadcasted_iota(jnp.int32, (QB, QB), 1)

        @pl.loop(0, nq)
        def _(i):
            row = pl.ds(pl.multiple_of(i * QB, QB), QB)

            def qk(kb, h, masked=False):
                kk = k[pl.ds(pl.multiple_of(kb * QB, QB), QB), :]
                t = lax.dot_general(kk, q[row, h * HEAD:(h + 1) * HEAD], (((1,), (1,)), ((), ())),
                                    preferred_element_type=F32)
                if masked:
                    t = jnp.where(ki <= qi, t, -jnp.inf)
                sb[h] = t
                mx[h] = jnp.max(t, axis=0, keepdims=True)

            def soft(kb, h):
                mo = mm[h]
                mn = jnp.maximum(mo, mx[h])
                mm[h] = mn
                al = jnp.exp2((mo - mn) * sc)
                p = jnp.exp2((sb[h] - mn) * sc)
                ll[h] = ll[h] * al + jnp.sum(p, axis=0, keepdims=True)
                acc[h] = acc[h] * al + jnp.dot(vt[:, pl.ds(pl.multiple_of(kb * QB, QB), QB)], p.astype(BF),
                                               preferred_element_type=F32)

            acc[...] = jnp.zeros_like(acc)
            ll[...] = jnp.zeros_like(ll)
            mm[...] = jnp.full_like(mm, -jnp.inf)

            def phases(kb, nxt, masked):
                for h in range(nh):
                    ahead = h + nh - 1
                    if ahead < nh:
                        qk(kb, ahead, masked)
                    else:
                        qk(nxt, ahead - nh)
                    soft(kb, h)

            for h in range(nh - 1):
                qk(i, h, True)
            phases(i, 0, True)

            @pl.loop(0, i)
            def _(kb):
                phases(kb, kb + 1, False)

            for h in range(nh):
                q[row, h * HEAD:(h + 1) * HEAD] = (acc[h] / ll[h]).T.astype(BF)

            per = C // QB

            @pl.when(i % per == per - 1)
            def _():
                j = i // per
                for m in range(1, 8):
                    a2a(j, m, q).start()
                a2a_own(j, q).start()

            @pl.when(i == nq // 2)
            def _():
                for n in (0, 1):
                    wo_recv(n)
                    wo_copy(n + 3).start()
                for n in (5, 6):
                    wo_copy(n).start()

        for n in (3, 4):
            wo_recv(n)
            wo_copy(n + 4).start()
        for cp in kv_out:
            cp.wait()

        @pl.loop(0, J)
        def _(j):
            a2a_own(j, q).wait()
            for m in range(1, 8):
                a2a(j, m, q).wait_send()

    pl.run_scoped(attention, pltpu.VMEM((T, hq), BF), pltpu.VMEM((T, HEAD), BF), pltpu.VMEM((T, HEAD), BF),
                  pltpu.VMEM((HEAD, T), BF), pltpu.VMEM((nh, HEAD, QB), F32),
                  pltpu.VMEM((nh, 1, QB), F32), pltpu.VMEM((nh, 1, QB), F32), pltpu.VMEM((nh, 1, QB), F32),
                  pltpu.VMEM((nh, QB, QB), F32), pltpu.SemaphoreType.DMA((2,)))
    wo_out.wait()
    for n in (2, 5, 6, 7, 8):
        wo_recv(n)
    for n in range(9):
        wo_copy(n).wait_send()

    NT = min(512, D)

    def oproj(oo, wt, osem, tsem):
        for j in range(J):
            pltpu.make_async_copy(x_ref.at[pl.ds(pl.multiple_of(j * C + mypos * R, R), R), :],
                                  hk.at[pl.ds(j * R, R), :], osem.at[1 + j]).start()

        def tile(n, slot):
            return pltpu.make_async_copy(woland.at[:, pl.ds(pl.multiple_of(n * NT, NT), NT)], wt.at[slot],
                                         tsem.at[slot])

        tile(0, 0).start()

        @pl.loop(0, J)
        def _(j):
            for m in range(1, 8):
                pltpu.make_async_remote_copy(src_ref=a2a_land(j, m), dst_ref=a2a_land(j, m), send_sem=a2s.at[j, m],
                                             recv_sem=a2r.at[j, m], device_id={"tp": frm(m)},
                                             device_id_type=MESH).wait_recv()

        cp = pltpu.make_async_copy(oland, oo, osem.at[0])
        cp.start()
        cp.wait()
        for j in range(J):
            pltpu.make_async_copy(x_ref.at[pl.ds(pl.multiple_of(j * C + mypos * R, R), R), :],
                                  hk.at[pl.ds(j * R, R), :], osem.at[1 + j]).wait()
        nt = D // NT

        @pl.loop(0, nt)
        def _(n):
            slot = n % 2

            @pl.when(n + 1 < nt)
            def _():
                tile(n + 1, 1 - slot).start()

            tile(n, slot).wait()
            col = pl.ds(pl.multiple_of(n * NT, NT), NT)
            hk[:, col] = (hk[:, col].astype(F32)
                          + jnp.dot(oo[...], wt[slot], preferred_element_type=F32)).astype(BF)

        _norm_rows(hk, g2_ref, own, J * R)

    pl.run_scoped(oproj, pltpu.VMEM((J * R, 8 * hq), BF), pltpu.VMEM((2, 8 * hq, NT), BF), pltpu.SemaphoreType.DMA((1 + J,)),
                  pltpu.SemaphoreType.DMA((2,)))

    R2 = R // 2

    def rows(land, j, pos, off=0, n=R):
        return land.at[pl.ds(pl.multiple_of(j * C + pos * R + off, R2), n), :]

    def ownrows(j):
        return own.at[pl.ds(pl.multiple_of(j * R, R), R), :]

    def g_copy(land, ss, rs, j, i):
        k = dict(ss=ss.at[j, i], rs=rs.at[j, i])
        if i < 3:
            return rcopy(ownrows(j), rows(land, j, mypos), to=(X, Y, PT)[i], **k)
        if i == 3:
            return rcopy(rows(land, j, px, 0, R2), rows(land, j, px, 0, R2), to=Y, **k)
        if i == 4:
            return rcopy(rows(land, j, py, R2, R2), rows(land, j, py, R2, R2), to=X, **k)
        if i == 5:
            return rcopy(rows(land, j, px), rows(land, j, px), to=PT, **k)
        if i == 6:
            return rcopy(rows(land, j, py), rows(land, j, py), to=PT, **k)
        off = 0 if i == 7 else R2
        return rcopy(rows(land, j, pd, off, R2), rows(land, j, pd, off, R2), to=PT, **k)

    def g_recv(land, ss, rs, j, i):
        o4 = (1 - s) * 4
        src = [(px, 0, R), (py, 0, R), (o4 + c, 0, R), (pd, 0, R2), (pd, R2, R2), (o4 + cx, 0, R), (o4 + cy, 0, R),
               (o4 + cd, 0, R2), (o4 + cd, R2, R2)][i]
        d = rows(land, j, *src)
        rcopy(d, d, ss.at[j, i], rs.at[j, i], PT).wait_recv()

    def g_local(land, j, kind):
        return pltpu.make_async_copy(ownrows(j), rows(land, j, mypos), lsem.at[kind, j])

    def g_own(land, ss, rs, j, kind):
        for i in range(3):
            g_copy(land, ss, rs, j, i).start()
        g_local(land, j, kind).start()

    def g_fwd(land, ss, rs, j):
        g_recv(land, ss, rs, j, 0)
        g_copy(land, ss, rs, j, 3).start()
        g_recv(land, ss, rs, j, 1)
        g_copy(land, ss, rs, j, 4).start()
        g_copy(land, ss, rs, j, 5).start()
        g_copy(land, ss, rs, j, 6).start()

    def g_fwd2(land, ss, rs, j):
        for i in (3, 4):
            g_recv(land, ss, rs, j, i)
            g_copy(land, ss, rs, j, i + 4).start()

    def g_finish(land, ss, rs, j):
        for i in (2, 5, 6, 7, 8):
            g_recv(land, ss, rs, j, i)

    gb = (bland, abs_, abr)
    gy = (y_ref, ays, ayr)

    def ew(n, f):
        @pl.loop(0, n // 16)
        def _(i):
            f(pl.ds(pl.multiple_of(i * 16, 16), 16))

    def mlp(bt, us, pb, rt, sums, bsem):
        def sumsl(j, chip, col):
            return sums.at[j % 2, pl.ds(pl.multiple_of(chip * R, R), R), col]

        lo, hi = pl.ds(0, H), pl.ds(H, H)

        def rs_copy(j, i):
            k = dict(ss=rss.at[j, i], rs=rsr.at[j, i])
            if i == 0:
                return rcopy(pb.at[0], rs1land.at[j], to=PT, **k)
            if i == 1:
                return rcopy(sumsl(j, cx, lo), rs2x.at[j, 0], to=X, **k)
            if i == 2:
                return rcopy(sumsl(j, cd, lo), rs2x.at[j, 1], to=X, **k)
            if i == 3:
                return rcopy(sumsl(j, cy, hi), rs2y.at[j, 0], to=Y, **k)
            if i == 4:
                return rcopy(sumsl(j, cd, hi), rs2y.at[j, 1], to=Y, **k)
            if i == 5:
                return rcopy(sumsl(j, cy, lo), rs3a.at[j], to=Y, **k)
            return rcopy(sumsl(j, cx, hi), rs3b.at[j], to=X, **k)

        def load_b(j, half):
            pos = jnp.where(half == 0, 1 - s, s) * 4 if not isinstance(half, int) else ((1 - s) if half == 0 else s) * 4
            return pltpu.make_async_copy(bland.at[pl.ds(pl.multiple_of(j * C + pos * R, R4), R4), :], bt.at[half],
                                         bsem.at[half])

        def compute(j):
            for half in range(2):
                load_b(j, half).start()
            for half in range(2):
                load_b(j, half).wait()
                if half == 0:
                    @pl.when(j >= 1)
                    def _():
                        rs_copy(j - 1, 0).wait_send()

                @pl.loop(0, us.shape[1] // 256)
                def _(n):
                    col = pl.ds(pl.multiple_of(n * 256, 256), 256)
                    g = jnp.dot(bt[half], wg[:, col], preferred_element_type=F32)
                    u = jnp.dot(bt[half], wu[:, col], preferred_element_type=F32)
                    us[:, col] = (g * jax.nn.sigmoid(g) * u).astype(BF)

                @pl.loop(0, D // 512)
                def _(n):
                    col = pl.ds(pl.multiple_of(n * 512, 512), 512)
                    pb[half, :, col] = jnp.dot(us[...], wd[:, col], preferred_element_type=F32).astype(BF)

                if half == 0:
                    rs_copy(j, 0).start()

            rs_copy(j, 0).wait_recv()
            cp = pltpu.make_async_copy(rs1land.at[j], rt, bsem.at[0])
            cp.start()
            cp.wait()

            @pl.when(j >= 2)
            def _():
                for i in range(1, 7):
                    rs_copy(j - 2, i).wait_send()

            def add(sl):
                sums[j % 2, sl, :] = (pb[1, sl, :].astype(F32) + rt[sl, :].astype(F32)).astype(BF)

            ew(R4, add)
            for i in (1, 3, 2, 4):
                rs_copy(j, i).start()

        def rs3(j):
            for i in (1, 3, 2, 4):
                rs_copy(j, i).wait_recv()

            def addy(sl):
                b = pl.ds(pl.multiple_of(cy * R + sl.start, 16), 16)
                sums[j % 2, b, lo] = (sums[j % 2, b, lo].astype(F32) + rs2x[j, 1, sl, :].astype(F32)).astype(BF)
                b = pl.ds(pl.multiple_of(cx * R + sl.start, 16), 16)
                sums[j % 2, b, hi] = (sums[j % 2, b, hi].astype(F32) + rs2y[j, 1, sl, :].astype(F32)).astype(BF)

            ew(R, addy)
            rs_copy(j, 5).start()
            rs_copy(j, 6).start()

        def final(j):
            rs_copy(j, 5).wait_recv()
            rs_copy(j, 6).wait_recv()
            for i in range(3):
                g_copy(*gb, j, i).wait_send()

            def fin(sl):
                b = pl.ds(pl.multiple_of(c * R + sl.start, 16), 16)
                o = pl.ds(pl.multiple_of(j * R + sl.start, 16), 16)
                for col, r2, r3 in ((lo, rs2x, rs3a), (hi, rs2y, rs3b)):
                    t = (sums[j % 2, b, col].astype(F32) + r2[j, 0, sl, :].astype(F32)) + r3[j, sl, :].astype(F32)
                    own[o, col] = (hk[o, col].astype(F32) + t).astype(BF)

            ew(R, fin)
            g_own(*gy, j, 1)

        g_own(*gb, 0, 0)
        for cp in wcp:
            cp.wait()

        @pl.loop(0, J + 2)
        def _(t):
            @pl.when(t < J)
            def _():
                g_fwd(*gb, t)

            @pl.when(jnp.logical_and(t >= 1, t <= J))
            def _():
                rs3(t - 1)

            @pl.when(t >= 2)
            def _():
                g_fwd(*gy, t - 2)

            @pl.when(t + 1 < J)
            def _():
                g_own(*gb, t + 1, 0)

            @pl.when(t < J)
            def _():
                g_fwd2(*gb, t)

            @pl.when(jnp.logical_and(t >= 1, t <= J))
            def _():
                final(t - 1)

            @pl.when(t < J)
            def _():
                g_finish(*gb, t)
                g_local(bland, t, 0).wait()
                compute(t)

            @pl.when(t >= 2)
            def _():
                g_fwd2(*gy, t - 2)

        rs_copy(J - 1, 0).wait_send()
        for j in range(max(J - 2, 0), J):
            for i in range(1, 7):
                rs_copy(j, i).wait_send()

    pl.run_scoped(mlp, pltpu.VMEM((2, R4, D), BF), pltpu.VMEM((R4, wg.shape[1]), BF), pltpu.VMEM((2, R4, D), BF),
                  pltpu.VMEM((R4, D), BF), pltpu.VMEM((2, R4, D), BF), pltpu.SemaphoreType.DMA((2,)))

    @pl.loop(0, J)
    def _(j):
        g_finish(*gy, j)
        for i in range(3, 9):
            g_copy(*gb, j, i).wait_send()
        for i in range(9):
            g_copy(*gy, j, i).wait_send()
        g_local(y_ref, j, 1).wait()


def _tables(pos):
    half = HEAD // 2
    inv = ROPE_BASE ** (-2.0 * jnp.arange(half, dtype=F32) / HEAD)
    t = pos.shape[0]
    p = pos.astype(F32)
    lane = lax.broadcasted_iota(jnp.int32, (t // 2, HEAD), 1)
    pp = jnp.where(lane < half, p[:t // 2, None], p[t // 2:, None])
    ang = pp * jnp.concatenate([inv, inv])[None, :]
    return jnp.cos(ang), jnp.sin(ang)


def solution(mesh):
    def local(x, pos, g1, g2, wq, wk, wv, wo, wg, wu, wd):
        t, d = x.shape
        hq = wq.shape[1]
        ff = wg.shape[1]
        cs, sn = _tables(pos)
        J = NCHUNK
        R = t // 8 // J
        QB = min(512, 8 * R)
        dma = pltpu.SemaphoreType.DMA
        vm = pl.BlockSpec(memory_space=pltpu.VMEM)
        big = lambda *sh: jax.ShapeDtypeStruct(sh, BF)
        y, k, v, *_ = pl.pallas_call(
            functools.partial(_big_kernel, J, R, QB),
            in_specs=[ANY, vm, vm] + [ANY] * 9,
            out_specs=[ANY] * 7,
            out_shape=[big(t, d), big(t, HEAD), big(t, HEAD), big(J * R, 8 * hq), big(t, d), big(J, 4 * R, d),
                       big(8 * hq, d)],
            scratch_shapes=[pltpu.VMEM((d, ff), BF), pltpu.VMEM((d, ff), BF), pltpu.VMEM((ff, d), BF),
                            pltpu.VMEM((J, 2, R, d // 2), BF), pltpu.VMEM((J, 2, R, d // 2), BF),
                            pltpu.VMEM((J, R, d // 2), BF), pltpu.VMEM((J, R, d // 2), BF),
                            pltpu.VMEM((J * R, d), BF), pltpu.VMEM((J * R, d), BF),
                            dma((J, 8)), dma((J, 8)), dma((J, 9)), dma((J, 9)), dma((J, 9)), dma((J, 9)),
                            dma((J, 7)), dma((J, 7)), dma((9,)), dma((9,)), dma((2, J)), dma((3,))],
            compiler_params=pltpu.CompilerParams(collective_id=0, has_side_effects=True,
                                                 vmem_limit_bytes=67043328),
            cost_estimate=pl.CostEstimate(flops=2 * t * d * ff * 4, bytes_accessed=2 * t * d * 6, transcendentals=0),
            name="layer",
        )(x, g1.reshape(1, d), g2.reshape(1, d), cs, sn, wq, wk, wv, wo, wg, wu, wd)
        return y, k.reshape(t, 1, HEAD), v.reshape(t, 1, HEAD)

    return jax.shard_map(
        local,
        mesh=mesh,
        in_specs=(P("dp", None), P("dp"), P(), P(), P(None, "tp"), P(), P(), P("tp", None),
                  P(None, "tp"), P(None, "tp"), P("tp", None)),
        out_specs=(P("dp", None), P("dp", "tp", None), P("dp", "tp", None)),
        check_vma=False,
    )
```

```python
import functools

import jax
import jax.numpy as jnp
from jax import lax
from jax.experimental import pallas as pl
from jax.experimental.pallas import tpu as pltpu
from jax.sharding import PartitionSpec as P

HEAD = 128
EPS = 1e-5
ROPE_BASE = 500000.0
LOG2E = 1.4426950408889634
NCHUNK = 8
MESH = pl.DeviceIdType.MESH
F32, BF = jnp.float32, jnp.bfloat16
ANY = pl.BlockSpec(memory_space=pl.ANY)


def _pos_of(r):
    return (r % 2) * 4 + r // 2


def _norm_rows(src, g_ref, dst, rows, step=16):
    @pl.loop(0, rows // step, unroll=2)
    def _(n):
        sl = pl.ds(pl.multiple_of(n * step, step), step)
        t = src[sl, :].astype(F32)
        inv = lax.rsqrt(jnp.mean(t * t, axis=-1, keepdims=True) + EPS)
        dst[sl, :] = (t * inv * g_ref[...].astype(F32)).astype(BF)


def _copy_kernel(i_ref, o_ref):
    o_ref[...] = i_ref[...]


def _big_kernel(J, R, QB, x_ref, g1_ref, g2_ref, cos_ref, sin_ref, wq_ref, wk_ref, wv_ref, wo_ref, wg_ref, wu_ref,
                wd_ref, y_ref, kout, vout, oland, bland, rs1land, woland,
                wg, wu, wd, rs2x, rs2y, rs3a, rs3b, hk, own,
                a2s, a2r, abs_, abr, ays, ayr, rss, rsr, wos, wor, lsem, wsem):
    me = lax.axis_index("tp")
    c, s = me // 2, me % 2
    T, D = x_ref.shape
    H = D // 2
    C = 8 * R
    R4 = 4 * R
    hq = wq_ref.shape[1]
    nh = hq // HEAD
    cx = c + 1 - 2 * (c % 2)
    cy = (c + 2) % 4
    cd = 3 - c
    dev = lambda chip, core: chip * 2 + core
    X, Y, DG, PT = dev(cx, s), dev(cy, s), dev(cd, s), dev(c, 1 - s)
    mypos = s * 4 + c
    px, py, pd = s * 4 + cx, s * 4 + cy, s * 4 + cd

    def rcopy(src, dst, ss, rs, to):
        return pltpu.make_async_remote_copy(src_ref=src, dst_ref=dst, send_sem=ss, recv_sem=rs,
                                            device_id={"tp": to}, device_id_type=MESH)

    wcp = [pltpu.make_async_copy(wg_ref, wg, wsem.at[0]), pltpu.make_async_copy(wu_ref, wu, wsem.at[1]),
           pltpu.make_async_copy(wd_ref, wd, wsem.at[2])]

    bar = pltpu.get_barrier_semaphore()
    for m in range(1, 8):
        pl.semaphore_signal(bar, inc=1, device_id={"tp": (me + m) % 8}, device_id_type=MESH)
    pl.semaphore_wait(bar, 7)

    W2 = hq // 2

    def worows(d, off=0, n=hq):
        return woland.at[pl.ds(pl.multiple_of(d * hq + off, W2), n), :]

    def wo_copy(i):
        k = dict(ss=wos.at[i], rs=wor.at[i])
        if i < 3:
            return rcopy(wo_ref, worows(me), to=(X, Y, PT)[i], **k)
        d, off, n, to = ((X, 0, W2, Y), (Y, W2, W2, X), (X, 0, hq, PT), (Y, 0, hq, PT), (DG, 0, W2, PT),
                         (DG, W2, W2, PT))[i - 3]
        return rcopy(worows(d, off, n), worows(d, off, n), to=to, **k)

    def wo_recv(i):
        d = worows(*((X,), (Y,), (PT,), (DG, 0, W2), (DG, W2, W2), (dev(cx, 1 - s),), (dev(cy, 1 - s),),
                     (dev(cd, 1 - s), 0, W2), (dev(cd, 1 - s), W2, W2))[i])
        rcopy(d, d, wos.at[i], wor.at[i], PT).wait_recv()

    wo_in = pltpu.make_async_copy(wo_ref, hk.at[pl.ds(0, hq), :], lsem.at[0, 0])
    wo_out = pltpu.make_async_copy(hk.at[pl.ds(0, hq), :], worows(me), lsem.at[0, 0])

    def peer(m):
        return (me + m) % 8

    def frm(m):
        return (me + 8 - m) % 8

    def a2a(j, m, o):
        to = peer(m)
        return rcopy(o.at[pl.ds(pl.multiple_of(j * C + _pos_of(to) * R, R), R), :],
                     oland.at[pl.ds(pl.multiple_of(j * R, R), R), pl.ds(pl.multiple_of(me * hq, HEAD), hq)],
                     a2s.at[j, m], a2r.at[j, m], to)

    def a2a_land(j, m):
        return oland.at[pl.ds(pl.multiple_of(j * R, R), R), pl.ds(pl.multiple_of(frm(m) * hq, HEAD), hq)]

    def a2a_own(j, o):
        return pltpu.make_async_copy(o.at[pl.ds(pl.multiple_of(j * C + mypos * R, R), R), :], a2a_land(j, 0),
                                     a2s.at[j, 0])

    TM = min(512, T // 2)

    def qkv(q, k, v, vt):
        def run(w, xt, ct, st, tsem, msem):
            nb = T // TM
            col = pl.ds(pl.multiple_of(me * HEAD, HEAD), HEAD)
            cps = [pltpu.make_async_copy(wq_ref, w.at[:, pl.ds(0, hq)], msem.at[0]),
                   pltpu.make_async_copy(wk_ref.at[:, col], w.at[:, pl.ds(hq, HEAD)], msem.at[1]),
                   pltpu.make_async_copy(wv_ref.at[:, col], w.at[:, pl.ds(hq + HEAD, HEAD)], msem.at[2])]

            def tile(i, slot):
                r = pl.ds(pl.multiple_of(i * TM, TM), TM)
                t = pl.ds(pl.multiple_of((i % (nb // 2)) * TM, TM), TM)
                return [pltpu.make_async_copy(x_ref.at[r, :], xt.at[slot], tsem.at[slot, 0]),
                        pltpu.make_async_copy(cos_ref.at[t, :], ct.at[slot], tsem.at[slot, 1]),
                        pltpu.make_async_copy(sin_ref.at[t, :], st.at[slot], tsem.at[slot, 2])]

            for cp in tile(0, 0) + cps:
                cp.start()
            for i in range(3):
                wo_copy(i).start()
            wo_in.start()

            @pl.loop(0, nb)
            def _(i):
                slot = i % 2

                @pl.when(i + 1 < nb)
                def _():
                    for cp in tile(i + 1, 1 - slot):
                        cp.start()

                for cp in tile(i, slot):
                    cp.wait()
                _norm_rows(xt.at[slot], g1_ref, xt.at[slot], TM)

                @pl.when(i == 0)
                def _():
                    for cp in cps:
                        cp.wait()

                row = pl.ds(pl.multiple_of(i * TM, TM), TM)
                low = lax.broadcasted_iota(jnp.int32, (TM, HEAD), 1) < HEAD // 2
                keep = jnp.logical_xor(low, i >= nb // 2)
                cb, sb = ct[slot], st[slot]
                cc = jnp.where(keep, cb, pltpu.roll(cb, HEAD // 2, 1))
                ss = jnp.where(keep, sb, pltpu.roll(sb, HEAD // 2, 1))
                ss = jnp.where(low, -ss, ss)
                z = jnp.dot(xt[slot], w[...], preferred_element_type=F32)
                for h in range(nh + 1):
                    t = z[:, h * HEAD:(h + 1) * HEAD]
                    t = (t * cc + pltpu.roll(t, HEAD // 2, 1) * ss).astype(BF)
                    if h < nh:
                        q[row, h * HEAD:(h + 1) * HEAD] = t
                    else:
                        k[row, :] = t
                zv = z[:, hq + HEAD:]
                v[row, :] = zv.astype(BF)
                vt[:, row] = zv.T.astype(BF)

        pl.run_scoped(run, pltpu.VMEM((D, hq + 2 * HEAD), BF), pltpu.VMEM((2, TM, D), BF),
                      pltpu.VMEM((2, TM, HEAD), F32), pltpu.VMEM((2, TM, HEAD), F32),
                      pltpu.SemaphoreType.DMA((2, 3)), pltpu.SemaphoreType.DMA((3,)))

    def attention(q, k, v, vt, acc, mm, ll, mx, sb, asem):
        qkv(q, k, v, vt)
        kv_out = [pltpu.make_async_copy(k, kout, asem.at[0]), pltpu.make_async_copy(v, vout, asem.at[1])]
        for cp in kv_out + wcp:
            cp.start()
        wo_in.wait()
        wo_out.start()
        sc = (HEAD ** -0.5) * LOG2E
        nq = T // QB
        ki = lax.broadcasted_iota(jnp.int32, (QB, QB), 0)
        qi = lax.broadcasted_iota(jnp.int32, (QB, QB), 1)

        @pl.loop(0, nq)
        def _(i):
            row = pl.ds(pl.multiple_of(i * QB, QB), QB)

            def qk(kb, h, masked=False):
                kk = k[pl.ds(pl.multiple_of(kb * QB, QB), QB), :]
                t = lax.dot_general(kk, q[row, h * HEAD:(h + 1) * HEAD], (((1,), (1,)), ((), ())),
                                    preferred_element_type=F32)
                if masked:
                    t = jnp.where(ki <= qi, t, -jnp.inf)
                sb[h] = t
                mx[h] = jnp.max(t, axis=0, keepdims=True)

            def soft(kb, h):
                mo = mm[h]
                mn = jnp.maximum(mo, mx[h])
                mm[h] = mn
                al = jnp.exp2((mo - mn) * sc)
                p = jnp.exp2((sb[h] - mn) * sc)
                ll[h] = ll[h] * al + jnp.sum(p, axis=0, keepdims=True)
                acc[h] = acc[h] * al + jnp.dot(vt[:, pl.ds(pl.multiple_of(kb * QB, QB), QB)], p.astype(BF),
                                               preferred_element_type=F32)

            acc[...] = jnp.zeros_like(acc)
            ll[...] = jnp.zeros_like(ll)
            mm[...] = jnp.full_like(mm, -jnp.inf)

            def phases(kb, nxt, masked):
                for h in range(nh):
                    ahead = h + nh - 1
                    if ahead < nh:
                        qk(kb, ahead, masked)
                    else:
                        qk(nxt, ahead - nh)
                    soft(kb, h)

            for h in range(nh - 1):
                qk(i, h, True)
            phases(i, 0, True)

            @pl.loop(0, i)
            def _(kb):
                phases(kb, kb + 1, False)

            for h in range(nh):
                q[row, h * HEAD:(h + 1) * HEAD] = (acc[h] / ll[h]).T.astype(BF)

            per = C // QB

            @pl.when(i % per == per - 1)
            def _():
                j = i // per
                for m in range(1, 8):
                    a2a(j, m, q).start()
                a2a_own(j, q).start()

            @pl.when(i == nq // 2)
            def _():
                for n in (0, 1):
                    wo_recv(n)
                    wo_copy(n + 3).start()
                for n in (5, 6):
                    wo_copy(n).start()

        for n in (3, 4):
            wo_recv(n)
            wo_copy(n + 4).start()
        for cp in kv_out:
            cp.wait()

        @pl.loop(0, J)
        def _(j):
            a2a_own(j, q).wait()
            for m in range(1, 8):
                a2a(j, m, q).wait_send()

    pl.run_scoped(attention, pltpu.VMEM((T, hq), BF), pltpu.VMEM((T, HEAD), BF), pltpu.VMEM((T, HEAD), BF),
                  pltpu.VMEM((HEAD, T), BF), pltpu.VMEM((nh, HEAD, QB), F32),
                  pltpu.VMEM((nh, 1, QB), F32), pltpu.VMEM((nh, 1, QB), F32), pltpu.VMEM((nh, 1, QB), F32),
                  pltpu.VMEM((nh, QB, QB), F32), pltpu.SemaphoreType.DMA((2,)))
    wo_out.wait()
    for n in (2, 5, 6, 7, 8):
        wo_recv(n)
    for n in range(9):
        wo_copy(n).wait_send()

    R2 = R // 2

    def rows(land, j, pos, off=0, n=R):
        return land.at[pl.ds(pl.multiple_of(j * C + pos * R + off, R2), n), :]

    def ownrows(j):
        return own.at[pl.ds(pl.multiple_of(j * R, R), R), :]

    def g_copy(land, ss, rs, j, i):
        k = dict(ss=ss.at[j, i], rs=rs.at[j, i])
        if i < 3:
            return rcopy(ownrows(j), rows(land, j, mypos), to=(X, Y, PT)[i], **k)
        if i == 3:
            return rcopy(rows(land, j, px, 0, R2), rows(land, j, px, 0, R2), to=Y, **k)
        if i == 4:
            return rcopy(rows(land, j, py, R2, R2), rows(land, j, py, R2, R2), to=X, **k)
        if i == 5:
            return rcopy(rows(land, j, px), rows(land, j, px), to=PT, **k)
        if i == 6:
            return rcopy(rows(land, j, py), rows(land, j, py), to=PT, **k)
        off = 0 if i == 7 else R2
        return rcopy(rows(land, j, pd, off, R2), rows(land, j, pd, off, R2), to=PT, **k)

    def g_recv(land, ss, rs, j, i):
        o4 = (1 - s) * 4
        src = [(px, 0, R), (py, 0, R), (o4 + c, 0, R), (pd, 0, R2), (pd, R2, R2), (o4 + cx, 0, R), (o4 + cy, 0, R),
               (o4 + cd, 0, R2), (o4 + cd, R2, R2)][i]
        d = rows(land, j, *src)
        rcopy(d, d, ss.at[j, i], rs.at[j, i], PT).wait_recv()

    def g_local(land, j, kind):
        return pltpu.make_async_copy(ownrows(j), rows(land, j, mypos), lsem.at[kind, j])

    def g_own(land, ss, rs, j, kind):
        for i in range(3):
            g_copy(land, ss, rs, j, i).start()
        g_local(land, j, kind).start()

    def g_fwd(land, ss, rs, j):
        g_recv(land, ss, rs, j, 0)
        g_copy(land, ss, rs, j, 3).start()
        g_recv(land, ss, rs, j, 1)
        g_copy(land, ss, rs, j, 4).start()
        g_copy(land, ss, rs, j, 5).start()
        g_copy(land, ss, rs, j, 6).start()

    def g_fwd2(land, ss, rs, j):
        for i in (3, 4):
            g_recv(land, ss, rs, j, i)
            g_copy(land, ss, rs, j, i + 4).start()

    def g_finish(land, ss, rs, j):
        for i in (2, 5, 6, 7, 8):
            g_recv(land, ss, rs, j, i)

    gb = (bland, abs_, abr)
    gy = (y_ref, ays, ayr)

    def ew(n, f):
        @pl.loop(0, n // 16)
        def _(i):
            f(pl.ds(pl.multiple_of(i * 16, 16), 16))

    def mlp(bt, us, pb, rt, sums, oo, wt, bsem, osem, tsem):
        NT = wt.shape[2]
        JH = J // 2
        RH = JH * R

        def x_in(j):
            return pltpu.make_async_copy(x_ref.at[pl.ds(pl.multiple_of(j * C + mypos * R, R), R), :],
                                         hk.at[pl.ds(pl.multiple_of(j * R, R), R), :], osem.at[1 + j])

        def oproj(half):
            part = pl.ds(half * RH, RH)

            def tile(n, slot):
                return pltpu.make_async_copy(woland.at[:, pl.ds(pl.multiple_of(n * NT, NT), NT)], wt.at[slot],
                                             tsem.at[slot])

            tile(0, 0).start()

            @pl.loop(half * JH, (half + 1) * JH)
            def _(j):
                for m in range(1, 8):
                    d = a2a_land(j, m)
                    rcopy(d, d, a2s.at[j, m], a2r.at[j, m], PT).wait_recv()

            cp = pltpu.make_async_copy(oland.at[part, :], oo, osem.at[0])
            cp.start()
            cp.wait()
            for j in range(half * JH, (half + 1) * JH):
                x_in(j).wait()
            nt = D // NT

            @pl.loop(0, nt)
            def _(n):
                slot = n % 2

                @pl.when(n + 1 < nt)
                def _():
                    tile(n + 1, 1 - slot).start()

                tile(n, slot).wait()
                col = pl.ds(pl.multiple_of(n * NT, NT), NT)
                hk[part, col] = (hk[part, col].astype(F32)
                                 + jnp.dot(oo[...], wt[slot], preferred_element_type=F32)).astype(BF)

            _norm_rows(hk.at[part, :], g2_ref, own.at[part, :], RH)

        def sumsl(j, chip, col):
            return sums.at[j % 2, pl.ds(pl.multiple_of(chip * R, R), R), col]

        lo, hi = pl.ds(0, H), pl.ds(H, H)

        def rs_copy(j, i):
            k = dict(ss=rss.at[j, i], rs=rsr.at[j, i])
            if i == 0:
                return rcopy(pb.at[0], rs1land.at[j], to=PT, **k)
            if i == 1:
                return rcopy(sumsl(j, cx, lo), rs2x.at[j, 0], to=X, **k)
            if i == 2:
                return rcopy(sumsl(j, cd, lo), rs2x.at[j, 1], to=X, **k)
            if i == 3:
                return rcopy(sumsl(j, cy, hi), rs2y.at[j, 0], to=Y, **k)
            if i == 4:
                return rcopy(sumsl(j, cd, hi), rs2y.at[j, 1], to=Y, **k)
            if i == 5:
                return rcopy(sumsl(j, cy, lo), rs3a.at[j], to=Y, **k)
            return rcopy(sumsl(j, cx, hi), rs3b.at[j], to=X, **k)

        def load_b(j, half):
            pos = ((1 - s) if half == 0 else s) * 4
            return pltpu.make_async_copy(bland.at[pl.ds(pl.multiple_of(j * C + pos * R, R4), R4), :], bt.at[half],
                                         bsem.at[half])

        def compute(j):
            for half in range(2):
                load_b(j, half).wait()
                if half == 0:
                    @pl.when(j >= 1)
                    def _():
                        rs_copy(j - 1, 0).wait_send()

                @pl.loop(0, us.shape[1] // 256)
                def _(n):
                    col = pl.ds(pl.multiple_of(n * 256, 256), 256)
                    g = jnp.dot(bt[half], wg[:, col], preferred_element_type=F32)
                    u = jnp.dot(bt[half], wu[:, col], preferred_element_type=F32)
                    us[:, col] = (g * jax.nn.sigmoid(g) * u).astype(BF)

                @pl.loop(0, D // 512)
                def _(n):
                    col = pl.ds(pl.multiple_of(n * 512, 512), 512)
                    pb[half, :, col] = jnp.dot(us[...], wd[:, col], preferred_element_type=F32).astype(BF)

                if half == 0:
                    rs_copy(j, 0).start()

            rs_copy(j, 0).wait_recv()
            cp = pltpu.make_async_copy(rs1land.at[j], rt, bsem.at[2])
            cp.start()
            cp.wait()

            @pl.when(j >= 2)
            def _():
                for i in range(1, 7):
                    rs_copy(j - 2, i).wait_send()

            def add(sl):
                sums[j % 2, sl, :] = (pb[1, sl, :].astype(F32) + rt[sl, :].astype(F32)).astype(BF)

            ew(R4, add)
            for i in (1, 3, 2, 4):
                rs_copy(j, i).start()

        def rs3(j):
            for i in (1, 3, 2, 4):
                rs_copy(j, i).wait_recv()

            def addy(sl):
                b = pl.ds(pl.multiple_of(cy * R + sl.start, 16), 16)
                sums[j % 2, b, lo] = (sums[j % 2, b, lo].astype(F32) + rs2x[j, 1, sl, :].astype(F32)).astype(BF)
                b = pl.ds(pl.multiple_of(cx * R + sl.start, 16), 16)
                sums[j % 2, b, hi] = (sums[j % 2, b, hi].astype(F32) + rs2y[j, 1, sl, :].astype(F32)).astype(BF)

            ew(R, addy)
            rs_copy(j, 5).start()
            rs_copy(j, 6).start()

        def final(j):
            rs_copy(j, 5).wait_recv()
            rs_copy(j, 6).wait_recv()
            for i in range(3):
                g_copy(*gb, j, i).wait_send()

            def fin(sl):
                b = pl.ds(pl.multiple_of(c * R + sl.start, 16), 16)
                o = pl.ds(pl.multiple_of(j * R + sl.start, 16), 16)
                for col, r2, r3 in ((lo, rs2x, rs3a), (hi, rs2y, rs3b)):
                    t = (sums[j % 2, b, col].astype(F32) + r2[j, 0, sl, :].astype(F32)) + r3[j, sl, :].astype(F32)
                    own[o, col] = (hk[o, col].astype(F32) + t).astype(BF)

            ew(R, fin)
            g_own(*gy, j, 1)

        for j in range(J):
            x_in(j).start()
        oproj(0)
        g_own(*gb, 0, 0)
        for cp in wcp:
            cp.wait()
        oproj(1)
        g_fwd(*gb, 0)
        g_own(*gb, 1, 0)

        @pl.loop(0, J + 4)
        def _(t):
            @pl.when(t < J)
            def _():
                g_fwd2(*gb, t)

            @pl.when(t + 1 < J)
            def _():
                g_fwd(*gb, t + 1)

            @pl.when(t >= 4)
            def _():
                g_fwd2(*gy, t - 4)

            @pl.when(jnp.logical_and(t >= 3, t < J + 3))
            def _():
                g_fwd(*gy, t - 3)

            @pl.when(t + 2 < J)
            def _():
                g_own(*gb, t + 2, 0)

            @pl.when(t < J)
            def _():
                g_finish(*gb, t)
                g_local(bland, t, 0).wait()
                for half in range(2):
                    load_b(t, half).start()

            @pl.when(jnp.logical_and(t >= 2, t < J + 2))
            def _():
                final(t - 2)

            @pl.when(t < J)
            def _():
                compute(t)

            @pl.when(jnp.logical_and(t >= 1, t < J + 1))
            def _():
                rs3(t - 1)

        rs_copy(J - 1, 0).wait_send()
        for j in range(max(J - 2, 0), J):
            for i in range(1, 7):
                rs_copy(j, i).wait_send()

    pl.run_scoped(mlp, pltpu.VMEM((2, R4, D), BF), pltpu.VMEM((R4, wg.shape[1]), BF), pltpu.VMEM((2, R4, D), BF),
                  pltpu.VMEM((R4, D), BF), pltpu.VMEM((2, R4, D), BF), pltpu.VMEM((J * R // 2, 8 * hq), BF),
                  pltpu.VMEM((2, 8 * hq, min(512, D)), BF), pltpu.SemaphoreType.DMA((3,)),
                  pltpu.SemaphoreType.DMA((1 + J,)), pltpu.SemaphoreType.DMA((2,)))

    @pl.loop(0, J)
    def _(j):
        g_finish(*gy, j)
        for i in range(3, 9):
            g_copy(*gb, j, i).wait_send()
        for i in range(9):
            g_copy(*gy, j, i).wait_send()
        g_local(y_ref, j, 1).wait()


def _tables(pos):
    half = HEAD // 2
    inv = ROPE_BASE ** (-2.0 * jnp.arange(half, dtype=F32) / HEAD)
    t = pos.shape[0]
    p = pos.astype(F32)
    lane = lax.broadcasted_iota(jnp.int32, (t // 2, HEAD), 1)
    pp = jnp.where(lane < half, p[:t // 2, None], p[t // 2:, None])
    ang = pp * jnp.concatenate([inv, inv])[None, :]
    return jnp.cos(ang), jnp.sin(ang)


def solution(mesh):
    def local(x, pos, g1, g2, wq, wk, wv, wo, wg, wu, wd):
        t, d = x.shape
        hq = wq.shape[1]
        ff = wg.shape[1]
        cs, sn = _tables(pos)
        J = NCHUNK
        R = t // 8 // J
        QB = min(512, 8 * R)
        dma = pltpu.SemaphoreType.DMA
        vm = pl.BlockSpec(memory_space=pltpu.VMEM)
        big = lambda *sh: jax.ShapeDtypeStruct(sh, BF)
        y, k, v, *_ = pl.pallas_call(
            functools.partial(_big_kernel, J, R, QB),
            in_specs=[ANY, vm, vm] + [ANY] * 9,
            out_specs=[ANY] * 7,
            out_shape=[big(t, d), big(t, HEAD), big(t, HEAD), big(J * R, 8 * hq), big(t, d), big(J, 4 * R, d),
                       big(8 * hq, d)],
            scratch_shapes=[pltpu.VMEM((d, ff), BF), pltpu.VMEM((d, ff), BF), pltpu.VMEM((ff, d), BF),
                            pltpu.VMEM((J, 2, R, d // 2), BF), pltpu.VMEM((J, 2, R, d // 2), BF),
                            pltpu.VMEM((J, R, d // 2), BF), pltpu.VMEM((J, R, d // 2), BF),
                            pltpu.VMEM((J * R, d), BF), pltpu.VMEM((J * R, d), BF),
                            dma((J, 8)), dma((J, 8)), dma((J, 9)), dma((J, 9)), dma((J, 9)), dma((J, 9)),
                            dma((J, 7)), dma((J, 7)), dma((9,)), dma((9,)), dma((2, J)), dma((3,))],
            compiler_params=pltpu.CompilerParams(collective_id=0, has_side_effects=True,
                                                 vmem_limit_bytes=67043328),
            cost_estimate=pl.CostEstimate(flops=2 * t * d * ff * 4, bytes_accessed=2 * t * d * 6, transcendentals=0),
            name="layer",
        )(x, g1.reshape(1, d), g2.reshape(1, d), cs, sn, wq, wk, wv, wo, wg, wu, wd)
        cb = pl.BlockSpec((min(256, t), d), lambda i: (i, 0))
        y = pl.pallas_call(_copy_kernel, grid=(t // min(256, t),), in_specs=[cb], out_specs=cb, out_shape=big(t, d),
                           compiler_params=pltpu.CompilerParams(dimension_semantics=("arbitrary",)),
                           name="out")(y)
        return y, k.reshape(t, 1, HEAD), v.reshape(t, 1, HEAD)

    return jax.shard_map(
        local,
        mesh=mesh,
        in_specs=(P("dp", None), P("dp"), P(), P(), P(None, "tp"), P(), P(), P("tp", None),
                  P(None, "tp"), P(None, "tp"), P("tp", None)),
        out_specs=(P("dp", None), P("dp", "tp", None), P("dp", "tp", None)),
        check_vma=False,
    )
```

```python
import functools

import jax
import jax.numpy as jnp
from jax import lax
from jax.experimental import pallas as pl
from jax.experimental.pallas import tpu as pltpu
from jax.sharding import PartitionSpec as P

HEAD = 128
EPS = 1e-5
ROPE_BASE = 500000.0
LOG2E = 1.4426950408889634
NCHUNK = 8
MESH = pl.DeviceIdType.MESH
F32, BF = jnp.float32, jnp.bfloat16
ANY = pl.BlockSpec(memory_space=pl.ANY)


def _pos_of(r):
    return (r % 2) * 4 + r // 2


def _norm_rows(src, g_ref, dst, rows, step=16):
    @pl.loop(0, rows // step, unroll=2)
    def _(n):
        sl = pl.ds(pl.multiple_of(n * step, step), step)
        t = src[sl, :].astype(F32)
        inv = lax.rsqrt(jnp.mean(t * t, axis=-1, keepdims=True) + EPS)
        dst[sl, :] = (t * inv * g_ref[...].astype(F32)).astype(BF)


def _copy_kernel(nt, y, k, v, yo, ko, vo, yb, kb, vb, si, so):
    rows = y.shape[0] // nt
    ins, outs = [], []
    for i in range(nt):
        r = pl.ds(i * rows, rows)
        ins.append(pltpu.make_async_copy(y.at[r, :], yb.at[r, :], si.at[i]))
        outs.append(pltpu.make_async_copy(yb.at[r, :], yo.at[r, :], so.at[i]))
    for i, (a, b, o) in enumerate(((k, kb, ko), (v, vb, vo))):
        ins.append(pltpu.make_async_copy(a, b, si.at[nt + i]))
        outs.append(pltpu.make_async_copy(b, o, so.at[nt + i]))
    for cp in ins:
        cp.start()
    for a, b in zip(ins, outs):
        a.wait()
        b.start()
    for cp in outs:
        cp.wait()


def _big_kernel(J, R, QB, x_ref, g1_ref, g2_ref, cos_ref, sin_ref, wq_ref, wk_ref, wv_ref, wo_ref, wg_ref, wu_ref,
                wd_ref, y_ref, kout, vout, oland, bland, rs1land, woland,
                wg, wu, wd, rs2x, rs2y, rs3a, rs3b, hk, own,
                a2s, a2r, abs_, abr, ays, ayr, rss, rsr, wos, wor, lsem, wsem):
    me = lax.axis_index("tp")
    c, s = me // 2, me % 2
    T, D = x_ref.shape
    H = D // 2
    C = 8 * R
    R4 = 4 * R
    hq = wq_ref.shape[1]
    nh = hq // HEAD
    cx = c + 1 - 2 * (c % 2)
    cy = (c + 2) % 4
    cd = 3 - c
    dev = lambda chip, core: chip * 2 + core
    X, Y, DG, PT = dev(cx, s), dev(cy, s), dev(cd, s), dev(c, 1 - s)
    mypos = s * 4 + c
    px, py, pd = s * 4 + cx, s * 4 + cy, s * 4 + cd

    z = lax.axis_index("dp")

    def rcopy(src, dst, ss, rs, to):
        where = {"dp": 1 - z, "tp": me} if to is None else {"tp": to}
        return pltpu.make_async_remote_copy(src_ref=src, dst_ref=dst, send_sem=ss, recv_sem=rs,
                                            device_id=where, device_id_type=MESH)

    wcp = [pltpu.make_async_copy(wg_ref, wg, wsem.at[0]), pltpu.make_async_copy(wu_ref, wu, wsem.at[1]),
           pltpu.make_async_copy(wd_ref, wd, wsem.at[2])]

    bar = pltpu.get_barrier_semaphore()
    for m in range(1, 8):
        pl.semaphore_signal(bar, inc=1, device_id={"tp": (me + m) % 8}, device_id_type=MESH)
    pl.semaphore_signal(bar, inc=1, device_id={"dp": 1 - z, "tp": me}, device_id_type=MESH)
    pl.semaphore_wait(bar, 8)

    WB = hq // 3
    zr, ob, lr = z * 2 * WB, WB, (1 - z) * 2 * WB

    def worows(d, off=0, n=WB):
        return woland.at[pl.ds(pl.multiple_of(d * hq + off, WB), n), :]

    def wo_copy(i):
        k = dict(ss=wos.at[i], rs=wor.at[i])
        if i < 4:
            off = (zr, ob)[i // 2]
            return rcopy(wo_ref.at[pl.ds(pl.multiple_of(off, WB), WB), :], worows(me, off), to=(X, Y)[i % 2], **k)
        if i == 4:
            return rcopy(wo_ref, worows(me, 0, hq), to=PT, **k)
        d, off, to = ((X, zr, Y), (Y, ob, X), (X, zr, None), (Y, zr, None), (DG, zr, None), (X, zr, PT), (Y, zr, PT),
                      (X, ob, PT), (Y, ob, PT), (DG, zr, PT), (DG, ob, PT), (X, lr, PT), (Y, lr, PT),
                      (DG, lr, PT))[i - 5]
        return rcopy(worows(d, off), worows(d, off), to=to, **k)

    def wo_recv(i):
        x1, y1, d1 = dev(cx, 1 - s), dev(cy, 1 - s), dev(cd, 1 - s)
        d = worows(*((X, zr), (Y, zr), (X, ob), (Y, ob), (PT, 0, hq), (DG, zr), (DG, ob), (X, lr), (Y, lr), (DG, lr),
                     (x1, zr), (y1, zr), (x1, ob), (y1, ob), (d1, zr), (d1, ob), (x1, lr), (y1, lr), (d1, lr))[i])
        rcopy(d, d, wos.at[i], wor.at[i], PT).wait_recv()

    def wo_step(recvs, sends):
        for n in recvs:
            wo_recv(n)
        for n in sends:
            wo_copy(n).start()

    wo_in = pltpu.make_async_copy(wo_ref, hk.at[pl.ds(0, hq), :], lsem.at[0, 0])
    wo_out = pltpu.make_async_copy(hk.at[pl.ds(0, hq), :], worows(me, 0, hq), lsem.at[0, 0])

    def peer(m):
        return (me + m) % 8

    def frm(m):
        return (me + 8 - m) % 8

    def a2a(j, m, o):
        to = peer(m)
        return rcopy(o.at[pl.ds(pl.multiple_of(j * C + _pos_of(to) * R, R), R), :],
                     oland.at[pl.ds(pl.multiple_of(j * R, R), R), pl.ds(pl.multiple_of(me * hq, HEAD), hq)],
                     a2s.at[j, m], a2r.at[j, m], to)

    def a2a_land(j, m):
        return oland.at[pl.ds(pl.multiple_of(j * R, R), R), pl.ds(pl.multiple_of(frm(m) * hq, HEAD), hq)]

    def a2a_own(j, o):
        return pltpu.make_async_copy(o.at[pl.ds(pl.multiple_of(j * C + mypos * R, R), R), :], a2a_land(j, 0),
                                     a2s.at[j, 0])

    TM = min(512, T // 2)

    def qkv(q, k, v, vt):
        def run(w, xt, ct, st, tsem, msem):
            nb = T // TM
            col = pl.ds(pl.multiple_of(me * HEAD, HEAD), HEAD)
            cps = [pltpu.make_async_copy(wq_ref, w.at[:, pl.ds(0, hq)], msem.at[0]),
                   pltpu.make_async_copy(wk_ref.at[:, col], w.at[:, pl.ds(hq, HEAD)], msem.at[1]),
                   pltpu.make_async_copy(wv_ref.at[:, col], w.at[:, pl.ds(hq + HEAD, HEAD)], msem.at[2])]

            def tile(i, slot):
                r = pl.ds(pl.multiple_of(i * TM, TM), TM)
                t = pl.ds(pl.multiple_of((i % (nb // 2)) * TM, TM), TM)
                return [pltpu.make_async_copy(x_ref.at[r, :], xt.at[slot], tsem.at[slot, 0]),
                        pltpu.make_async_copy(cos_ref.at[t, :], ct.at[slot], tsem.at[slot, 1]),
                        pltpu.make_async_copy(sin_ref.at[t, :], st.at[slot], tsem.at[slot, 2])]

            for cp in tile(0, 0) + cps:
                cp.start()
            wo_step((), range(5))
            wo_in.start()

            @pl.loop(0, nb)
            def _(i):
                slot = i % 2

                @pl.when(i + 1 < nb)
                def _():
                    for cp in tile(i + 1, 1 - slot):
                        cp.start()

                for cp in tile(i, slot):
                    cp.wait()
                _norm_rows(xt.at[slot], g1_ref, xt.at[slot], TM)

                @pl.when(i == 0)
                def _():
                    for cp in cps:
                        cp.wait()

                row = pl.ds(pl.multiple_of(i * TM, TM), TM)
                low = lax.broadcasted_iota(jnp.int32, (TM, HEAD), 1) < HEAD // 2
                keep = jnp.logical_xor(low, i >= nb // 2)
                cb, sb = ct[slot], st[slot]
                cc = jnp.where(keep, cb, pltpu.roll(cb, HEAD // 2, 1))
                ss = jnp.where(keep, sb, pltpu.roll(sb, HEAD // 2, 1))
                ss = jnp.where(low, -ss, ss)
                z = jnp.dot(xt[slot], w[...], preferred_element_type=F32)
                for h in range(nh + 1):
                    t = z[:, h * HEAD:(h + 1) * HEAD]
                    t = (t * cc + pltpu.roll(t, HEAD // 2, 1) * ss).astype(BF)
                    if h < nh:
                        q[row, h * HEAD:(h + 1) * HEAD] = t
                    else:
                        k[row, :] = t
                zv = z[:, hq + HEAD:]
                v[row, :] = zv.astype(BF)
                vt[:, row] = zv.T.astype(BF)

                @pl.when(i == nb // 2)
                def _():
                    wo_step((0, 1), (7, 8, 5, 10, 11))

        pl.run_scoped(run, pltpu.VMEM((D, hq + 2 * HEAD), BF), pltpu.VMEM((2, TM, D), BF),
                      pltpu.VMEM((2, TM, HEAD), F32), pltpu.VMEM((2, TM, HEAD), F32),
                      pltpu.SemaphoreType.DMA((2, 3)), pltpu.SemaphoreType.DMA((3,)))

    def attention(q, k, v, vt, acc, mm, ll, mx, sb, asem):
        qkv(q, k, v, vt)
        kv_out = [pltpu.make_async_copy(k, kout, asem.at[0]), pltpu.make_async_copy(v, vout, asem.at[1])]
        for cp in kv_out + wcp:
            cp.start()
        wo_in.wait()
        wo_out.start()
        wo_step((2, 3), (6, 12, 13))
        sc = (HEAD ** -0.5) * LOG2E
        nq = T // QB
        ki = lax.broadcasted_iota(jnp.int32, (QB, QB), 0)
        qi = lax.broadcasted_iota(jnp.int32, (QB, QB), 1)

        @pl.loop(0, nq)
        def _(i):
            row = pl.ds(pl.multiple_of(i * QB, QB), QB)

            def qk(kb, h, masked=False):
                kk = k[pl.ds(pl.multiple_of(kb * QB, QB), QB), :]
                t = lax.dot_general(kk, q[row, h * HEAD:(h + 1) * HEAD], (((1,), (1,)), ((), ())),
                                    preferred_element_type=F32)
                if masked:
                    t = jnp.where(ki <= qi, t, -jnp.inf)
                sb[h] = t
                mx[h] = jnp.max(t, axis=0, keepdims=True)

            def soft(kb, h):
                mo = mm[h]
                mn = jnp.maximum(mo, mx[h])
                mm[h] = mn
                al = jnp.exp2((mo - mn) * sc)
                p = jnp.exp2((sb[h] - mn) * sc)
                ll[h] = ll[h] * al + jnp.sum(p, axis=0, keepdims=True)
                acc[h] = acc[h] * al + jnp.dot(vt[:, pl.ds(pl.multiple_of(kb * QB, QB), QB)], p.astype(BF),
                                               preferred_element_type=F32)

            acc[...] = jnp.zeros_like(acc)
            ll[...] = jnp.zeros_like(ll)
            mm[...] = jnp.full_like(mm, -jnp.inf)

            def phases(kb, nxt, masked):
                for h in range(nh):
                    ahead = h + nh - 1
                    if ahead < nh:
                        qk(kb, ahead, masked)
                    else:
                        qk(nxt, ahead - nh)
                    soft(kb, h)

            for h in range(nh - 1):
                qk(i, h, True)
            phases(i, 0, True)

            @pl.loop(0, i)
            def _(kb):
                phases(kb, kb + 1, False)

            for h in range(nh):
                q[row, h * HEAD:(h + 1) * HEAD] = (acc[h] / ll[h]).T.astype(BF)

            def send_o(j):
                for m in range(1, 8):
                    a2a(j, m, q).start()
                a2a_own(j, q).start()

            if C < QB:
                for jj in range(QB // C):
                    send_o(i * (QB // C) + jj)
            else:
                per = C // QB

                @pl.when(i % per == per - 1)
                def _():
                    send_o(i // per)

            @pl.when(i == nq * 3 // 4 - 1)
            def _():
                wo_step((5, 7, 8), (9, 14, 16, 17))

        wo_step((6, 9), (15, 18))
        for cp in kv_out:
            cp.wait()

        @pl.loop(0, J)
        def _(j):
            a2a_own(j, q).wait()
            for m in range(1, 8):
                a2a(j, m, q).wait_send()

    pl.run_scoped(attention, pltpu.VMEM((T, hq), BF), pltpu.VMEM((T, HEAD), BF), pltpu.VMEM((T, HEAD), BF),
                  pltpu.VMEM((HEAD, T), BF), pltpu.VMEM((nh, HEAD, QB), F32),
                  pltpu.VMEM((nh, 1, QB), F32), pltpu.VMEM((nh, 1, QB), F32), pltpu.VMEM((nh, 1, QB), F32),
                  pltpu.VMEM((nh, QB, QB), F32), pltpu.SemaphoreType.DMA((2,)))
    wo_out.wait()
    wo_step((4,) + tuple(range(10, 19)), ())
    for n in range(19):
        wo_copy(n).wait_send()

    R2 = R // 2

    def rows(land, j, pos, off=0, n=R):
        return land.at[pl.ds(pl.multiple_of(j * C + pos * R + off, R2), n), :]

    def ownrows(j):
        return own.at[pl.ds(pl.multiple_of(j * R, R), R), :]

    def g_copy(land, ss, rs, j, i):
        k = dict(ss=ss.at[j, i], rs=rs.at[j, i])
        if i < 3:
            return rcopy(ownrows(j), rows(land, j, mypos), to=(X, Y, PT)[i], **k)
        if i == 3:
            return rcopy(rows(land, j, px, 0, R2), rows(land, j, px, 0, R2), to=Y, **k)
        if i == 4:
            return rcopy(rows(land, j, py, R2, R2), rows(land, j, py, R2, R2), to=X, **k)
        if i == 5:
            return rcopy(rows(land, j, px), rows(land, j, px), to=PT, **k)
        if i == 6:
            return rcopy(rows(land, j, py), rows(land, j, py), to=PT, **k)
        off = 0 if i == 7 else R2
        return rcopy(rows(land, j, pd, off, R2), rows(land, j, pd, off, R2), to=PT, **k)

    def g_recv(land, ss, rs, j, i):
        o4 = (1 - s) * 4
        src = [(px, 0, R), (py, 0, R), (o4 + c, 0, R), (pd, 0, R2), (pd, R2, R2), (o4 + cx, 0, R), (o4 + cy, 0, R),
               (o4 + cd, 0, R2), (o4 + cd, R2, R2)][i]
        d = rows(land, j, *src)
        rcopy(d, d, ss.at[j, i], rs.at[j, i], PT).wait_recv()

    def g_local(land, j, kind):
        return pltpu.make_async_copy(ownrows(j), rows(land, j, mypos), lsem.at[kind, j])

    def g_own(land, ss, rs, j, kind):
        for i in range(3):
            g_copy(land, ss, rs, j, i).start()
        g_local(land, j, kind).start()

    def g_fwd(land, ss, rs, j):
        g_recv(land, ss, rs, j, 0)
        g_copy(land, ss, rs, j, 3).start()
        g_recv(land, ss, rs, j, 1)
        g_copy(land, ss, rs, j, 4).start()
        g_copy(land, ss, rs, j, 5).start()
        g_copy(land, ss, rs, j, 6).start()

    def g_fwd2(land, ss, rs, j):
        for i in (3, 4):
            g_recv(land, ss, rs, j, i)
            g_copy(land, ss, rs, j, i + 4).start()

    def g_finish(land, ss, rs, j):
        for i in (2, 5, 6, 7, 8):
            g_recv(land, ss, rs, j, i)

    gb = (bland, abs_, abr)
    gy = (y_ref, ays, ayr)

    def ew(n, f):
        @pl.loop(0, n // 16)
        def _(i):
            f(pl.ds(pl.multiple_of(i * 16, 16), 16))

    def mlp(bt, us, pb, rt, sums, oo, wt, bsem, osem, tsem):
        NT = wt.shape[2]
        JH = J // 2
        RH = JH * R

        def x_in(j):
            return pltpu.make_async_copy(x_ref.at[pl.ds(pl.multiple_of(j * C + mypos * R, R), R), :],
                                         hk.at[pl.ds(pl.multiple_of(j * R, R), R), :], osem.at[1 + j])

        def oproj(half):
            part = pl.ds(half * RH, RH)

            def tile(n, slot):
                return pltpu.make_async_copy(woland.at[:, pl.ds(pl.multiple_of(n * NT, NT), NT)], wt.at[slot],
                                             tsem.at[slot])

            tile(0, 0).start()

            @pl.loop(half * JH, (half + 1) * JH)
            def _(j):
                for m in range(1, 8):
                    d = a2a_land(j, m)
                    rcopy(d, d, a2s.at[j, m], a2r.at[j, m], PT).wait_recv()

            cp = pltpu.make_async_copy(oland.at[part, :], oo, osem.at[0])
            cp.start()
            cp.wait()
            for j in range(half * JH, (half + 1) * JH):
                x_in(j).wait()
            nt = D // NT

            @pl.loop(0, nt)
            def _(n):
                slot = n % 2

                @pl.when(n + 1 < nt)
                def _():
                    tile(n + 1, 1 - slot).start()

                tile(n, slot).wait()
                col = pl.ds(pl.multiple_of(n * NT, NT), NT)
                hk[part, col] = (hk[part, col].astype(F32)
                                 + jnp.dot(oo[...], wt[slot], preferred_element_type=F32)).astype(BF)

            _norm_rows(hk.at[part, :], g2_ref, own.at[part, :], RH)

        def sumsl(j, chip, col):
            return sums.at[j % 2, pl.ds(pl.multiple_of(chip * R, R), R), col]

        lo, hi = pl.ds(0, H), pl.ds(H, H)

        def rs_copy(j, i):
            k = dict(ss=rss.at[j, i], rs=rsr.at[j, i])
            if i == 0:
                return rcopy(pb.at[0], rs1land.at[j], to=PT, **k)
            if i == 1:
                return rcopy(sumsl(j, cx, lo), rs2x.at[j, 0], to=X, **k)
            if i == 2:
                return rcopy(sumsl(j, cd, lo), rs2x.at[j, 1], to=X, **k)
            if i == 3:
                return rcopy(sumsl(j, cy, hi), rs2y.at[j, 0], to=Y, **k)
            if i == 4:
                return rcopy(sumsl(j, cd, hi), rs2y.at[j, 1], to=Y, **k)
            if i == 5:
                return rcopy(sumsl(j, cy, lo), rs3a.at[j], to=Y, **k)
            return rcopy(sumsl(j, cx, hi), rs3b.at[j], to=X, **k)

        def load_b(j, half):
            pos = ((1 - s) if half == 0 else s) * 4
            return pltpu.make_async_copy(bland.at[pl.ds(pl.multiple_of(j * C + pos * R, R4), R4), :], bt.at[half],
                                         bsem.at[half])

        def compute(j):
            for half in range(2):
                load_b(j, half).wait()
                if half == 0:
                    @pl.when(j >= 1)
                    def _():
                        rs_copy(j - 1, 0).wait_send()

                @pl.loop(0, us.shape[1] // 256)
                def _(n):
                    col = pl.ds(pl.multiple_of(n * 256, 256), 256)
                    g = jnp.dot(bt[half], wg[:, col], preferred_element_type=F32)
                    u = jnp.dot(bt[half], wu[:, col], preferred_element_type=F32)
                    us[:, col] = (g * jax.nn.sigmoid(g) * u).astype(BF)

                @pl.loop(0, D // 512)
                def _(n):
                    col = pl.ds(pl.multiple_of(n * 512, 512), 512)
                    pb[half, :, col] = jnp.dot(us[...], wd[:, col], preferred_element_type=F32).astype(BF)

                if half == 0:
                    rs_copy(j, 0).start()

            rs_copy(j, 0).wait_recv()
            cp = pltpu.make_async_copy(rs1land.at[j], rt, bsem.at[2])
            cp.start()
            cp.wait()

            @pl.when(j >= 2)
            def _():
                for i in range(1, 7):
                    rs_copy(j - 2, i).wait_send()

            def add(sl):
                sums[j % 2, sl, :] = (pb[1, sl, :].astype(F32) + rt[sl, :].astype(F32)).astype(BF)

            ew(R4, add)
            for i in (1, 3, 2, 4):
                rs_copy(j, i).start()

        def rs3(j):
            for i in (1, 3, 2, 4):
                rs_copy(j, i).wait_recv()

            def addy(sl):
                b = pl.ds(pl.multiple_of(cy * R + sl.start, 16), 16)
                sums[j % 2, b, lo] = (sums[j % 2, b, lo].astype(F32) + rs2x[j, 1, sl, :].astype(F32)).astype(BF)
                b = pl.ds(pl.multiple_of(cx * R + sl.start, 16), 16)
                sums[j % 2, b, hi] = (sums[j % 2, b, hi].astype(F32) + rs2y[j, 1, sl, :].astype(F32)).astype(BF)

            ew(R, addy)
            rs_copy(j, 5).start()
            rs_copy(j, 6).start()

        def final(j):
            rs_copy(j, 5).wait_recv()
            rs_copy(j, 6).wait_recv()
            for i in range(3):
                g_copy(*gb, j, i).wait_send()

            def fin(sl):
                b = pl.ds(pl.multiple_of(c * R + sl.start, 16), 16)
                o = pl.ds(pl.multiple_of(j * R + sl.start, 16), 16)
                for col, r2, r3 in ((lo, rs2x, rs3a), (hi, rs2y, rs3b)):
                    t = (sums[j % 2, b, col].astype(F32) + r2[j, 0, sl, :].astype(F32)) + r3[j, sl, :].astype(F32)
                    own[o, col] = (hk[o, col].astype(F32) + t).astype(BF)

            ew(R, fin)
            g_own(*gy, j, 1)

        for j in range(J):
            x_in(j).start()
        oproj(0)
        g_own(*gb, 0, 0)
        for cp in wcp:
            cp.wait()
        oproj(1)
        g_fwd(*gb, 0)
        g_own(*gb, 1, 0)

        @pl.loop(0, J + 4)
        def _(t):
            @pl.when(t < J)
            def _():
                g_fwd2(*gb, t)

            @pl.when(t + 1 < J)
            def _():
                g_fwd(*gb, t + 1)

            @pl.when(t >= 4)
            def _():
                g_fwd2(*gy, t - 4)

            @pl.when(jnp.logical_and(t >= 3, t < J + 3))
            def _():
                g_fwd(*gy, t - 3)

            @pl.when(t + 2 < J)
            def _():
                g_own(*gb, t + 2, 0)

            @pl.when(t < J)
            def _():
                g_finish(*gb, t)
                g_local(bland, t, 0).wait()
                for half in range(2):
                    load_b(t, half).start()

            @pl.when(jnp.logical_and(t >= 2, t < J + 2))
            def _():
                final(t - 2)

            @pl.when(t < J)
            def _():
                compute(t)

            @pl.when(jnp.logical_and(t >= 1, t < J + 1))
            def _():
                rs3(t - 1)

        rs_copy(J - 1, 0).wait_send()
        for j in range(max(J - 2, 0), J):
            for i in range(1, 7):
                rs_copy(j, i).wait_send()

    pl.run_scoped(mlp, pltpu.VMEM((2, R4, D), BF), pltpu.VMEM((R4, wg.shape[1]), BF), pltpu.VMEM((2, R4, D), BF),
                  pltpu.VMEM((R4, D), BF), pltpu.VMEM((2, R4, D), BF), pltpu.VMEM((J * R // 2, 8 * hq), BF),
                  pltpu.VMEM((2, 8 * hq, min(512, D)), BF), pltpu.SemaphoreType.DMA((3,)),
                  pltpu.SemaphoreType.DMA((1 + J,)), pltpu.SemaphoreType.DMA((2,)))

    @pl.loop(0, J)
    def _(j):
        g_finish(*gy, j)
        for i in range(3, 9):
            g_copy(*gb, j, i).wait_send()
        for i in range(9):
            g_copy(*gy, j, i).wait_send()
        g_local(y_ref, j, 1).wait()


def _tables(pos):
    half = HEAD // 2
    inv = ROPE_BASE ** (-2.0 * jnp.arange(half, dtype=F32) / HEAD)
    t = pos.shape[0]
    p = pos.astype(F32)
    lane = lax.broadcasted_iota(jnp.int32, (t // 2, HEAD), 1)
    pp = jnp.where(lane < half, p[:t // 2, None], p[t // 2:, None])
    ang = pp * jnp.concatenate([inv, inv])[None, :]
    return jnp.cos(ang), jnp.sin(ang)


def solution(mesh):
    def local(x, pos, g1, g2, wq, wk, wv, wo, wg, wu, wd):
        t, d = x.shape
        hq = wq.shape[1]
        ff = wg.shape[1]
        cs, sn = _tables(pos)
        J = NCHUNK
        R = t // 8 // J
        QB = min(512, 8 * R)
        dma = pltpu.SemaphoreType.DMA
        vm = pl.BlockSpec(memory_space=pltpu.VMEM)
        big = lambda *sh: jax.ShapeDtypeStruct(sh, BF)
        y, k, v, *_ = pl.pallas_call(
            functools.partial(_big_kernel, J, R, QB),
            in_specs=[ANY, vm, vm] + [ANY] * 9,
            out_specs=[ANY] * 7,
            out_shape=[big(t, d), big(t, HEAD), big(t, HEAD), big(J * R, 8 * hq), big(t, d), big(J, 4 * R, d),
                       big(8 * hq, d)],
            scratch_shapes=[pltpu.VMEM((d, ff), BF), pltpu.VMEM((d, ff), BF), pltpu.VMEM((ff, d), BF),
                            pltpu.VMEM((J, 2, R, d // 2), BF), pltpu.VMEM((J, 2, R, d // 2), BF),
                            pltpu.VMEM((J, R, d // 2), BF), pltpu.VMEM((J, R, d // 2), BF),
                            pltpu.VMEM((J * R, d), BF), pltpu.VMEM((J * R, d), BF),
                            dma((J, 8)), dma((J, 8)), dma((J, 9)), dma((J, 9)), dma((J, 9)), dma((J, 9)),
                            dma((J, 7)), dma((J, 7)), dma((19,)), dma((19,)), dma((2, J)), dma((3,))],
            compiler_params=pltpu.CompilerParams(collective_id=0, has_side_effects=True,
                                                 vmem_limit_bytes=67043328),
            cost_estimate=pl.CostEstimate(flops=2 * t * d * ff * 4, bytes_accessed=2 * t * d * 6, transcendentals=0),
            name="layer",
        )(x, g1.reshape(1, d), g2.reshape(1, d), cs, sn, wq, wk, wv, wo, wg, wu, wd)
        nt = 16
        y, k, v = pl.pallas_call(
            functools.partial(_copy_kernel, nt), in_specs=[ANY] * 3, out_specs=[ANY] * 3,
            out_shape=[big(t, d), big(t, HEAD), big(t, HEAD)],
            scratch_shapes=[pltpu.VMEM((t, d), BF), pltpu.VMEM((t, HEAD), BF), pltpu.VMEM((t, HEAD), BF),
                            dma((nt + 2,)), dma((nt + 2,))],
            compiler_params=pltpu.CompilerParams(vmem_limit_bytes=32 << 20), name="out")(y, k, v)
        return y, k.reshape(t, 1, HEAD), v.reshape(t, 1, HEAD)

    return jax.shard_map(
        local,
        mesh=mesh,
        in_specs=(P("dp", None), P("dp"), P(), P(), P(None, "tp"), P(), P(), P("tp", None),
                  P(None, "tp"), P(None, "tp"), P("tp", None)),
        out_specs=(P("dp", None), P("dp", "tp", None), P("dp", "tp", None)),
        check_vma=False,
    )
```

```python
import functools

import jax
import jax.numpy as jnp
from jax import lax
from jax.experimental import pallas as pl
from jax.experimental.pallas import tpu as pltpu
from jax.sharding import PartitionSpec as P

HEAD = 128
EPS = 1e-5
ROPE_BASE = 500000.0
LOG2E = 1.4426950408889634
NCHUNK = 8
MESH = pl.DeviceIdType.MESH
F32, BF = jnp.float32, jnp.bfloat16
ANY = pl.BlockSpec(memory_space=pl.ANY)


def _pos_of(r):
    return (r % 2) * 4 + r // 2


def _norm_rows(src, g_ref, dst, rows, step=16):
    @pl.loop(0, rows // step, unroll=2)
    def _(n):
        sl = pl.ds(pl.multiple_of(n * step, step), step)
        t = src[sl, :].astype(F32)
        inv = lax.rsqrt(jnp.mean(t * t, axis=-1, keepdims=True) + EPS)
        dst[sl, :] = (t * inv * g_ref[...].astype(F32)).astype(BF)


def _copy_kernel(nt, y, k, v, yo, ko, vo, yb, kb, vb, si, so):
    rows = y.shape[0] // nt
    ins, outs = [], []
    for i in range(nt):
        r = pl.ds(i * rows, rows)
        ins.append(pltpu.make_async_copy(y.at[r, :], yb.at[r, :], si.at[i]))
        outs.append(pltpu.make_async_copy(yb.at[r, :], yo.at[r, :], so.at[i]))
    for i, (a, b, o) in enumerate(((k, kb, ko), (v, vb, vo))):
        ins.append(pltpu.make_async_copy(a, b, si.at[nt + i]))
        outs.append(pltpu.make_async_copy(b, o, so.at[nt + i]))
    for cp in ins:
        cp.start()
    for a, b in zip(ins, outs):
        a.wait()
        b.start()
    for cp in outs:
        cp.wait()


def _big_kernel(J, R, QB, x_ref, g1_ref, g2_ref, cos_ref, sin_ref, wq_ref, wk_ref, wv_ref, wo_ref, wg_ref, wu_ref,
                wd_ref, y_ref, kout, vout, oland, bland, rs1land, woland,
                wg, wu, wd, rs2x, rs2y, rs3a, rs3b, hk, own, q,
                a2s, a2r, abs_, abr, ays, ayr, rss, rsr, wos, wor, lsem, wsem):
    me = lax.axis_index("tp")
    c, s = me // 2, me % 2
    T, D = x_ref.shape
    H = D // 2
    C = 8 * R
    R4 = 4 * R
    hq = wq_ref.shape[1]
    nh = hq // HEAD
    cx = c + 1 - 2 * (c % 2)
    cy = (c + 2) % 4
    cd = 3 - c
    dev = lambda chip, core: chip * 2 + core
    X, Y, DG, PT = dev(cx, s), dev(cy, s), dev(cd, s), dev(c, 1 - s)
    mypos = s * 4 + c
    px, py, pd = s * 4 + cx, s * 4 + cy, s * 4 + cd

    z = lax.axis_index("dp")

    def rcopy(src, dst, ss, rs, to):
        where = {"dp": 1 - z, "tp": me} if to is None else {"tp": to}
        return pltpu.make_async_remote_copy(src_ref=src, dst_ref=dst, send_sem=ss, recv_sem=rs,
                                            device_id=where, device_id_type=MESH)

    wcp = [pltpu.make_async_copy(wg_ref, wg, wsem.at[0]), pltpu.make_async_copy(wu_ref, wu, wsem.at[1]),
           pltpu.make_async_copy(wd_ref, wd, wsem.at[2])]

    bar = pltpu.get_barrier_semaphore()
    for m in range(1, 8):
        pl.semaphore_signal(bar, inc=1, device_id={"tp": (me + m) % 8}, device_id_type=MESH)
    pl.semaphore_signal(bar, inc=1, device_id={"dp": 1 - z, "tp": me}, device_id_type=MESH)
    pl.semaphore_wait(bar, 8)

    WB = hq // 3
    zr, ob, lr = z * 2 * WB, WB, (1 - z) * 2 * WB

    def worows(d, off=0, n=WB):
        return woland.at[pl.ds(pl.multiple_of(d * hq + off, WB), n), :]

    def wo_copy(i):
        k = dict(ss=wos.at[i], rs=wor.at[i])
        if i < 4:
            off = (zr, ob)[i // 2]
            return rcopy(wo_ref.at[pl.ds(pl.multiple_of(off, WB), WB), :], worows(me, off), to=(X, Y)[i % 2], **k)
        if i == 4:
            return rcopy(wo_ref, worows(me, 0, hq), to=PT, **k)
        d, off, to = ((X, zr, Y), (Y, ob, X), (X, zr, None), (Y, zr, None), (DG, zr, None), (X, zr, PT), (Y, zr, PT),
                      (X, ob, PT), (Y, ob, PT), (DG, zr, PT), (DG, ob, PT), (X, lr, PT), (Y, lr, PT),
                      (DG, lr, PT))[i - 5]
        return rcopy(worows(d, off), worows(d, off), to=to, **k)

    def wo_recv(i):
        x1, y1, d1 = dev(cx, 1 - s), dev(cy, 1 - s), dev(cd, 1 - s)
        d = worows(*((X, zr), (Y, zr), (X, ob), (Y, ob), (PT, 0, hq), (DG, zr), (DG, ob), (X, lr), (Y, lr), (DG, lr),
                     (x1, zr), (y1, zr), (x1, ob), (y1, ob), (d1, zr), (d1, ob), (x1, lr), (y1, lr), (d1, lr))[i])
        rcopy(d, d, wos.at[i], wor.at[i], PT).wait_recv()

    def wo_step(recvs, sends):
        for n in recvs:
            wo_recv(n)
        for n in sends:
            wo_copy(n).start()

    wo_in = pltpu.make_async_copy(wo_ref, hk.at[pl.ds(0, hq), :], lsem.at[0, 0])
    wo_out = pltpu.make_async_copy(hk.at[pl.ds(0, hq), :], worows(me, 0, hq), lsem.at[0, 0])

    def peer(m):
        return (me + m) % 8

    def frm(m):
        return (me + 8 - m) % 8

    JH = J // 2

    def a2a(b, m):
        to = peer(m)
        return rcopy(q.at[pl.ds(b * JH, JH), _pos_of(to)],
                     oland.at[pl.ds(b * JH, JH), :, pl.ds(pl.multiple_of(me * hq, HEAD), hq)],
                     a2s.at[b, m], a2r.at[b, m], to)

    def a2a_land(b, m):
        return oland.at[pl.ds(b * JH, JH), :, pl.ds(pl.multiple_of(frm(m) * hq, HEAD), hq)]

    def a2a_own(b):
        return pltpu.make_async_copy(q.at[pl.ds(b * JH, JH), mypos], a2a_land(b, 0), a2s.at[b, 0])

    def send_o(b):
        for m in range(1, 8):
            a2a(b, m).start()
        a2a_own(b).start()

    def qblock(i, h, n):
        return (pl.ds(i * (n // C), n // C), slice(None), slice(None), pl.ds(h * HEAD, HEAD))

    TM = min(512, T // 2)

    def qkv(k, v, vt):
        def run(w, xt, ct, st, tsem, msem):
            nb = T // TM
            col = pl.ds(pl.multiple_of(me * HEAD, HEAD), HEAD)
            cps = [pltpu.make_async_copy(wq_ref, w.at[:, pl.ds(0, hq)], msem.at[0]),
                   pltpu.make_async_copy(wk_ref.at[:, col], w.at[:, pl.ds(hq, HEAD)], msem.at[1]),
                   pltpu.make_async_copy(wv_ref.at[:, col], w.at[:, pl.ds(hq + HEAD, HEAD)], msem.at[2])]

            def tile(i, slot):
                r = pl.ds(pl.multiple_of(i * TM, TM), TM)
                t = pl.ds(pl.multiple_of((i % (nb // 2)) * TM, TM), TM)
                return [pltpu.make_async_copy(x_ref.at[r, :], xt.at[slot], tsem.at[slot, 0]),
                        pltpu.make_async_copy(cos_ref.at[t, :], ct.at[slot], tsem.at[slot, 1]),
                        pltpu.make_async_copy(sin_ref.at[t, :], st.at[slot], tsem.at[slot, 2])]

            for cp in tile(0, 0) + cps:
                cp.start()
            wo_step((), range(5))
            wo_in.start()

            @pl.loop(0, nb)
            def _(i):
                slot = i % 2

                @pl.when(i + 1 < nb)
                def _():
                    for cp in tile(i + 1, 1 - slot):
                        cp.start()

                for cp in tile(i, slot):
                    cp.wait()
                _norm_rows(xt.at[slot], g1_ref, xt.at[slot], TM)

                @pl.when(i == 0)
                def _():
                    for cp in cps:
                        cp.wait()

                row = pl.ds(pl.multiple_of(i * TM, TM), TM)
                low = lax.broadcasted_iota(jnp.int32, (TM, HEAD), 1) < HEAD // 2
                keep = jnp.logical_xor(low, i >= nb // 2)
                cb, sb = ct[slot], st[slot]
                cc = jnp.where(keep, cb, pltpu.roll(cb, HEAD // 2, 1))
                ss = jnp.where(keep, sb, pltpu.roll(sb, HEAD // 2, 1))
                ss = jnp.where(low, -ss, ss)
                z = jnp.dot(xt[slot], w[...], preferred_element_type=F32)
                for h in range(nh + 1):
                    t = z[:, h * HEAD:(h + 1) * HEAD]
                    t = (t * cc + pltpu.roll(t, HEAD // 2, 1) * ss).astype(BF)
                    if h < nh:
                        q[qblock(i, h, TM)] = t.reshape(TM // C, 8, R, HEAD)
                    else:
                        k[row, :] = t
                zv = z[:, hq + HEAD:]
                v[row, :] = zv.astype(BF)
                vt[:, row] = zv.T.astype(BF)

                @pl.when(i == nb // 2)
                def _():
                    wo_step((0, 1), (7, 8, 5, 10, 11))

        pl.run_scoped(run, pltpu.VMEM((D, hq + 2 * HEAD), BF), pltpu.VMEM((2, TM, D), BF),
                      pltpu.VMEM((2, TM, HEAD), F32), pltpu.VMEM((2, TM, HEAD), F32),
                      pltpu.SemaphoreType.DMA((2, 3)), pltpu.SemaphoreType.DMA((3,)))

    def attention(k, v, vt, acc, mm, ll, mx, sb, asem):
        qkv(k, v, vt)
        kv_out = [pltpu.make_async_copy(k, kout, asem.at[0]), pltpu.make_async_copy(v, vout, asem.at[1])]
        for cp in kv_out + wcp:
            cp.start()
        wo_in.wait()
        wo_out.start()
        wo_step((2, 3), (6, 12, 13))
        sc = (HEAD ** -0.5) * LOG2E
        nq = T // QB
        ki = lax.broadcasted_iota(jnp.int32, (QB, QB), 0)
        qi = lax.broadcasted_iota(jnp.int32, (QB, QB), 1)

        @pl.loop(0, nq)
        def _(i):
            def qk(kb, h, masked=False):
                kk = k[pl.ds(pl.multiple_of(kb * QB, QB), QB), :]
                t = lax.dot_general(kk, q[qblock(i, h, QB)].reshape(QB, HEAD), (((1,), (1,)), ((), ())),
                                    preferred_element_type=F32)
                if masked:
                    t = jnp.where(ki <= qi, t, -jnp.inf)
                sb[h] = t
                mx[h] = jnp.max(t, axis=0, keepdims=True)

            def soft(kb, h):
                mo = mm[h]
                mn = jnp.maximum(mo, mx[h])
                mm[h] = mn
                al = jnp.exp2((mo - mn) * sc)
                p = jnp.exp2((sb[h] - mn) * sc)
                ll[h] = ll[h] * al + jnp.sum(p, axis=0, keepdims=True)
                acc[h] = acc[h] * al + jnp.dot(vt[:, pl.ds(pl.multiple_of(kb * QB, QB), QB)], p.astype(BF),
                                               preferred_element_type=F32)

            acc[...] = jnp.zeros_like(acc)
            ll[...] = jnp.zeros_like(ll)
            mm[...] = jnp.full_like(mm, -jnp.inf)

            def phases(kb, nxt, masked):
                for h in range(nh):
                    ahead = h + nh - 1
                    if ahead < nh:
                        qk(kb, ahead, masked)
                    else:
                        qk(nxt, ahead - nh)
                    soft(kb, h)

            for h in range(nh - 1):
                qk(i, h, True)
            phases(i, 0, True)

            @pl.loop(0, i)
            def _(kb):
                phases(kb, kb + 1, False)

            for h in range(nh):
                q[qblock(i, h, QB)] = (acc[h] / ll[h]).T.astype(BF).reshape(QB // C, 8, R, HEAD)

            @pl.when(i == nq // 2 - 1)
            def _():
                send_o(0)

            @pl.when(i == nq * 3 // 4 - 1)
            def _():
                wo_step((5, 7, 8), (9, 14, 16, 17))

        send_o(1)
        wo_step((6, 9), (15, 18))
        for cp in kv_out:
            cp.wait()

    pl.run_scoped(attention, pltpu.VMEM((T, HEAD), BF), pltpu.VMEM((T, HEAD), BF),
                  pltpu.VMEM((HEAD, T), BF), pltpu.VMEM((nh, HEAD, QB), F32),
                  pltpu.VMEM((nh, 1, QB), F32), pltpu.VMEM((nh, 1, QB), F32), pltpu.VMEM((nh, 1, QB), F32),
                  pltpu.VMEM((nh, QB, QB), F32), pltpu.SemaphoreType.DMA((2,)))
    wo_out.wait()
    wo_step((4,) + tuple(range(10, 19)), ())
    for n in range(19):
        wo_copy(n).wait_send()

    R2 = R // 2

    def rows(land, j, pos, off=0, n=R):
        return land.at[pl.ds(pl.multiple_of(j * C + pos * R + off, R2), n), :]

    def ownrows(j):
        return own.at[pl.ds(pl.multiple_of(j * R, R), R), :]

    def g_copy(land, ss, rs, j, i):
        k = dict(ss=ss.at[j, i], rs=rs.at[j, i])
        if i < 3:
            return rcopy(ownrows(j), rows(land, j, mypos), to=(X, Y, PT)[i], **k)
        if i == 3:
            return rcopy(rows(land, j, px, 0, R2), rows(land, j, px, 0, R2), to=Y, **k)
        if i == 4:
            return rcopy(rows(land, j, py, R2, R2), rows(land, j, py, R2, R2), to=X, **k)
        if i == 5:
            return rcopy(rows(land, j, px), rows(land, j, px), to=PT, **k)
        if i == 6:
            return rcopy(rows(land, j, py), rows(land, j, py), to=PT, **k)
        off = 0 if i == 7 else R2
        return rcopy(rows(land, j, pd, off, R2), rows(land, j, pd, off, R2), to=PT, **k)

    def g_recv(land, ss, rs, j, i):
        o4 = (1 - s) * 4
        src = [(px, 0, R), (py, 0, R), (o4 + c, 0, R), (pd, 0, R2), (pd, R2, R2), (o4 + cx, 0, R), (o4 + cy, 0, R),
               (o4 + cd, 0, R2), (o4 + cd, R2, R2)][i]
        d = rows(land, j, *src)
        rcopy(d, d, ss.at[j, i], rs.at[j, i], PT).wait_recv()

    def g_local(land, j, kind):
        return pltpu.make_async_copy(ownrows(j), rows(land, j, mypos), lsem.at[kind, j])

    def g_own(land, ss, rs, j, kind):
        for i in range(3):
            g_copy(land, ss, rs, j, i).start()
        g_local(land, j, kind).start()

    def g_fwd(land, ss, rs, j):
        g_recv(land, ss, rs, j, 0)
        g_copy(land, ss, rs, j, 3).start()
        g_recv(land, ss, rs, j, 1)
        g_copy(land, ss, rs, j, 4).start()
        g_copy(land, ss, rs, j, 5).start()
        g_copy(land, ss, rs, j, 6).start()

    def g_fwd2(land, ss, rs, j):
        for i in (3, 4):
            g_recv(land, ss, rs, j, i)
            g_copy(land, ss, rs, j, i + 4).start()

    def g_finish(land, ss, rs, j):
        for i in (2, 5, 6, 7, 8):
            g_recv(land, ss, rs, j, i)

    gb = (bland, abs_, abr)
    gy = (y_ref, ays, ayr)

    def ew(n, f):
        @pl.loop(0, n // 16)
        def _(i):
            f(pl.ds(pl.multiple_of(i * 16, 16), 16))

    def mlp(bt, us, pb, rt, sums, oo, wt, bsem, osem, tsem):
        NT = wt.shape[2]
        RH = JH * R

        def x_in(j):
            return pltpu.make_async_copy(x_ref.at[pl.ds(pl.multiple_of(j * C + mypos * R, R), R), :],
                                         hk.at[pl.ds(pl.multiple_of(j * R, R), R), :], osem.at[1 + j])

        def oproj(half):
            part = pl.ds(half * RH, RH)

            def tile(n, slot):
                return pltpu.make_async_copy(woland.at[:, pl.ds(pl.multiple_of(n * NT, NT), NT)], wt.at[slot],
                                             tsem.at[slot])

            tile(0, 0).start()

            for m in range(1, 8):
                d = a2a_land(half, m)
                rcopy(d, d, a2s.at[half, m], a2r.at[half, m], PT).wait_recv()
            a2a_own(half).wait()
            cp = pltpu.make_async_copy(oland.at[pl.ds(half * JH, JH)], oo, osem.at[0])
            cp.start()
            cp.wait()
            for j in range(half * JH, (half + 1) * JH):
                x_in(j).wait()
            nt = D // NT

            @pl.loop(0, nt)
            def _(n):
                slot = n % 2

                @pl.when(n + 1 < nt)
                def _():
                    tile(n + 1, 1 - slot).start()

                tile(n, slot).wait()
                col = pl.ds(pl.multiple_of(n * NT, NT), NT)
                hk[part, col] = (hk[part, col].astype(F32)
                                 + jnp.dot(oo[...].reshape(RH, 8 * hq), wt[slot], preferred_element_type=F32)).astype(BF)

            _norm_rows(hk.at[part, :], g2_ref, own.at[part, :], RH)

        def sumsl(j, chip, col):
            return sums.at[j % 2, pl.ds(pl.multiple_of(chip * R, R), R), col]

        lo, hi = pl.ds(0, H), pl.ds(H, H)

        def rs_copy(j, i):
            k = dict(ss=rss.at[j, i], rs=rsr.at[j, i])
            if i == 0:
                return rcopy(pb.at[0], rs1land.at[j], to=PT, **k)
            if i == 1:
                return rcopy(sumsl(j, cx, lo), rs2x.at[j, 0], to=X, **k)
            if i == 2:
                return rcopy(sumsl(j, cd, lo), rs2x.at[j, 1], to=X, **k)
            if i == 3:
                return rcopy(sumsl(j, cy, hi), rs2y.at[j, 0], to=Y, **k)
            if i == 4:
                return rcopy(sumsl(j, cd, hi), rs2y.at[j, 1], to=Y, **k)
            if i == 5:
                return rcopy(sumsl(j, cy, lo), rs3a.at[j], to=Y, **k)
            return rcopy(sumsl(j, cx, hi), rs3b.at[j], to=X, **k)

        def load_b(j, half):
            pos = ((1 - s) if half == 0 else s) * 4
            return pltpu.make_async_copy(bland.at[pl.ds(pl.multiple_of(j * C + pos * R, R4), R4), :], bt.at[half],
                                         bsem.at[half])

        def compute(j):
            for half in range(2):
                load_b(j, half).wait()
                if half == 0:
                    @pl.when(j >= 1)
                    def _():
                        rs_copy(j - 1, 0).wait_send()

                @pl.loop(0, us.shape[1] // 256)
                def _(n):
                    col = pl.ds(pl.multiple_of(n * 256, 256), 256)
                    g = jnp.dot(bt[half], wg[:, col], preferred_element_type=F32)
                    u = jnp.dot(bt[half], wu[:, col], preferred_element_type=F32)
                    us[:, col] = (g * jax.nn.sigmoid(g) * u).astype(BF)

                @pl.loop(0, D // 512)
                def _(n):
                    col = pl.ds(pl.multiple_of(n * 512, 512), 512)
                    pb[half, :, col] = jnp.dot(us[...], wd[:, col], preferred_element_type=F32).astype(BF)

                if half == 0:
                    rs_copy(j, 0).start()

            rs_copy(j, 0).wait_recv()
            cp = pltpu.make_async_copy(rs1land.at[j], rt, bsem.at[2])
            cp.start()
            cp.wait()

            @pl.when(j >= 2)
            def _():
                for i in range(1, 7):
                    rs_copy(j - 2, i).wait_send()

            def add(sl):
                sums[j % 2, sl, :] = (pb[1, sl, :].astype(F32) + rt[sl, :].astype(F32)).astype(BF)

            ew(R4, add)
            for i in (1, 3, 2, 4):
                rs_copy(j, i).start()

        def rs3(j):
            for i in (1, 3, 2, 4):
                rs_copy(j, i).wait_recv()

            def addy(sl):
                b = pl.ds(pl.multiple_of(cy * R + sl.start, 16), 16)
                sums[j % 2, b, lo] = (sums[j % 2, b, lo].astype(F32) + rs2x[j, 1, sl, :].astype(F32)).astype(BF)
                b = pl.ds(pl.multiple_of(cx * R + sl.start, 16), 16)
                sums[j % 2, b, hi] = (sums[j % 2, b, hi].astype(F32) + rs2y[j, 1, sl, :].astype(F32)).astype(BF)

            ew(R, addy)
            rs_copy(j, 5).start()
            rs_copy(j, 6).start()

        def final(j):
            rs_copy(j, 5).wait_recv()
            rs_copy(j, 6).wait_recv()
            for i in range(3):
                g_copy(*gb, j, i).wait_send()

            def fin(sl):
                b = pl.ds(pl.multiple_of(c * R + sl.start, 16), 16)
                o = pl.ds(pl.multiple_of(j * R + sl.start, 16), 16)
                for col, r2, r3 in ((lo, rs2x, rs3a), (hi, rs2y, rs3b)):
                    t = (sums[j % 2, b, col].astype(F32) + r2[j, 0, sl, :].astype(F32)) + r3[j, sl, :].astype(F32)
                    own[o, col] = (hk[o, col].astype(F32) + t).astype(BF)

            ew(R, fin)
            g_own(*gy, j, 1)

        for j in range(J):
            x_in(j).start()
        oproj(0)
        g_own(*gb, 0, 0)
        for cp in wcp:
            cp.wait()
        oproj(1)
        g_fwd(*gb, 0)
        g_own(*gb, 1, 0)

        @pl.loop(0, J + 4)
        def _(t):
            @pl.when(t < J)
            def _():
                g_fwd2(*gb, t)

            @pl.when(t + 1 < J)
            def _():
                g_fwd(*gb, t + 1)

            @pl.when(t >= 4)
            def _():
                g_fwd2(*gy, t - 4)

            @pl.when(jnp.logical_and(t >= 3, t < J + 3))
            def _():
                g_fwd(*gy, t - 3)

            @pl.when(t + 2 < J)
            def _():
                g_own(*gb, t + 2, 0)

            @pl.when(t < J)
            def _():
                g_finish(*gb, t)
                g_local(bland, t, 0).wait()
                for half in range(2):
                    load_b(t, half).start()

            @pl.when(jnp.logical_and(t >= 2, t < J + 2))
            def _():
                final(t - 2)

            @pl.when(t < J)
            def _():
                compute(t)

            @pl.when(jnp.logical_and(t >= 1, t < J + 1))
            def _():
                rs3(t - 1)

        for b in range(2):
            for m in range(1, 8):
                a2a(b, m).wait_send()
        rs_copy(J - 1, 0).wait_send()
        for j in range(max(J - 2, 0), J):
            for i in range(1, 7):
                rs_copy(j, i).wait_send()

    pl.run_scoped(mlp, pltpu.VMEM((2, R4, D), BF), pltpu.VMEM((R4, wg.shape[1]), BF), pltpu.VMEM((2, R4, D), BF),
                  pltpu.VMEM((R4, D), BF), pltpu.VMEM((2, R4, D), BF), pltpu.VMEM((J // 2, R, 8 * hq), BF),
                  pltpu.VMEM((2, 8 * hq, min(512, D)), BF), pltpu.SemaphoreType.DMA((3,)),
                  pltpu.SemaphoreType.DMA((1 + J,)), pltpu.SemaphoreType.DMA((2,)))

    @pl.loop(0, J)
    def _(j):
        g_finish(*gy, j)
        for i in range(3, 9):
            g_copy(*gb, j, i).wait_send()
        for i in range(9):
            g_copy(*gy, j, i).wait_send()
        g_local(y_ref, j, 1).wait()


def _tables(pos):
    half = HEAD // 2
    inv = ROPE_BASE ** (-2.0 * jnp.arange(half, dtype=F32) / HEAD)
    t = pos.shape[0]
    p = pos.astype(F32)
    lane = lax.broadcasted_iota(jnp.int32, (t // 2, HEAD), 1)
    pp = jnp.where(lane < half, p[:t // 2, None], p[t // 2:, None])
    ang = pp * jnp.concatenate([inv, inv])[None, :]
    return jnp.cos(ang), jnp.sin(ang)


def solution(mesh):
    def local(x, pos, g1, g2, wq, wk, wv, wo, wg, wu, wd):
        t, d = x.shape
        hq = wq.shape[1]
        ff = wg.shape[1]
        cs, sn = _tables(pos)
        J = NCHUNK
        R = t // 8 // J
        QB = min(512, 8 * R)
        dma = pltpu.SemaphoreType.DMA
        vm = pl.BlockSpec(memory_space=pltpu.VMEM)
        big = lambda *sh: jax.ShapeDtypeStruct(sh, BF)
        y, k, v, *_ = pl.pallas_call(
            functools.partial(_big_kernel, J, R, QB),
            in_specs=[ANY, vm, vm] + [ANY] * 9,
            out_specs=[ANY] * 7,
            out_shape=[big(t, d), big(t, HEAD), big(t, HEAD), big(J, R, 8 * hq), big(t, d), big(J, 4 * R, d),
                       big(8 * hq, d)],
            scratch_shapes=[pltpu.VMEM((d, ff), BF), pltpu.VMEM((d, ff), BF), pltpu.VMEM((ff, d), BF),
                            pltpu.VMEM((J, 2, R, d // 2), BF), pltpu.VMEM((J, 2, R, d // 2), BF),
                            pltpu.VMEM((J, R, d // 2), BF), pltpu.VMEM((J, R, d // 2), BF),
                            pltpu.VMEM((J * R, d), BF), pltpu.VMEM((J * R, d), BF), pltpu.VMEM((J, 8, R, hq), BF),
                            dma((2, 8)), dma((2, 8)), dma((J, 9)), dma((J, 9)), dma((J, 9)), dma((J, 9)),
                            dma((J, 7)), dma((J, 7)), dma((19,)), dma((19,)), dma((2, J)), dma((3,))],
            compiler_params=pltpu.CompilerParams(collective_id=0, has_side_effects=True,
                                                 vmem_limit_bytes=67043328),
            cost_estimate=pl.CostEstimate(flops=2 * t * d * ff * 4, bytes_accessed=2 * t * d * 6, transcendentals=0),
            name="layer",
        )(x, g1.reshape(1, d), g2.reshape(1, d), cs, sn, wq, wk, wv, wo, wg, wu, wd)
        nt = 16
        y, k, v = pl.pallas_call(
            functools.partial(_copy_kernel, nt), in_specs=[ANY] * 3, out_specs=[ANY] * 3,
            out_shape=[big(t, d), big(t, HEAD), big(t, HEAD)],
            scratch_shapes=[pltpu.VMEM((t, d), BF), pltpu.VMEM((t, HEAD), BF), pltpu.VMEM((t, HEAD), BF),
                            dma((nt + 2,)), dma((nt + 2,))],
            compiler_params=pltpu.CompilerParams(vmem_limit_bytes=32 << 20), name="out")(y, k, v)
        return y, k.reshape(t, 1, HEAD), v.reshape(t, 1, HEAD)

    return jax.shard_map(
        local,
        mesh=mesh,
        in_specs=(P("dp", None), P("dp"), P(), P(), P(None, "tp"), P(), P(), P("tp", None),
                  P(None, "tp"), P(None, "tp"), P("tp", None)),
        out_specs=(P("dp", None), P("dp", "tp", None), P("dp", "tp", None)),
        check_vma=False,
    )
```

```python
import functools

import jax
import jax.numpy as jnp
from jax import lax
from jax.experimental import pallas as pl
from jax.experimental.pallas import tpu as pltpu
from jax.sharding import PartitionSpec as P

HEAD = 128
EPS = 1e-5
ROPE_BASE = 500000.0
LOG2E = 1.4426950408889634
NCHUNK = 8
MESH = pl.DeviceIdType.MESH
F32, BF = jnp.float32, jnp.bfloat16
ANY = pl.BlockSpec(memory_space=pl.ANY)


def _pos_of(r):
    return (r % 2) * 4 + r // 2


def _norm_rows(src, g_ref, dst, rows, step=16):
    @pl.loop(0, rows // step, unroll=2)
    def _(n):
        sl = pl.ds(pl.multiple_of(n * step, step), step)
        t = src[sl, :].astype(F32)
        inv = lax.rsqrt(jnp.mean(t * t, axis=-1, keepdims=True) + EPS)
        dst[sl, :] = (t * inv * g_ref[...]).astype(BF)


def _copy_kernel(nt, y, k, v, yo, ko, vo, yb, kb, vb, si, so):
    rows = y.shape[0] // nt
    ins, outs = [], []
    for i in range(nt):
        r = pl.ds(i * rows, rows)
        ins.append(pltpu.make_async_copy(y.at[r, :], yb.at[r, :], si.at[i]))
        outs.append(pltpu.make_async_copy(yb.at[r, :], yo.at[r, :], so.at[i]))
    for i, (a, b, o) in enumerate(((k, kb, ko), (v, vb, vo))):
        ins.append(pltpu.make_async_copy(a, b, si.at[nt + i]))
        outs.append(pltpu.make_async_copy(b, o, so.at[nt + i]))
    for cp in ins:
        cp.start()
    for a, b in zip(ins, outs):
        a.wait()
        b.start()
    for cp in outs:
        cp.wait()


def _big_kernel(J, R, QB, x_ref, g_ref, cos_ref, sin_ref, wq_ref, wk_ref, wv_ref, wo_ref, wg_ref, wu_ref,
                wd_ref, y_ref, kout, vout, oland, bland, rs1land, woland,
                wg, wu, wd, rs2x, rs2y, rs3a, rs3b, hk, own, q,
                a2s, a2r, abs_, abr, ays, ayr, rss, rsr, wos, wor, lsem, wsem):
    me = lax.axis_index("tp")
    c, s = me // 2, me % 2
    T, D = x_ref.shape
    H = D // 2
    g1_ref, g2_ref = g_ref.at[pl.ds(0, 1), :], g_ref.at[pl.ds(1, 1), :]
    C = 8 * R
    R4 = 4 * R
    hq = wq_ref.shape[1]
    nh = hq // HEAD
    cx = c + 1 - 2 * (c % 2)
    cy = (c + 2) % 4
    cd = 3 - c
    dev = lambda chip, core: chip * 2 + core
    X, Y, DG, PT = dev(cx, s), dev(cy, s), dev(cd, s), dev(c, 1 - s)
    mypos = s * 4 + c
    px, py, pd = s * 4 + cx, s * 4 + cy, s * 4 + cd

    z = lax.axis_index("dp")

    def rcopy(src, dst, ss, rs, to):
        where = {"dp": 1 - z, "tp": me} if to is None else {"tp": to}
        return pltpu.make_async_remote_copy(src_ref=src, dst_ref=dst, send_sem=ss, recv_sem=rs,
                                            device_id=where, device_id_type=MESH)

    wcp = [pltpu.make_async_copy(wg_ref, wg, wsem.at[0]), pltpu.make_async_copy(wu_ref, wu, wsem.at[1]),
           pltpu.make_async_copy(wd_ref, wd, wsem.at[2])]

    bar = pltpu.get_barrier_semaphore()
    for m in range(1, 8):
        pl.semaphore_signal(bar, inc=1, device_id={"tp": (me + m) % 8}, device_id_type=MESH)
    pl.semaphore_signal(bar, inc=1, device_id={"dp": 1 - z, "tp": me}, device_id_type=MESH)
    pl.semaphore_wait(bar, 8)

    WB = hq // 3
    zr, ob, lr = z * 2 * WB, WB, (1 - z) * 2 * WB

    def worows(d, off=0, n=WB):
        return woland.at[pl.ds(pl.multiple_of(d * hq + off, WB), n), :]

    def wo_copy(i):
        k = dict(ss=wos.at[i], rs=wor.at[i])
        if i < 4:
            off = (zr, ob)[i // 2]
            return rcopy(wo_ref.at[pl.ds(pl.multiple_of(off, WB), WB), :], worows(me, off), to=(X, Y)[i % 2], **k)
        if i == 4:
            return rcopy(wo_ref, worows(me, 0, hq), to=PT, **k)
        d, off, to = ((X, zr, Y), (Y, ob, X), (X, zr, None), (Y, zr, None), (DG, zr, None), (X, zr, PT), (Y, zr, PT),
                      (X, ob, PT), (Y, ob, PT), (DG, zr, PT), (DG, ob, PT), (X, lr, PT), (Y, lr, PT),
                      (DG, lr, PT))[i - 5]
        return rcopy(worows(d, off), worows(d, off), to=to, **k)

    def wo_recv(i):
        x1, y1, d1 = dev(cx, 1 - s), dev(cy, 1 - s), dev(cd, 1 - s)
        d = worows(*((X, zr), (Y, zr), (X, ob), (Y, ob), (PT, 0, hq), (DG, zr), (DG, ob), (X, lr), (Y, lr), (DG, lr),
                     (x1, zr), (y1, zr), (x1, ob), (y1, ob), (d1, zr), (d1, ob), (x1, lr), (y1, lr), (d1, lr))[i])
        rcopy(d, d, wos.at[i], wor.at[i], PT).wait_recv()

    def wo_step(recvs, sends):
        for n in recvs:
            wo_recv(n)
        for n in sends:
            wo_copy(n).start()

    wo_in = pltpu.make_async_copy(wo_ref, hk.at[pl.ds(0, hq), :], lsem.at[0, 0])
    wo_out = pltpu.make_async_copy(hk.at[pl.ds(0, hq), :], worows(me, 0, hq), lsem.at[0, 0])

    def peer(m):
        return (me + m) % 8

    def frm(m):
        return (me + 8 - m) % 8

    JH = J // 2

    def a2a(b, m):
        to = peer(m)
        return rcopy(q.at[pl.ds(b * JH, JH), _pos_of(to)],
                     oland.at[me, pl.ds(b * JH, JH)],
                     a2s.at[b, m], a2r.at[b, m], to)

    def a2a_land(b, m):
        return oland.at[frm(m), pl.ds(b * JH, JH)]

    def a2a_own(b):
        return pltpu.make_async_copy(q.at[pl.ds(b * JH, JH), mypos], a2a_land(b, 0), a2s.at[b, 0])

    def send_o(b):
        for m in range(1, 8):
            a2a(b, m).start()
        a2a_own(b).start()

    def qblock(i, h, n):
        return (pl.ds(i * (n // C), n // C), slice(None), slice(None), pl.ds(h * HEAD, HEAD))

    TM = min(512, T // 2)

    def qkv(k, v, vt):
        def run(w, xt, ct, st, tsem, msem):
            nb = T // TM
            col = pl.ds(pl.multiple_of(me * HEAD, HEAD), HEAD)
            cps = [pltpu.make_async_copy(wq_ref, w.at[:, pl.ds(0, hq)], msem.at[0]),
                   pltpu.make_async_copy(wk_ref.at[:, col], w.at[:, pl.ds(hq, HEAD)], msem.at[1]),
                   pltpu.make_async_copy(wv_ref.at[:, col], w.at[:, pl.ds(hq + HEAD, HEAD)], msem.at[2])]

            def tile(i, slot):
                r = pl.ds(pl.multiple_of(i * TM, TM), TM)
                t = pl.ds(pl.multiple_of((i % (nb // 2)) * TM, TM), TM)
                return [pltpu.make_async_copy(x_ref.at[r, :], xt.at[slot], tsem.at[slot, 0]),
                        pltpu.make_async_copy(cos_ref.at[t, :], ct.at[slot], tsem.at[slot, 1]),
                        pltpu.make_async_copy(sin_ref.at[t, :], st.at[slot], tsem.at[slot, 2])]

            for cp in tile(0, 0) + cps:
                cp.start()
            wo_step((), range(5))
            wo_in.start()

            @pl.loop(0, nb)
            def _(i):
                slot = i % 2

                @pl.when(i + 1 < nb)
                def _():
                    for cp in tile(i + 1, 1 - slot):
                        cp.start()

                for cp in tile(i, slot):
                    cp.wait()
                _norm_rows(xt.at[slot], g1_ref, xt.at[slot], TM)

                @pl.when(i == 0)
                def _():
                    for cp in cps:
                        cp.wait()

                row = pl.ds(pl.multiple_of(i * TM, TM), TM)
                low = lax.broadcasted_iota(jnp.int32, (TM, HEAD), 1) < HEAD // 2
                keep = jnp.logical_xor(low, i >= nb // 2)
                cb, sb = ct[slot], st[slot]
                cc = jnp.where(keep, cb, pltpu.roll(cb, HEAD // 2, 1))
                ss = jnp.where(keep, sb, pltpu.roll(sb, HEAD // 2, 1))
                ss = jnp.where(low, -ss, ss)
                z = jnp.dot(xt[slot], w[...], preferred_element_type=F32)
                for h in range(nh + 1):
                    t = z[:, h * HEAD:(h + 1) * HEAD]
                    t = (t * cc + pltpu.roll(t, HEAD // 2, 1) * ss).astype(BF)
                    if h < nh:
                        q[qblock(i, h, TM)] = t.reshape(TM // C, 8, R, HEAD)
                    else:
                        k[row, :] = t
                zv = z[:, hq + HEAD:]
                v[row, :] = zv.astype(BF)
                vt[:, row] = zv.T.astype(BF)

                @pl.when(i == nb // 2)
                def _():
                    wo_step((0, 1), (7, 8, 5, 10, 11))

        pl.run_scoped(run, pltpu.VMEM((D, hq + 2 * HEAD), BF), pltpu.VMEM((2, TM, D), BF),
                      pltpu.VMEM((2, TM, HEAD), F32), pltpu.VMEM((2, TM, HEAD), F32),
                      pltpu.SemaphoreType.DMA((2, 3)), pltpu.SemaphoreType.DMA((3,)))

    def attention(k, v, vt, acc, mm, ll, mx, sb, asem):
        qkv(k, v, vt)
        kv_out = [pltpu.make_async_copy(k, kout, asem.at[0]), pltpu.make_async_copy(v, vout, asem.at[1])]
        for cp in kv_out + wcp:
            cp.start()
        wo_in.wait()
        wo_out.start()
        wo_step((2, 3), (6, 12, 13))
        sc = (HEAD ** -0.5) * LOG2E
        nq = T // QB
        ki = lax.broadcasted_iota(jnp.int32, (QB, QB), 0)
        qi = lax.broadcasted_iota(jnp.int32, (QB, QB), 1)

        @pl.loop(0, nq)
        def _(i):
            def qk(kb, h, masked=False):
                kk = k[pl.ds(pl.multiple_of(kb * QB, QB), QB), :]
                t = lax.dot_general(kk, q[qblock(i, h, QB)].reshape(QB, HEAD), (((1,), (1,)), ((), ())),
                                    preferred_element_type=F32)
                if masked:
                    t = jnp.where(ki <= qi, t, -jnp.inf)
                sb[h] = t
                mx[h] = jnp.max(t, axis=0, keepdims=True)

            def soft(kb, h):
                mo = mm[h]
                mn = jnp.maximum(mo, mx[h])
                mm[h] = mn
                al = jnp.exp2((mo - mn) * sc)
                p = jnp.exp2((sb[h] - mn) * sc)
                ll[h] = ll[h] * al + jnp.sum(p, axis=0, keepdims=True)
                acc[h] = acc[h] * al + jnp.dot(vt[:, pl.ds(pl.multiple_of(kb * QB, QB), QB)], p.astype(BF),
                                               preferred_element_type=F32)

            acc[...] = jnp.zeros_like(acc)
            ll[...] = jnp.zeros_like(ll)
            mm[...] = jnp.full_like(mm, -jnp.inf)

            def phases(kb, nxt, masked):
                for h in range(nh):
                    ahead = h + nh - 1
                    if ahead < nh:
                        qk(kb, ahead, masked)
                    else:
                        qk(nxt, ahead - nh)
                    soft(kb, h)

            for h in range(nh - 1):
                qk(i, h, True)
            phases(i, 0, True)

            @pl.loop(0, i)
            def _(kb):
                phases(kb, kb + 1, False)

            for h in range(nh):
                q[qblock(i, h, QB)] = (acc[h] / ll[h]).T.astype(BF).reshape(QB // C, 8, R, HEAD)

            @pl.when(i == nq // 2 - 1)
            def _():
                send_o(0)

            @pl.when(i == nq * 3 // 4 - 1)
            def _():
                wo_step((5, 7, 8), (9, 14, 16, 17))

        wo_step((6, 9), (15, 18))
        for cp in kv_out:
            cp.wait()

    pl.run_scoped(attention, pltpu.VMEM((T, HEAD), BF), pltpu.VMEM((T, HEAD), BF),
                  pltpu.VMEM((HEAD, T), BF), pltpu.VMEM((nh, HEAD, QB), F32),
                  pltpu.VMEM((nh, 1, QB), F32), pltpu.VMEM((nh, 1, QB), F32), pltpu.VMEM((nh, 1, QB), F32),
                  pltpu.VMEM((nh, QB, QB), F32), pltpu.SemaphoreType.DMA((2,)))
    wo_out.wait()
    wo_step((4,) + tuple(range(10, 19)), ())
    for n in range(19):
        wo_copy(n).wait_send()

    R2 = R // 2

    def rows(land, j, pos, off=0, n=R):
        return land.at[pl.ds(pl.multiple_of(j * C + pos * R + off, R2), n), :]

    def ownrows(j):
        return own.at[pl.ds(pl.multiple_of(j * R, R), R), :]

    def g_copy(land, ss, rs, j, i):
        k = dict(ss=ss.at[j, i], rs=rs.at[j, i])
        if i < 3:
            return rcopy(ownrows(j), rows(land, j, mypos), to=(X, Y, PT)[i], **k)
        if i == 3:
            return rcopy(rows(land, j, px, 0, R2), rows(land, j, px, 0, R2), to=Y, **k)
        if i == 4:
            return rcopy(rows(land, j, py, R2, R2), rows(land, j, py, R2, R2), to=X, **k)
        if i == 5:
            return rcopy(rows(land, j, px), rows(land, j, px), to=PT, **k)
        if i == 6:
            return rcopy(rows(land, j, py), rows(land, j, py), to=PT, **k)
        off = 0 if i == 7 else R2
        return rcopy(rows(land, j, pd, off, R2), rows(land, j, pd, off, R2), to=PT, **k)

    def g_recv(land, ss, rs, j, i):
        o4 = (1 - s) * 4
        src = [(px, 0, R), (py, 0, R), (o4 + c, 0, R), (pd, 0, R2), (pd, R2, R2), (o4 + cx, 0, R), (o4 + cy, 0, R),
               (o4 + cd, 0, R2), (o4 + cd, R2, R2)][i]
        d = rows(land, j, *src)
        rcopy(d, d, ss.at[j, i], rs.at[j, i], PT).wait_recv()

    def g_local(land, j, kind):
        return pltpu.make_async_copy(ownrows(j), rows(land, j, mypos), lsem.at[kind, j])

    def g_own(land, ss, rs, j, kind):
        for i in range(3):
            g_copy(land, ss, rs, j, i).start()
        g_local(land, j, kind).start()

    def g_fwd(land, ss, rs, j):
        g_recv(land, ss, rs, j, 0)
        g_copy(land, ss, rs, j, 3).start()
        g_recv(land, ss, rs, j, 1)
        g_copy(land, ss, rs, j, 4).start()
        g_copy(land, ss, rs, j, 5).start()
        g_copy(land, ss, rs, j, 6).start()

    def g_fwd2(land, ss, rs, j):
        for i in (3, 4):
            g_recv(land, ss, rs, j, i)
            g_copy(land, ss, rs, j, i + 4).start()

    def g_finish(land, ss, rs, j):
        for i in (2, 5, 6, 7, 8):
            g_recv(land, ss, rs, j, i)

    gb = (bland, abs_, abr)
    gy = (y_ref, ays, ayr)

    def ew(n, f):
        @pl.loop(0, n // 16)
        def _(i):
            f(pl.ds(pl.multiple_of(i * 16, 16), 16))

    def mlp(bt, us, pb, rt, sums, oo, wt, bsem, osem, tsem):
        NT = wt.shape[2]
        RH = JH * R

        def x_in(j):
            return pltpu.make_async_copy(x_ref.at[pl.ds(pl.multiple_of(j * C + mypos * R, R), R), :],
                                         hk.at[pl.ds(pl.multiple_of(j * R, R), R), :], osem.at[j])

        def oproj(half):
            part = pl.ds(half * RH, RH)

            def tile(n, slot):
                return pltpu.make_async_copy(woland.at[:, pl.ds(pl.multiple_of(n * NT, NT), NT)], wt.at[slot],
                                             tsem.at[slot])

            tile(0, 0).start()

            for m in range(1, 8):
                d = a2a_land(half, m)
                rcopy(d, d, a2s.at[half, m], a2r.at[half, m], PT).wait_recv()
            a2a_own(half).wait()
            cps = [pltpu.make_async_copy(oland.at[d, pl.ds(half * JH, JH)], oo.at[:, :, pl.ds(d * hq, hq)],
                                         osem.at[J + d]) for d in range(8)]
            for cp in cps:
                cp.start()
            for cp in cps:
                cp.wait()
            for j in range(half * JH, (half + 1) * JH):
                x_in(j).wait()
            nt = D // NT

            @pl.loop(0, nt)
            def _(n):
                slot = n % 2

                @pl.when(n + 1 < nt)
                def _():
                    tile(n + 1, 1 - slot).start()

                tile(n, slot).wait()
                col = pl.ds(pl.multiple_of(n * NT, NT), NT)
                hk[part, col] = (hk[part, col].astype(F32)
                                 + jnp.dot(oo[...].reshape(RH, 8 * hq), wt[slot], preferred_element_type=F32)).astype(BF)

            _norm_rows(hk.at[part, :], g2_ref, own.at[part, :], RH)

        def sumsl(j, chip, col):
            return sums.at[j % 2, pl.ds(pl.multiple_of(chip * R, R), R), col]

        lo, hi = pl.ds(0, H), pl.ds(H, H)

        def rs_copy(j, i):
            k = dict(ss=rss.at[j, i], rs=rsr.at[j, i])
            if i == 0:
                return rcopy(pb.at[0], rs1land.at[j], to=PT, **k)
            if i == 1:
                return rcopy(sumsl(j, cx, lo), rs2x.at[j, 0], to=X, **k)
            if i == 2:
                return rcopy(sumsl(j, cd, lo), rs2x.at[j, 1], to=X, **k)
            if i == 3:
                return rcopy(sumsl(j, cy, hi), rs2y.at[j, 0], to=Y, **k)
            if i == 4:
                return rcopy(sumsl(j, cd, hi), rs2y.at[j, 1], to=Y, **k)
            if i == 5:
                return rcopy(sumsl(j, cy, lo), rs3a.at[j], to=Y, **k)
            return rcopy(sumsl(j, cx, hi), rs3b.at[j], to=X, **k)

        def load_b(j, half):
            pos = ((1 - s) if half == 0 else s) * 4
            return pltpu.make_async_copy(bland.at[pl.ds(pl.multiple_of(j * C + pos * R, R4), R4), :], bt.at[half],
                                         bsem.at[half])

        def compute(j):
            for half in range(2):
                load_b(j, half).wait()
                if half == 0:
                    @pl.when(j >= 1)
                    def _():
                        rs_copy(j - 1, 0).wait_send()

                @pl.loop(0, us.shape[1] // 256)
                def _(n):
                    col = pl.ds(pl.multiple_of(n * 256, 256), 256)
                    g = jnp.dot(bt[half], wg[:, col], preferred_element_type=F32)
                    u = jnp.dot(bt[half], wu[:, col], preferred_element_type=F32)
                    us[:, col] = (g * jax.nn.sigmoid(g) * u).astype(BF)

                @pl.loop(0, D // 512)
                def _(n):
                    col = pl.ds(pl.multiple_of(n * 512, 512), 512)
                    pb[half, :, col] = jnp.dot(us[...], wd[:, col], preferred_element_type=F32).astype(BF)

                if half == 0:
                    rs_copy(j, 0).start()

            rs_copy(j, 0).wait_recv()
            cp = pltpu.make_async_copy(rs1land.at[j], rt, bsem.at[2])
            cp.start()
            cp.wait()

            @pl.when(j >= 2)
            def _():
                for i in range(1, 7):
                    rs_copy(j - 2, i).wait_send()

            def add(sl):
                sums[j % 2, sl, :] = (pb[1, sl, :].astype(F32) + rt[sl, :].astype(F32)).astype(BF)

            ew(R4, add)
            for i in (1, 3, 2, 4):
                rs_copy(j, i).start()

        def rs3(j):
            for i in (1, 3, 2, 4):
                rs_copy(j, i).wait_recv()

            def addy(sl):
                b = pl.ds(pl.multiple_of(cy * R + sl.start, 16), 16)
                sums[j % 2, b, lo] = (sums[j % 2, b, lo].astype(F32) + rs2x[j, 1, sl, :].astype(F32)).astype(BF)
                b = pl.ds(pl.multiple_of(cx * R + sl.start, 16), 16)
                sums[j % 2, b, hi] = (sums[j % 2, b, hi].astype(F32) + rs2y[j, 1, sl, :].astype(F32)).astype(BF)

            ew(R, addy)
            rs_copy(j, 5).start()
            rs_copy(j, 6).start()

        def final(j):
            rs_copy(j, 5).wait_recv()
            rs_copy(j, 6).wait_recv()
            for i in range(3):
                g_copy(*gb, j, i).wait_send()

            def fin(sl):
                b = pl.ds(pl.multiple_of(c * R + sl.start, 16), 16)
                o = pl.ds(pl.multiple_of(j * R + sl.start, 16), 16)
                for col, r2, r3 in ((lo, rs2x, rs3a), (hi, rs2y, rs3b)):
                    t = (sums[j % 2, b, col].astype(F32) + r2[j, 0, sl, :].astype(F32)) + r3[j, sl, :].astype(F32)
                    own[o, col] = (hk[o, col].astype(F32) + t).astype(BF)

            ew(R, fin)
            g_own(*gy, j, 1)

        for j in range(J):
            x_in(j).start()
        oproj(0)
        g_own(*gb, 0, 0)
        for cp in wcp:
            cp.wait()
        g_fwd(*gb, 0)
        g_own(*gb, 1, 0)
        send_o(1)

        @pl.loop(0, J + 4)
        def _(t):
            @pl.when(t < J)
            def _():
                g_fwd2(*gb, t)

            @pl.when(t + 1 < J)
            def _():
                g_fwd(*gb, t + 1)

            @pl.when(t >= 4)
            def _():
                g_fwd2(*gy, t - 4)

            @pl.when(jnp.logical_and(t >= 3, t < J + 3))
            def _():
                g_fwd(*gy, t - 3)

            @pl.when(t + 2 < J)
            def _():
                g_own(*gb, t + 2, 0)

            @pl.when(t < J)
            def _():
                g_finish(*gb, t)
                g_local(bland, t, 0).wait()
                for half in range(2):
                    load_b(t, half).start()

            @pl.when(jnp.logical_and(t >= 2, t < J + 2))
            def _():
                final(t - 2)

            @pl.when(t < J)
            def _():
                compute(t)

            @pl.when(jnp.logical_and(t >= 1, t < J + 1))
            def _():
                rs3(t - 1)

            @pl.when(t == 0)
            def _():
                oproj(1)

        for b in range(2):
            for m in range(1, 8):
                a2a(b, m).wait_send()
        rs_copy(J - 1, 0).wait_send()
        for j in range(max(J - 2, 0), J):
            for i in range(1, 7):
                rs_copy(j, i).wait_send()

    pl.run_scoped(mlp, pltpu.VMEM((2, R4, D), BF), pltpu.VMEM((R4, wg.shape[1]), BF), pltpu.VMEM((2, R4, D), BF),
                  pltpu.VMEM((R4, D), BF), pltpu.VMEM((2, R4, D), BF), pltpu.VMEM((J // 2, R, 8 * hq), BF),
                  pltpu.VMEM((2, 8 * hq, min(512, D)), BF), pltpu.SemaphoreType.DMA((3,)),
                  pltpu.SemaphoreType.DMA((8 + J,)), pltpu.SemaphoreType.DMA((2,)))

    @pl.loop(0, J)
    def _(j):
        g_finish(*gy, j)
        for i in range(3, 9):
            g_copy(*gb, j, i).wait_send()
        for i in range(9):
            g_copy(*gy, j, i).wait_send()
        g_local(y_ref, j, 1).wait()


def _tables(pos):
    half = HEAD // 2
    inv = ROPE_BASE ** (-2.0 * jnp.arange(half, dtype=F32) / HEAD)
    t = pos.shape[0]
    p = pos.astype(F32)
    lane = lax.broadcasted_iota(jnp.int32, (t // 2, HEAD), 1)
    pp = jnp.where(lane < half, p[:t // 2, None], p[t // 2:, None])
    ang = pp * jnp.concatenate([inv, inv])[None, :]
    return jnp.cos(ang), jnp.sin(ang)


def solution(mesh):
    def local(x, pos, g1, g2, wq, wk, wv, wo, wg, wu, wd):
        t, d = x.shape
        hq = wq.shape[1]
        ff = wg.shape[1]
        cs, sn = _tables(pos)
        J = NCHUNK
        R = t // 8 // J
        QB = min(512, 8 * R)
        dma = pltpu.SemaphoreType.DMA
        vm = pl.BlockSpec(memory_space=pltpu.VMEM)
        big = lambda *sh: jax.ShapeDtypeStruct(sh, BF)
        y, k, v, *_ = pl.pallas_call(
            functools.partial(_big_kernel, J, R, QB),
            in_specs=[ANY, vm] + [ANY] * 9,
            out_specs=[ANY] * 7,
            out_shape=[big(t, d), big(t, HEAD), big(t, HEAD), big(8, J, R, hq), big(t, d), big(J, 4 * R, d),
                       big(8 * hq, d)],
            scratch_shapes=[pltpu.VMEM((d, ff), BF), pltpu.VMEM((d, ff), BF), pltpu.VMEM((ff, d), BF),
                            pltpu.VMEM((J, 2, R, d // 2), BF), pltpu.VMEM((J, 2, R, d // 2), BF),
                            pltpu.VMEM((J, R, d // 2), BF), pltpu.VMEM((J, R, d // 2), BF),
                            pltpu.VMEM((J * R, d), BF), pltpu.VMEM((J * R, d), BF), pltpu.VMEM((J, 8, R, hq), BF),
                            dma((2, 8)), dma((2, 8)), dma((J, 9)), dma((J, 9)), dma((J, 9)), dma((J, 9)),
                            dma((J, 7)), dma((J, 7)), dma((19,)), dma((19,)), dma((2, J)), dma((3,))],
            compiler_params=pltpu.CompilerParams(collective_id=0, has_side_effects=True,
                                                 vmem_limit_bytes=67043328),
            cost_estimate=pl.CostEstimate(flops=2 * t * d * ff * 4, bytes_accessed=2 * t * d * 6, transcendentals=0),
            name="layer",
        )(x, jnp.stack([g1, g2]).astype(F32), cs, sn, wq, wk, wv, wo, wg, wu, wd)
        nt = 16
        y, k, v = pl.pallas_call(
            functools.partial(_copy_kernel, nt), in_specs=[ANY] * 3, out_specs=[ANY] * 3,
            out_shape=[big(t, d), big(t, HEAD), big(t, HEAD)],
            scratch_shapes=[pltpu.VMEM((t, d), BF), pltpu.VMEM((t, HEAD), BF), pltpu.VMEM((t, HEAD), BF),
                            dma((nt + 2,)), dma((nt + 2,))],
            compiler_params=pltpu.CompilerParams(vmem_limit_bytes=67043328), name="out")(y, k, v)
        return y, k.reshape(t, 1, HEAD), v.reshape(t, 1, HEAD)

    return jax.shard_map(
        local,
        mesh=mesh,
        in_specs=(P("dp", None), P("dp"), P(), P(), P(None, "tp"), P(), P(), P("tp", None),
                  P(None, "tp"), P(None, "tp"), P("tp", None)),
        out_specs=(P("dp", None), P("dp", "tp", None), P("dp", "tp", None)),
        check_vma=False,
    )
```

```python
import functools

import jax
import jax.numpy as jnp
from jax import lax
from jax.experimental import pallas as pl
from jax.experimental.pallas import tpu as pltpu
from jax.sharding import PartitionSpec as P

HEAD = 128
EPS = 1e-5
ROPE_BASE = 500000.0
LOG2E = 1.4426950408889634
NCHUNK = 8
MESH = pl.DeviceIdType.MESH
F32, BF = jnp.float32, jnp.bfloat16
ANY = pl.BlockSpec(memory_space=pl.ANY)


def _pos_of(r):
    return (r % 2) * 4 + r // 2


def _norm_rows(src, g_ref, dst, rows, step=16):
    @pl.loop(0, rows // step, unroll=2)
    def _(n):
        sl = pl.ds(pl.multiple_of(n * step, step), step)
        t = src[sl, :].astype(F32)
        inv = lax.rsqrt(jnp.mean(t * t, axis=-1, keepdims=True) + EPS)
        dst[sl, :] = (t * inv * g_ref[...]).astype(BF)


def _copy_kernel(nt, y, k, v, yo, ko, vo, yb, kb, vb, si, so):
    rows = y.shape[0] // nt
    ins, outs = [], []
    for i in range(nt):
        r = pl.ds(i * rows, rows)
        ins.append(pltpu.make_async_copy(y.at[r, :], yb.at[r, :], si.at[i]))
        outs.append(pltpu.make_async_copy(yb.at[r, :], yo.at[r, :], so.at[i]))
    for i, (a, b, o) in enumerate(((k, kb, ko), (v, vb, vo))):
        ins.append(pltpu.make_async_copy(a, b, si.at[nt + i]))
        outs.append(pltpu.make_async_copy(b, o, so.at[nt + i]))
    for cp in ins:
        cp.start()
    for a, b in zip(ins, outs):
        a.wait()
        b.start()
    for cp in outs:
        cp.wait()


def _big_kernel(J, R, QB, x_ref, g_ref, cos_ref, sin_ref, wq_ref, wk_ref, wv_ref, wo_ref, wg_ref, wu_ref,
                wd_ref, y_ref, kout, vout, oland, bland, rs1land, woland,
                wg, wu, wd, rs2x, rs2y, rs3a, rs3b, hk, own, q,
                a2s, a2r, abs_, abr, ays, ayr, rss, rsr, wos, wor, lsem, wsem):
    me = lax.axis_index("tp")
    c, s = me // 2, me % 2
    T, D = x_ref.shape
    H = D // 2
    g1_ref, g2_ref = g_ref.at[pl.ds(0, 1), :], g_ref.at[pl.ds(1, 1), :]
    C = 8 * R
    R4 = 4 * R
    hq = wq_ref.shape[1]
    nh = hq // HEAD
    cx = c + 1 - 2 * (c % 2)
    cy = (c + 2) % 4
    cd = 3 - c
    dev = lambda chip, core: chip * 2 + core
    X, Y, DG, PT = dev(cx, s), dev(cy, s), dev(cd, s), dev(c, 1 - s)
    mypos = s * 4 + c
    px, py, pd = s * 4 + cx, s * 4 + cy, s * 4 + cd

    z = lax.axis_index("dp")

    def rcopy(src, dst, ss, rs, to):
        where = {"dp": 1 - z, "tp": me} if to is None else {"tp": to}
        return pltpu.make_async_remote_copy(src_ref=src, dst_ref=dst, send_sem=ss, recv_sem=rs,
                                            device_id=where, device_id_type=MESH)

    wcp = [pltpu.make_async_copy(wg_ref, wg, wsem.at[0]), pltpu.make_async_copy(wu_ref, wu, wsem.at[1]),
           pltpu.make_async_copy(wd_ref, wd, wsem.at[2])]

    bar = pltpu.get_barrier_semaphore()
    for m in range(1, 8):
        pl.semaphore_signal(bar, inc=1, device_id={"tp": (me + m) % 8}, device_id_type=MESH)
    pl.semaphore_signal(bar, inc=1, device_id={"dp": 1 - z, "tp": me}, device_id_type=MESH)
    pl.semaphore_wait(bar, 8)

    WB = hq // 3
    zr, ob, lr = z * 2 * WB, WB, (1 - z) * 2 * WB

    def worows(d, off=0, n=WB):
        return woland.at[pl.ds(pl.multiple_of(d * hq + off, WB), n), :]

    def wo_copy(i):
        k = dict(ss=wos.at[i], rs=wor.at[i])
        if i < 4:
            off = (zr, ob)[i // 2]
            return rcopy(wo_ref.at[pl.ds(pl.multiple_of(off, WB), WB), :], worows(me, off), to=(X, Y)[i % 2], **k)
        if i == 4:
            return rcopy(wo_ref, worows(me, 0, hq), to=PT, **k)
        d, off, to = ((X, zr, Y), (Y, ob, X), (X, zr, None), (Y, zr, None), (DG, zr, None), (X, zr, PT), (Y, zr, PT),
                      (X, ob, PT), (Y, ob, PT), (DG, zr, PT), (DG, ob, PT), (X, lr, PT), (Y, lr, PT),
                      (DG, lr, PT))[i - 5]
        return rcopy(worows(d, off), worows(d, off), to=to, **k)

    def wo_recv(i):
        x1, y1, d1 = dev(cx, 1 - s), dev(cy, 1 - s), dev(cd, 1 - s)
        d = worows(*((X, zr), (Y, zr), (X, ob), (Y, ob), (PT, 0, hq), (DG, zr), (DG, ob), (X, lr), (Y, lr), (DG, lr),
                     (x1, zr), (y1, zr), (x1, ob), (y1, ob), (d1, zr), (d1, ob), (x1, lr), (y1, lr), (d1, lr))[i])
        rcopy(d, d, wos.at[i], wor.at[i], PT).wait_recv()

    def wo_step(recvs, sends):
        for n in recvs:
            wo_recv(n)
        for n in sends:
            wo_copy(n).start()

    wo_in = pltpu.make_async_copy(wo_ref, hk.at[pl.ds(0, hq), :], lsem.at[0, 0])
    wo_out = pltpu.make_async_copy(hk.at[pl.ds(0, hq), :], worows(me, 0, hq), lsem.at[0, 0])

    def peer(m):
        return (me + m) % 8

    def frm(m):
        return (me + 8 - m) % 8

    JH = J // 2

    def a2a(b, m):
        to = peer(m)
        return rcopy(q.at[pl.ds(b * JH, JH), _pos_of(to)],
                     oland.at[me, pl.ds(b * JH, JH)],
                     a2s.at[b, m], a2r.at[b, m], to)

    def a2a_land(b, m):
        return oland.at[frm(m), pl.ds(b * JH, JH)]

    def a2a_own(b):
        return pltpu.make_async_copy(q.at[pl.ds(b * JH, JH), mypos], a2a_land(b, 0), a2s.at[b, 0])

    def send_o(b):
        for m in range(1, 8):
            a2a(b, m).start()
        a2a_own(b).start()

    def qblock(i, h, n):
        return (pl.ds(i * (n // C), n // C), slice(None), slice(None), pl.ds(h * HEAD, HEAD))

    TM = min(512, T // 2)

    def qkv(k, v, vt):
        def run(w, xt, ct, st, tsem, msem):
            nb = T // TM
            col = pl.ds(pl.multiple_of(me * HEAD, HEAD), HEAD)
            cps = [pltpu.make_async_copy(wq_ref, w.at[:, pl.ds(0, hq)], msem.at[0]),
                   pltpu.make_async_copy(wk_ref.at[:, col], w.at[:, pl.ds(hq, HEAD)], msem.at[1]),
                   pltpu.make_async_copy(wv_ref.at[:, col], w.at[:, pl.ds(hq + HEAD, HEAD)], msem.at[2])]

            def tile(i, slot):
                r = pl.ds(pl.multiple_of(i * TM, TM), TM)
                t = pl.ds(pl.multiple_of((i % (nb // 2)) * TM, TM), TM)
                return [pltpu.make_async_copy(x_ref.at[r, :], xt.at[slot], tsem.at[slot, 0]),
                        pltpu.make_async_copy(cos_ref.at[t, :], ct.at[slot], tsem.at[slot, 1]),
                        pltpu.make_async_copy(sin_ref.at[t, :], st.at[slot], tsem.at[slot, 2])]

            for cp in tile(0, 0) + cps:
                cp.start()
            wo_step((), range(5))
            wo_in.start()

            @pl.loop(0, nb)
            def _(i):
                slot = i % 2

                @pl.when(i + 1 < nb)
                def _():
                    for cp in tile(i + 1, 1 - slot):
                        cp.start()

                for cp in tile(i, slot):
                    cp.wait()
                _norm_rows(xt.at[slot], g1_ref, xt.at[slot], TM)

                @pl.when(i == 0)
                def _():
                    for cp in cps:
                        cp.wait()

                row = pl.ds(pl.multiple_of(i * TM, TM), TM)
                low = lax.broadcasted_iota(jnp.int32, (TM, HEAD), 1) < HEAD // 2
                keep = jnp.logical_xor(low, i >= nb // 2)
                cb, sb = ct[slot], st[slot]
                cc = jnp.where(keep, cb, pltpu.roll(cb, HEAD // 2, 1))
                ss = jnp.where(keep, sb, pltpu.roll(sb, HEAD // 2, 1))
                ss = jnp.where(low, -ss, ss)
                z = jnp.dot(xt[slot], w[...], preferred_element_type=F32)
                for h in range(nh + 1):
                    t = z[:, h * HEAD:(h + 1) * HEAD]
                    t = (t * cc + pltpu.roll(t, HEAD // 2, 1) * ss).astype(BF)
                    if h < nh:
                        q[qblock(i, h, TM)] = t.reshape(TM // C, 8, R, HEAD)
                    else:
                        k[row, :] = t
                zv = z[:, hq + HEAD:]
                v[row, :] = zv.astype(BF)
                vt[:, row] = zv.T.astype(BF)

                @pl.when(i == nb // 2)
                def _():
                    wo_step((0, 1), (7, 8, 5, 10, 11))

        pl.run_scoped(run, pltpu.VMEM((D, hq + 2 * HEAD), BF), pltpu.VMEM((2, TM, D), BF),
                      pltpu.VMEM((2, TM, HEAD), F32), pltpu.VMEM((2, TM, HEAD), F32),
                      pltpu.SemaphoreType.DMA((2, 3)), pltpu.SemaphoreType.DMA((3,)))

    def attention(k, v, vt, acc, mm, ll, mx, sb, asem):
        qkv(k, v, vt)
        kv_out = [pltpu.make_async_copy(k, kout, asem.at[0]), pltpu.make_async_copy(v, vout, asem.at[1])]
        for cp in kv_out + wcp:
            cp.start()
        wo_in.wait()
        wo_out.start()
        wo_step((2, 3), (6, 12, 13))
        sc = (HEAD ** -0.5) * LOG2E
        nq = T // QB
        ki = lax.broadcasted_iota(jnp.int32, (QB, QB), 0)
        qi = lax.broadcasted_iota(jnp.int32, (QB, QB), 1)

        @pl.loop(0, nq)
        def _(i):
            def qk(kb, h, masked=False):
                kk = k[pl.ds(pl.multiple_of(kb * QB, QB), QB), :]
                t = lax.dot_general(kk, q[qblock(i, h, QB)].reshape(QB, HEAD), (((1,), (1,)), ((), ())),
                                    preferred_element_type=F32)
                if masked:
                    t = jnp.where(ki <= qi, t, -jnp.inf)
                sb[h] = t
                mx[h] = jnp.max(t, axis=0, keepdims=True)

            def soft(kb, h):
                mo = mm[h]
                mn = jnp.maximum(mo, mx[h])
                mm[h] = mn
                al = jnp.exp2((mo - mn) * sc)
                p = jnp.exp2((sb[h] - mn) * sc)
                ll[h] = ll[h] * al + jnp.sum(p, axis=0, keepdims=True)
                acc[h] = acc[h] * al + jnp.dot(vt[:, pl.ds(pl.multiple_of(kb * QB, QB), QB)], p.astype(BF),
                                               preferred_element_type=F32)

            acc[...] = jnp.zeros_like(acc)
            ll[...] = jnp.zeros_like(ll)
            mm[...] = jnp.full_like(mm, -jnp.inf)

            def phases(kb, nxt, masked):
                for h in range(nh):
                    ahead = h + nh - 1
                    if ahead < nh:
                        qk(kb, ahead, masked)
                    else:
                        qk(nxt, ahead - nh)
                    soft(kb, h)

            for h in range(nh - 1):
                qk(i, h, True)
            phases(i, 0, True)

            @pl.loop(0, i)
            def _(kb):
                phases(kb, kb + 1, False)

            for h in range(nh):
                q[qblock(i, h, QB)] = (acc[h] / ll[h]).T.astype(BF).reshape(QB // C, 8, R, HEAD)

            @pl.when(i == nq // 2 - 1)
            def _():
                send_o(0)

            @pl.when(i == nq * 3 // 4 - 1)
            def _():
                wo_step((5,), (9, 14))

        send_o(1)
        wo_step((6,), (15,))
        wo_step((7, 8), (16, 17))
        wo_step((9,), (18,))
        for cp in kv_out:
            cp.wait()

    pl.run_scoped(attention, pltpu.VMEM((T, HEAD), BF), pltpu.VMEM((T, HEAD), BF),
                  pltpu.VMEM((HEAD, T), BF), pltpu.VMEM((nh, HEAD, QB), F32),
                  pltpu.VMEM((nh, 1, QB), F32), pltpu.VMEM((nh, 1, QB), F32), pltpu.VMEM((nh, 1, QB), F32),
                  pltpu.VMEM((nh, QB, QB), F32), pltpu.SemaphoreType.DMA((2,)))
    wo_out.wait()
    wo_step((4,) + tuple(range(10, 19)), ())
    for n in range(19):
        wo_copy(n).wait_send()

    R2 = R // 2

    def rows(land, j, pos, off=0, n=R):
        return land.at[pl.ds(pl.multiple_of(j * C + pos * R + off, R2), n), :]

    def ownrows(j):
        return own.at[pl.ds(pl.multiple_of(j * R, R), R), :]

    def g_copy(land, ss, rs, j, i):
        k = dict(ss=ss.at[j, i], rs=rs.at[j, i])
        if i < 3:
            return rcopy(ownrows(j), rows(land, j, mypos), to=(X, Y, PT)[i], **k)
        if i == 3:
            return rcopy(rows(land, j, px, 0, R2), rows(land, j, px, 0, R2), to=Y, **k)
        if i == 4:
            return rcopy(rows(land, j, py, R2, R2), rows(land, j, py, R2, R2), to=X, **k)
        if i == 5:
            return rcopy(rows(land, j, px), rows(land, j, px), to=PT, **k)
        if i == 6:
            return rcopy(rows(land, j, py), rows(land, j, py), to=PT, **k)
        off = 0 if i == 7 else R2
        return rcopy(rows(land, j, pd, off, R2), rows(land, j, pd, off, R2), to=PT, **k)

    def g_recv(land, ss, rs, j, i):
        o4 = (1 - s) * 4
        src = [(px, 0, R), (py, 0, R), (o4 + c, 0, R), (pd, 0, R2), (pd, R2, R2), (o4 + cx, 0, R), (o4 + cy, 0, R),
               (o4 + cd, 0, R2), (o4 + cd, R2, R2)][i]
        d = rows(land, j, *src)
        rcopy(d, d, ss.at[j, i], rs.at[j, i], PT).wait_recv()

    def g_local(land, j, kind):
        return pltpu.make_async_copy(ownrows(j), rows(land, j, mypos), lsem.at[kind, j])

    def g_own(land, ss, rs, j, kind):
        for i in range(3):
            g_copy(land, ss, rs, j, i).start()
        g_local(land, j, kind).start()

    def g_fwd(land, ss, rs, j):
        g_recv(land, ss, rs, j, 0)
        g_copy(land, ss, rs, j, 3).start()
        g_recv(land, ss, rs, j, 1)
        g_copy(land, ss, rs, j, 4).start()
        g_copy(land, ss, rs, j, 5).start()
        g_copy(land, ss, rs, j, 6).start()

    def g_fwd2(land, ss, rs, j):
        for i in (3, 4):
            g_recv(land, ss, rs, j, i)
            g_copy(land, ss, rs, j, i + 4).start()

    def g_finish(land, ss, rs, j):
        for i in (2, 5, 6, 7, 8):
            g_recv(land, ss, rs, j, i)

    gb = (bland, abs_, abr)
    gy = (y_ref, ays, ayr)

    def ew(n, f):
        @pl.loop(0, n // 16)
        def _(i):
            f(pl.ds(pl.multiple_of(i * 16, 16), 16))

    def mlp(bt, us, pb, rt, sums, oo, wt, bsem, osem, tsem):
        NT = wt.shape[2]
        RH = JH * R

        def x_in(j):
            return pltpu.make_async_copy(x_ref.at[pl.ds(pl.multiple_of(j * C + mypos * R, R), R), :],
                                         hk.at[pl.ds(pl.multiple_of(j * R, R), R), :], osem.at[j])

        def oproj(half):
            part = pl.ds(half * RH, RH)

            def tile(n, slot):
                return pltpu.make_async_copy(woland.at[:, pl.ds(pl.multiple_of(n * NT, NT), NT)], wt.at[slot],
                                             tsem.at[slot])

            tile(0, 0).start()

            for m in range(1, 8):
                d = a2a_land(half, m)
                rcopy(d, d, a2s.at[half, m], a2r.at[half, m], PT).wait_recv()
            a2a_own(half).wait()
            cps = [pltpu.make_async_copy(oland.at[d, pl.ds(half * JH, JH)], oo.at[:, :, pl.ds(d * hq, hq)],
                                         osem.at[J + d]) for d in range(8)]
            for cp in cps:
                cp.start()
            for cp in cps:
                cp.wait()
            for j in range(half * JH, (half + 1) * JH):
                x_in(j).wait()
            nt = D // NT

            @pl.loop(0, nt)
            def _(n):
                slot = n % 2

                @pl.when(n + 1 < nt)
                def _():
                    tile(n + 1, 1 - slot).start()

                tile(n, slot).wait()
                col = pl.ds(pl.multiple_of(n * NT, NT), NT)
                hk[part, col] = (hk[part, col].astype(F32)
                                 + jnp.dot(oo[...].reshape(RH, 8 * hq), wt[slot], preferred_element_type=F32)).astype(BF)

            _norm_rows(hk.at[part, :], g2_ref, own.at[part, :], RH)

        def sumsl(j, chip, col):
            return sums.at[j % 2, pl.ds(pl.multiple_of(chip * R, R), R), col]

        lo, hi = pl.ds(0, H), pl.ds(H, H)

        def rs_copy(j, i):
            k = dict(ss=rss.at[j, i], rs=rsr.at[j, i])
            if i == 0:
                return rcopy(pb.at[0], rs1land.at[j], to=PT, **k)
            if i == 1:
                return rcopy(sumsl(j, cx, lo), rs2x.at[j, 0], to=X, **k)
            if i == 2:
                return rcopy(sumsl(j, cd, lo), rs2x.at[j, 1], to=X, **k)
            if i == 3:
                return rcopy(sumsl(j, cy, hi), rs2y.at[j, 0], to=Y, **k)
            if i == 4:
                return rcopy(sumsl(j, cd, hi), rs2y.at[j, 1], to=Y, **k)
            if i == 5:
                return rcopy(sumsl(j, cy, lo), rs3a.at[j], to=Y, **k)
            return rcopy(sumsl(j, cx, hi), rs3b.at[j], to=X, **k)

        def load_b(j, half):
            pos = ((1 - s) if half == 0 else s) * 4
            return pltpu.make_async_copy(bland.at[pl.ds(pl.multiple_of(j * C + pos * R, R4), R4), :], bt.at[half],
                                         bsem.at[half])

        def compute(j):
            for half in range(2):
                load_b(j, half).wait()
                if half == 0:
                    @pl.when(j >= 1)
                    def _():
                        rs_copy(j - 1, 0).wait_send()

                @pl.loop(0, us.shape[1] // 256)
                def _(n):
                    col = pl.ds(pl.multiple_of(n * 256, 256), 256)
                    g = jnp.dot(bt[half], wg[:, col], preferred_element_type=F32)
                    u = jnp.dot(bt[half], wu[:, col], preferred_element_type=F32)
                    us[:, col] = (g * jax.nn.sigmoid(g) * u).astype(BF)

                @pl.loop(0, D // 512)
                def _(n):
                    col = pl.ds(pl.multiple_of(n * 512, 512), 512)
                    pb[half, :, col] = jnp.dot(us[...], wd[:, col], preferred_element_type=F32).astype(BF)

                if half == 0:
                    rs_copy(j, 0).start()

            rs_copy(j, 0).wait_recv()
            cp = pltpu.make_async_copy(rs1land.at[j], rt, bsem.at[2])
            cp.start()
            cp.wait()

            @pl.when(j >= 2)
            def _():
                for i in range(1, 7):
                    rs_copy(j - 2, i).wait_send()

            def add(sl):
                sums[j % 2, sl, :] = (pb[1, sl, :].astype(F32) + rt[sl, :].astype(F32)).astype(BF)

            ew(R4, add)
            for i in (1, 3, 2, 4):
                rs_copy(j, i).start()

        def rs3(j):
            for i in (1, 3, 2, 4):
                rs_copy(j, i).wait_recv()

            def addy(sl):
                b = pl.ds(pl.multiple_of(cy * R + sl.start, 16), 16)
                sums[j % 2, b, lo] = (sums[j % 2, b, lo].astype(F32) + rs2x[j, 1, sl, :].astype(F32)).astype(BF)
                b = pl.ds(pl.multiple_of(cx * R + sl.start, 16), 16)
                sums[j % 2, b, hi] = (sums[j % 2, b, hi].astype(F32) + rs2y[j, 1, sl, :].astype(F32)).astype(BF)

            ew(R, addy)
            rs_copy(j, 5).start()
            rs_copy(j, 6).start()

        def final(j):
            rs_copy(j, 5).wait_recv()
            rs_copy(j, 6).wait_recv()
            for i in range(3):
                g_copy(*gb, j, i).wait_send()

            def fin(sl):
                b = pl.ds(pl.multiple_of(c * R + sl.start, 16), 16)
                o = pl.ds(pl.multiple_of(j * R + sl.start, 16), 16)
                for col, r2, r3 in ((lo, rs2x, rs3a), (hi, rs2y, rs3b)):
                    t = (sums[j % 2, b, col].astype(F32) + r2[j, 0, sl, :].astype(F32)) + r3[j, sl, :].astype(F32)
                    own[o, col] = (hk[o, col].astype(F32) + t).astype(BF)

            ew(R, fin)
            g_own(*gy, j, 1)

        for j in range(J):
            x_in(j).start()
        oproj(0)
        g_own(*gb, 0, 0)
        for cp in wcp:
            cp.wait()
        oproj(1)
        g_fwd(*gb, 0)
        g_own(*gb, 1, 0)

        @pl.loop(0, J + 4)
        def _(t):
            @pl.when(t < J)
            def _():
                g_fwd2(*gb, t)

            @pl.when(t + 1 < J)
            def _():
                g_fwd(*gb, t + 1)

            @pl.when(t >= 4)
            def _():
                g_fwd2(*gy, t - 4)

            @pl.when(jnp.logical_and(t >= 3, t < J + 3))
            def _():
                g_fwd(*gy, t - 3)

            @pl.when(t + 2 < J)
            def _():
                g_own(*gb, t + 2, 0)

            @pl.when(t < J)
            def _():
                g_finish(*gb, t)
                g_local(bland, t, 0).wait()
                for half in range(2):
                    load_b(t, half).start()

            @pl.when(jnp.logical_and(t >= 2, t < J + 2))
            def _():
                final(t - 2)

            @pl.when(t < J)
            def _():
                compute(t)

            @pl.when(jnp.logical_and(t >= 1, t < J + 1))
            def _():
                rs3(t - 1)

        for b in range(2):
            for m in range(1, 8):
                a2a(b, m).wait_send()
        rs_copy(J - 1, 0).wait_send()
        for j in range(max(J - 2, 0), J):
            for i in range(1, 7):
                rs_copy(j, i).wait_send()

    pl.run_scoped(mlp, pltpu.VMEM((2, R4, D), BF), pltpu.VMEM((R4, wg.shape[1]), BF), pltpu.VMEM((2, R4, D), BF),
                  pltpu.VMEM((R4, D), BF), pltpu.VMEM((2, R4, D), BF), pltpu.VMEM((J // 2, R, 8 * hq), BF),
                  pltpu.VMEM((2, 8 * hq, min(512, D)), BF), pltpu.SemaphoreType.DMA((3,)),
                  pltpu.SemaphoreType.DMA((8 + J,)), pltpu.SemaphoreType.DMA((2,)))

    @pl.loop(0, J)
    def _(j):
        g_finish(*gy, j)
        for i in range(3, 9):
            g_copy(*gb, j, i).wait_send()
        for i in range(9):
            g_copy(*gy, j, i).wait_send()
        g_local(y_ref, j, 1).wait()


def _tables(pos):
    half = HEAD // 2
    inv = ROPE_BASE ** (-2.0 * jnp.arange(half, dtype=F32) / HEAD)
    t = pos.shape[0]
    p = pos.astype(F32)
    lane = lax.broadcasted_iota(jnp.int32, (t // 2, HEAD), 1)
    pp = jnp.where(lane < half, p[:t // 2, None], p[t // 2:, None])
    ang = pp * jnp.concatenate([inv, inv])[None, :]
    return jnp.cos(ang), jnp.sin(ang)


def solution(mesh):
    def local(x, pos, g1, g2, wq, wk, wv, wo, wg, wu, wd):
        t, d = x.shape
        hq = wq.shape[1]
        ff = wg.shape[1]
        cs, sn = _tables(pos)
        J = NCHUNK
        R = t // 8 // J
        QB = min(512, 8 * R)
        dma = pltpu.SemaphoreType.DMA
        vm = pl.BlockSpec(memory_space=pltpu.VMEM)
        big = lambda *sh: jax.ShapeDtypeStruct(sh, BF)
        y, k, v, *_ = pl.pallas_call(
            functools.partial(_big_kernel, J, R, QB),
            in_specs=[ANY, vm] + [ANY] * 9,
            out_specs=[ANY] * 7,
            out_shape=[big(t, d), big(t, HEAD), big(t, HEAD), big(8, J, R, hq), big(t, d), big(J, 4 * R, d),
                       big(8 * hq, d)],
            scratch_shapes=[pltpu.VMEM((d, ff), BF), pltpu.VMEM((d, ff), BF), pltpu.VMEM((ff, d), BF),
                            pltpu.VMEM((J, 2, R, d // 2), BF), pltpu.VMEM((J, 2, R, d // 2), BF),
                            pltpu.VMEM((J, R, d // 2), BF), pltpu.VMEM((J, R, d // 2), BF),
                            pltpu.VMEM((J * R, d), BF), pltpu.VMEM((J * R, d), BF), pltpu.VMEM((J, 8, R, hq), BF),
                            dma((2, 8)), dma((2, 8)), dma((J, 9)), dma((J, 9)), dma((J, 9)), dma((J, 9)),
                            dma((J, 7)), dma((J, 7)), dma((19,)), dma((19,)), dma((2, J)), dma((3,))],
            compiler_params=pltpu.CompilerParams(collective_id=0, has_side_effects=True,
                                                 vmem_limit_bytes=67043328),
            cost_estimate=pl.CostEstimate(flops=2 * t * d * ff * 4, bytes_accessed=2 * t * d * 6, transcendentals=0),
            name="layer",
        )(x, jnp.stack([g1, g2]).astype(F32), cs, sn, wq, wk, wv, wo, wg, wu, wd)
        nt = 16
        y, k, v = pl.pallas_call(
            functools.partial(_copy_kernel, nt), in_specs=[ANY] * 3, out_specs=[ANY] * 3,
            out_shape=[big(t, d), big(t, HEAD), big(t, HEAD)],
            scratch_shapes=[pltpu.VMEM((t, d), BF), pltpu.VMEM((t, HEAD), BF), pltpu.VMEM((t, HEAD), BF),
                            dma((nt + 2,)), dma((nt + 2,))],
            compiler_params=pltpu.CompilerParams(vmem_limit_bytes=67043328), name="out")(y, k, v)
        return y, k.reshape(t, 1, HEAD), v.reshape(t, 1, HEAD)

    return jax.shard_map(
        local,
        mesh=mesh,
        in_specs=(P("dp", None), P("dp"), P(), P(), P(None, "tp"), P(), P(), P("tp", None),
                  P(None, "tp"), P(None, "tp"), P("tp", None)),
        out_specs=(P("dp", None), P("dp", "tp", None), P("dp", "tp", None)),
        check_vma=False,
    )
```

```python
import functools

import jax
import jax.numpy as jnp
from jax import lax
from jax.experimental import pallas as pl
from jax.experimental.pallas import tpu as pltpu
from jax.sharding import PartitionSpec as P

HEAD = 128
EPS = 1e-5
ROPE_BASE = 500000.0
LOG2E = 1.4426950408889634
NCHUNK = 16
MESH = pl.DeviceIdType.MESH
F32, BF = jnp.float32, jnp.bfloat16
ANY = pl.BlockSpec(memory_space=pl.ANY)


def _pos_of(r):
    return (r % 2) * 4 + r // 2


def _norm_rows(src, g_ref, dst, rows, step=16):
    @pl.loop(0, rows // step, unroll=2)
    def _(n):
        sl = pl.ds(pl.multiple_of(n * step, step), step)
        t = src[sl, :].astype(F32)
        inv = lax.rsqrt(jnp.mean(t * t, axis=-1, keepdims=True) + EPS)
        dst[sl, :] = (t * inv * g_ref[...]).astype(BF)


def _copy_kernel(nt, y, k, v, yo, ko, vo, yb, kb, vb, si, so):
    rows = y.shape[0] // nt
    ins, outs = [], []
    for i in range(nt):
        r = pl.ds(i * rows, rows)
        ins.append(pltpu.make_async_copy(y.at[r, :], yb.at[r, :], si.at[i]))
        outs.append(pltpu.make_async_copy(yb.at[r, :], yo.at[r, :], so.at[i]))
    for i, (a, b, o) in enumerate(((k, kb, ko), (v, vb, vo))):
        ins.append(pltpu.make_async_copy(a, b, si.at[nt + i]))
        outs.append(pltpu.make_async_copy(b, o, so.at[nt + i]))
    for cp in ins:
        cp.start()
    for a, b in zip(ins, outs):
        a.wait()
        b.start()
    for cp in outs:
        cp.wait()


def _big_kernel(J, R, QB, x_ref, g_ref, cos_ref, sin_ref, wq_ref, wk_ref, wv_ref, wo_ref, wg_ref, wu_ref,
                wd_ref, y_ref, kout, vout, oland, bland, rs1land, woland,
                wg, wu, wd, rs2x, rs2y, rs3a, rs3b, hk, own, q,
                a2s, a2r, abs_, abr, ays, ayr, rss, rsr, wos, wor, lsem, wsem):
    me = lax.axis_index("tp")
    c, s = me // 2, me % 2
    T, D = x_ref.shape
    H = D // 2
    g1_ref, g2_ref = g_ref.at[pl.ds(0, 1), :], g_ref.at[pl.ds(1, 1), :]
    C = 8 * R
    R4 = 4 * R
    hq = wq_ref.shape[1]
    nh = hq // HEAD
    cx = c + 1 - 2 * (c % 2)
    cy = (c + 2) % 4
    cd = 3 - c
    dev = lambda chip, core: chip * 2 + core
    X, Y, DG, PT = dev(cx, s), dev(cy, s), dev(cd, s), dev(c, 1 - s)
    mypos = s * 4 + c
    px, py, pd = s * 4 + cx, s * 4 + cy, s * 4 + cd

    z = lax.axis_index("dp")

    def rcopy(src, dst, ss, rs, to):
        where = {"dp": 1 - z, "tp": me} if to is None else {"tp": to}
        return pltpu.make_async_remote_copy(src_ref=src, dst_ref=dst, send_sem=ss, recv_sem=rs,
                                            device_id=where, device_id_type=MESH)

    wcp = [pltpu.make_async_copy(wg_ref, wg, wsem.at[0]), pltpu.make_async_copy(wu_ref, wu, wsem.at[1]),
           pltpu.make_async_copy(wd_ref, wd, wsem.at[2])]

    bar = pltpu.get_barrier_semaphore()
    for m in range(1, 8):
        pl.semaphore_signal(bar, inc=1, device_id={"tp": (me + m) % 8}, device_id_type=MESH)
    pl.semaphore_signal(bar, inc=1, device_id={"dp": 1 - z, "tp": me}, device_id_type=MESH)
    pl.semaphore_wait(bar, 8)

    WB = hq // 3
    zr, ob, lr = z * 2 * WB, WB, (1 - z) * 2 * WB

    def worows(d, off=0, n=WB):
        return woland.at[pl.ds(pl.multiple_of(d * hq + off, WB), n), :]

    def wo_copy(i):
        k = dict(ss=wos.at[i], rs=wor.at[i])
        if i < 4:
            off = (zr, ob)[i // 2]
            return rcopy(wo_ref.at[pl.ds(pl.multiple_of(off, WB), WB), :], worows(me, off), to=(X, Y)[i % 2], **k)
        if i == 4:
            return rcopy(wo_ref, worows(me, 0, hq), to=PT, **k)
        d, off, to = ((X, zr, Y), (Y, ob, X), (X, zr, None), (Y, zr, None), (DG, zr, None), (X, zr, PT), (Y, zr, PT),
                      (X, ob, PT), (Y, ob, PT), (DG, zr, PT), (DG, ob, PT), (X, lr, PT), (Y, lr, PT),
                      (DG, lr, PT))[i - 5]
        return rcopy(worows(d, off), worows(d, off), to=to, **k)

    def wo_recv(i):
        x1, y1, d1 = dev(cx, 1 - s), dev(cy, 1 - s), dev(cd, 1 - s)
        d = worows(*((X, zr), (Y, zr), (X, ob), (Y, ob), (PT, 0, hq), (DG, zr), (DG, ob), (X, lr), (Y, lr), (DG, lr),
                     (x1, zr), (y1, zr), (x1, ob), (y1, ob), (d1, zr), (d1, ob), (x1, lr), (y1, lr), (d1, lr))[i])
        rcopy(d, d, wos.at[i], wor.at[i], PT).wait_recv()

    def wo_step(recvs, sends):
        for n in recvs:
            wo_recv(n)
        for n in sends:
            wo_copy(n).start()

    wo_in = pltpu.make_async_copy(wo_ref, hk.at[pl.ds(0, hq), :], lsem.at[0, 0])
    wo_out = pltpu.make_async_copy(hk.at[pl.ds(0, hq), :], worows(me, 0, hq), lsem.at[0, 0])

    def peer(m):
        return (me + m) % 8

    def frm(m):
        return (me + 8 - m) % 8

    JH = J // 2

    def a2a(b, m):
        to = peer(m)
        return rcopy(q.at[pl.ds(b * JH, JH), _pos_of(to)],
                     oland.at[me, pl.ds(b * JH, JH)],
                     a2s.at[b, m], a2r.at[b, m], to)

    def a2a_land(b, m):
        return oland.at[frm(m), pl.ds(b * JH, JH)]

    def a2a_own(b):
        return pltpu.make_async_copy(q.at[pl.ds(b * JH, JH), mypos], a2a_land(b, 0), a2s.at[b, 0])

    def send_o(b):
        for m in range(1, 8):
            a2a(b, m).start()
        a2a_own(b).start()

    def qblock(i, h, n):
        return (pl.ds(i * (n // C), n // C), slice(None), slice(None), pl.ds(h * HEAD, HEAD))

    TM = min(512, T // 2)

    def qkv(k, v, vt):
        def run(w, xt, ct, st, tsem, msem):
            nb = T // TM
            col = pl.ds(pl.multiple_of(me * HEAD, HEAD), HEAD)
            cps = [pltpu.make_async_copy(wq_ref, w.at[:, pl.ds(0, hq)], msem.at[0]),
                   pltpu.make_async_copy(wk_ref.at[:, col], w.at[:, pl.ds(hq, HEAD)], msem.at[1]),
                   pltpu.make_async_copy(wv_ref.at[:, col], w.at[:, pl.ds(hq + HEAD, HEAD)], msem.at[2])]

            def tile(i, slot):
                r = pl.ds(pl.multiple_of(i * TM, TM), TM)
                t = pl.ds(pl.multiple_of((i % (nb // 2)) * TM, TM), TM)
                return [pltpu.make_async_copy(x_ref.at[r, :], xt.at[slot], tsem.at[slot, 0]),
                        pltpu.make_async_copy(cos_ref.at[t, :], ct.at[slot], tsem.at[slot, 1]),
                        pltpu.make_async_copy(sin_ref.at[t, :], st.at[slot], tsem.at[slot, 2])]

            for cp in tile(0, 0) + cps:
                cp.start()
            wo_step((), range(5))
            wo_in.start()

            @pl.loop(0, nb)
            def _(i):
                slot = i % 2

                @pl.when(i + 1 < nb)
                def _():
                    for cp in tile(i + 1, 1 - slot):
                        cp.start()

                for cp in tile(i, slot):
                    cp.wait()
                _norm_rows(xt.at[slot], g1_ref, xt.at[slot], TM)

                @pl.when(i == 0)
                def _():
                    for cp in cps:
                        cp.wait()

                row = pl.ds(pl.multiple_of(i * TM, TM), TM)
                low = lax.broadcasted_iota(jnp.int32, (TM, HEAD), 1) < HEAD // 2
                keep = jnp.logical_xor(low, i >= nb // 2)
                cb, sb = ct[slot], st[slot]
                cc = jnp.where(keep, cb, pltpu.roll(cb, HEAD // 2, 1))
                ss = jnp.where(keep, sb, pltpu.roll(sb, HEAD // 2, 1))
                ss = jnp.where(low, -ss, ss)
                z = jnp.dot(xt[slot], w[...], preferred_element_type=F32)
                for h in range(nh + 1):
                    t = z[:, h * HEAD:(h + 1) * HEAD]
                    t = (t * cc + pltpu.roll(t, HEAD // 2, 1) * ss).astype(BF)
                    if h < nh:
                        q[qblock(i, h, TM)] = t.reshape(TM // C, 8, R, HEAD)
                    else:
                        k[row, :] = t
                zv = z[:, hq + HEAD:]
                v[row, :] = zv.astype(BF)
                vt[:, row] = zv.T.astype(BF)

                @pl.when(i == nb // 2)
                def _():
                    wo_step((0, 1), (7, 8, 5, 10, 11))

        pl.run_scoped(run, pltpu.VMEM((D, hq + 2 * HEAD), BF), pltpu.VMEM((2, TM, D), BF),
                      pltpu.VMEM((2, TM, HEAD), F32), pltpu.VMEM((2, TM, HEAD), F32),
                      pltpu.SemaphoreType.DMA((2, 3)), pltpu.SemaphoreType.DMA((3,)))

    def attention(k, v, vt, acc, mm, ll, mx, sb, asem):
        qkv(k, v, vt)
        kv_out = [pltpu.make_async_copy(k, kout, asem.at[0]), pltpu.make_async_copy(v, vout, asem.at[1])]
        for cp in kv_out + wcp:
            cp.start()
        wo_in.wait()
        wo_out.start()
        wo_step((2, 3), (6, 12, 13))
        sc = (HEAD ** -0.5) * LOG2E
        nq = T // QB
        ki = lax.broadcasted_iota(jnp.int32, (QB, QB), 0)
        qi = lax.broadcasted_iota(jnp.int32, (QB, QB), 1)

        @pl.loop(0, nq)
        def _(i):
            def qk(kb, h, masked=False):
                kk = k[pl.ds(pl.multiple_of(kb * QB, QB), QB), :]
                t = lax.dot_general(kk, q[qblock(i, h, QB)].reshape(QB, HEAD), (((1,), (1,)), ((), ())),
                                    preferred_element_type=F32)
                if masked:
                    t = jnp.where(ki <= qi, t, -jnp.inf)
                sb[h] = t
                mx[h] = jnp.max(t, axis=0, keepdims=True)

            def soft(kb, h):
                mo = mm[h]
                mn = jnp.maximum(mo, mx[h])
                mm[h] = mn
                al = jnp.exp2((mo - mn) * sc)
                p = jnp.exp2((sb[h] - mn) * sc)
                ll[h] = ll[h] * al + jnp.sum(p, axis=0, keepdims=True)
                acc[h] = acc[h] * al + jnp.dot(vt[:, pl.ds(pl.multiple_of(kb * QB, QB), QB)], p.astype(BF),
                                               preferred_element_type=F32)

            acc[...] = jnp.zeros_like(acc)
            ll[...] = jnp.zeros_like(ll)
            mm[...] = jnp.full_like(mm, -jnp.inf)

            def phases(kb, nxt, masked):
                for h in range(nh):
                    ahead = h + nh - 1
                    if ahead < nh:
                        qk(kb, ahead, masked)
                    else:
                        qk(nxt, ahead - nh)
                    soft(kb, h)

            for h in range(nh - 1):
                qk(i, h, True)
            phases(i, 0, True)

            @pl.loop(0, i)
            def _(kb):
                phases(kb, kb + 1, False)

            for h in range(nh):
                q[qblock(i, h, QB)] = (acc[h] / ll[h]).T.astype(BF).reshape(QB // C, 8, R, HEAD)

            @pl.when(i == nq // 2 - 1)
            def _():
                send_o(0)

            @pl.when(i == nq * 3 // 4 - 1)
            def _():
                wo_step((5,), (9, 14))

        send_o(1)
        wo_step((6,), (15,))
        wo_step((7, 8), (16, 17))
        wo_step((9,), (18,))
        for cp in kv_out:
            cp.wait()

    pl.run_scoped(attention, pltpu.VMEM((T, HEAD), BF), pltpu.VMEM((T, HEAD), BF),
                  pltpu.VMEM((HEAD, T), BF), pltpu.VMEM((nh, HEAD, QB), F32),
                  pltpu.VMEM((nh, 1, QB), F32), pltpu.VMEM((nh, 1, QB), F32), pltpu.VMEM((nh, 1, QB), F32),
                  pltpu.VMEM((nh, QB, QB), F32), pltpu.SemaphoreType.DMA((2,)))
    wo_out.wait()
    wo_step((4,) + tuple(range(10, 19)), ())
    for n in range(19):
        wo_copy(n).wait_send()

    R2 = R // 2

    def rows(land, j, pos, off=0, n=R):
        return land.at[pl.ds(pl.multiple_of(j * C + pos * R + off, R2), n), :]

    def ownrows(j):
        return own.at[pl.ds(pl.multiple_of(j * R, R), R), :]

    def g_copy(land, ss, rs, j, i):
        k = dict(ss=ss.at[j, i], rs=rs.at[j, i])
        if i < 3:
            return rcopy(ownrows(j), rows(land, j, mypos), to=(X, Y, PT)[i], **k)
        if i == 3:
            return rcopy(rows(land, j, px, 0, R2), rows(land, j, px, 0, R2), to=Y, **k)
        if i == 4:
            return rcopy(rows(land, j, py, R2, R2), rows(land, j, py, R2, R2), to=X, **k)
        if i == 5:
            return rcopy(rows(land, j, px), rows(land, j, px), to=PT, **k)
        if i == 6:
            return rcopy(rows(land, j, py), rows(land, j, py), to=PT, **k)
        off = 0 if i == 7 else R2
        return rcopy(rows(land, j, pd, off, R2), rows(land, j, pd, off, R2), to=PT, **k)

    def g_recv(land, ss, rs, j, i):
        o4 = (1 - s) * 4
        src = [(px, 0, R), (py, 0, R), (o4 + c, 0, R), (pd, 0, R2), (pd, R2, R2), (o4 + cx, 0, R), (o4 + cy, 0, R),
               (o4 + cd, 0, R2), (o4 + cd, R2, R2)][i]
        d = rows(land, j, *src)
        rcopy(d, d, ss.at[j, i], rs.at[j, i], PT).wait_recv()

    def g_local(land, j, kind):
        return pltpu.make_async_copy(ownrows(j), rows(land, j, mypos), lsem.at[kind, j])

    def g_own(land, ss, rs, j, kind):
        for i in range(3):
            g_copy(land, ss, rs, j, i).start()
        g_local(land, j, kind).start()

    def g_fwd(land, ss, rs, j):
        g_recv(land, ss, rs, j, 0)
        g_copy(land, ss, rs, j, 3).start()
        g_recv(land, ss, rs, j, 1)
        g_copy(land, ss, rs, j, 4).start()
        g_copy(land, ss, rs, j, 5).start()
        g_copy(land, ss, rs, j, 6).start()

    def g_fwd2(land, ss, rs, j):
        for i in (3, 4):
            g_recv(land, ss, rs, j, i)
            g_copy(land, ss, rs, j, i + 4).start()

    def g_finish(land, ss, rs, j):
        for i in (2, 5, 6, 7, 8):
            g_recv(land, ss, rs, j, i)

    gb = (bland, abs_, abr)
    gy = (y_ref, ays, ayr)

    def ew(n, f):
        @pl.loop(0, n // 16)
        def _(i):
            f(pl.ds(pl.multiple_of(i * 16, 16), 16))

    def mlp(bt, us, pb, rt, sums, oo, wt, bsem, osem, tsem):
        NT = wt.shape[2]
        RH = JH * R

        def x_in(j):
            return pltpu.make_async_copy(x_ref.at[pl.ds(pl.multiple_of(j * C + mypos * R, R), R), :],
                                         hk.at[pl.ds(pl.multiple_of(j * R, R), R), :], osem.at[j])

        def oproj(half):
            part = pl.ds(half * RH, RH)

            def tile(n, slot):
                return pltpu.make_async_copy(woland.at[:, pl.ds(pl.multiple_of(n * NT, NT), NT)], wt.at[slot],
                                             tsem.at[slot])

            tile(0, 0).start()

            for m in range(1, 8):
                d = a2a_land(half, m)
                rcopy(d, d, a2s.at[half, m], a2r.at[half, m], PT).wait_recv()
            a2a_own(half).wait()
            cps = [pltpu.make_async_copy(oland.at[d, pl.ds(half * JH, JH)], oo.at[:, :, pl.ds(d * hq, hq)],
                                         osem.at[J + d]) for d in range(8)]
            for cp in cps:
                cp.start()
            for cp in cps:
                cp.wait()
            for j in range(half * JH, (half + 1) * JH):
                x_in(j).wait()
            nt = D // NT

            @pl.loop(0, nt)
            def _(n):
                slot = n % 2

                @pl.when(n + 1 < nt)
                def _():
                    tile(n + 1, 1 - slot).start()

                tile(n, slot).wait()
                col = pl.ds(pl.multiple_of(n * NT, NT), NT)
                hk[part, col] = (hk[part, col].astype(F32)
                                 + jnp.dot(oo[...].reshape(RH, 8 * hq), wt[slot], preferred_element_type=F32)).astype(BF)

            _norm_rows(hk.at[part, :], g2_ref, own.at[part, :], RH)

        def sumsl(j, chip, col):
            return sums.at[j % 2, pl.ds(pl.multiple_of(chip * R, R), R), col]

        lo, hi = pl.ds(0, H), pl.ds(H, H)

        def rs_copy(j, i):
            k = dict(ss=rss.at[j, i], rs=rsr.at[j, i])
            if i == 0:
                return rcopy(pb.at[0], rs1land.at[j], to=PT, **k)
            if i == 1:
                return rcopy(sumsl(j, cx, lo), rs2x.at[j, 0], to=X, **k)
            if i == 2:
                return rcopy(sumsl(j, cd, lo), rs2x.at[j, 1], to=X, **k)
            if i == 3:
                return rcopy(sumsl(j, cy, hi), rs2y.at[j, 0], to=Y, **k)
            if i == 4:
                return rcopy(sumsl(j, cd, hi), rs2y.at[j, 1], to=Y, **k)
            if i == 5:
                return rcopy(sumsl(j, cy, lo), rs3a.at[j], to=Y, **k)
            return rcopy(sumsl(j, cx, hi), rs3b.at[j], to=X, **k)

        def load_b(j, half):
            pos = ((1 - s) if half == 0 else s) * 4
            return pltpu.make_async_copy(bland.at[pl.ds(pl.multiple_of(j * C + pos * R, R4), R4), :], bt.at[half],
                                         bsem.at[half])

        def compute(j):
            for half in range(2):
                load_b(j, half).wait()
                if half == 0:
                    @pl.when(j >= 1)
                    def _():
                        rs_copy(j - 1, 0).wait_send()

                @pl.loop(0, us.shape[1] // 256)
                def _(n):
                    col = pl.ds(pl.multiple_of(n * 256, 256), 256)
                    g = jnp.dot(bt[half], wg[:, col], preferred_element_type=F32)
                    u = jnp.dot(bt[half], wu[:, col], preferred_element_type=F32)
                    us[:, col] = (g * jax.nn.sigmoid(g) * u).astype(BF)

                @pl.loop(0, D // 512)
                def _(n):
                    col = pl.ds(pl.multiple_of(n * 512, 512), 512)
                    pb[half, :, col] = jnp.dot(us[...], wd[:, col], preferred_element_type=F32).astype(BF)

                if half == 0:
                    rs_copy(j, 0).start()

            rs_copy(j, 0).wait_recv()
            cp = pltpu.make_async_copy(rs1land.at[j], rt, bsem.at[2])
            cp.start()
            cp.wait()

            @pl.when(j >= 2)
            def _():
                for i in range(1, 7):
                    rs_copy(j - 2, i).wait_send()

            def add(sl):
                sums[j % 2, sl, :] = (pb[1, sl, :].astype(F32) + rt[sl, :].astype(F32)).astype(BF)

            ew(R4, add)
            for i in (1, 3, 2, 4):
                rs_copy(j, i).start()

        def rs3(j):
            for i in (1, 3, 2, 4):
                rs_copy(j, i).wait_recv()

            def addy(sl):
                b = pl.ds(pl.multiple_of(cy * R + sl.start, 16), 16)
                sums[j % 2, b, lo] = (sums[j % 2, b, lo].astype(F32) + rs2x[j, 1, sl, :].astype(F32)).astype(BF)
                b = pl.ds(pl.multiple_of(cx * R + sl.start, 16), 16)
                sums[j % 2, b, hi] = (sums[j % 2, b, hi].astype(F32) + rs2y[j, 1, sl, :].astype(F32)).astype(BF)

            ew(R, addy)
            rs_copy(j, 5).start()
            rs_copy(j, 6).start()

        def final(j):
            rs_copy(j, 5).wait_recv()
            rs_copy(j, 6).wait_recv()
            for i in range(3):
                g_copy(*gb, j, i).wait_send()

            def fin(sl):
                b = pl.ds(pl.multiple_of(c * R + sl.start, 16), 16)
                o = pl.ds(pl.multiple_of(j * R + sl.start, 16), 16)
                for col, r2, r3 in ((lo, rs2x, rs3a), (hi, rs2y, rs3b)):
                    t = (sums[j % 2, b, col].astype(F32) + r2[j, 0, sl, :].astype(F32)) + r3[j, sl, :].astype(F32)
                    own[o, col] = (hk[o, col].astype(F32) + t).astype(BF)

            ew(R, fin)
            g_own(*gy, j, 1)

        for j in range(J):
            x_in(j).start()
        oproj(0)
        g_own(*gb, 0, 0)
        for cp in wcp:
            cp.wait()
        oproj(1)
        g_fwd(*gb, 0)
        g_own(*gb, 1, 0)

        @pl.loop(0, J + 4)
        def _(t):
            @pl.when(t < J)
            def _():
                g_fwd2(*gb, t)

            @pl.when(t + 1 < J)
            def _():
                g_fwd(*gb, t + 1)

            @pl.when(t >= 4)
            def _():
                g_fwd2(*gy, t - 4)

            @pl.when(jnp.logical_and(t >= 3, t < J + 3))
            def _():
                g_fwd(*gy, t - 3)

            @pl.when(t + 2 < J)
            def _():
                g_own(*gb, t + 2, 0)

            @pl.when(t < J)
            def _():
                g_finish(*gb, t)
                g_local(bland, t, 0).wait()
                for half in range(2):
                    load_b(t, half).start()

            @pl.when(jnp.logical_and(t >= 2, t < J + 2))
            def _():
                final(t - 2)

            @pl.when(t < J)
            def _():
                compute(t)

            @pl.when(jnp.logical_and(t >= 1, t < J + 1))
            def _():
                rs3(t - 1)

        for b in range(2):
            for m in range(1, 8):
                a2a(b, m).wait_send()
        rs_copy(J - 1, 0).wait_send()
        for j in range(max(J - 2, 0), J):
            for i in range(1, 7):
                rs_copy(j, i).wait_send()

    pl.run_scoped(mlp, pltpu.VMEM((2, R4, D), BF), pltpu.VMEM((R4, wg.shape[1]), BF), pltpu.VMEM((2, R4, D), BF),
                  pltpu.VMEM((R4, D), BF), pltpu.VMEM((2, R4, D), BF), pltpu.VMEM((J // 2, R, 8 * hq), BF),
                  pltpu.VMEM((2, 8 * hq, min(512, D)), BF), pltpu.SemaphoreType.DMA((3,)),
                  pltpu.SemaphoreType.DMA((8 + J,)), pltpu.SemaphoreType.DMA((2,)))

    @pl.loop(0, J)
    def _(j):
        g_finish(*gy, j)
        for i in range(3, 9):
            g_copy(*gb, j, i).wait_send()
        for i in range(9):
            g_copy(*gy, j, i).wait_send()
        g_local(y_ref, j, 1).wait()


def _tables(pos):
    half = HEAD // 2
    inv = ROPE_BASE ** (-2.0 * jnp.arange(half, dtype=F32) / HEAD)
    t = pos.shape[0]
    p = pos.astype(F32)
    lane = lax.broadcasted_iota(jnp.int32, (t // 2, HEAD), 1)
    pp = jnp.where(lane < half, p[:t // 2, None], p[t // 2:, None])
    ang = pp * jnp.concatenate([inv, inv])[None, :]
    return jnp.cos(ang), jnp.sin(ang)


def solution(mesh):
    def local(x, pos, g1, g2, wq, wk, wv, wo, wg, wu, wd):
        t, d = x.shape
        hq = wq.shape[1]
        ff = wg.shape[1]
        cs, sn = _tables(pos)
        J = NCHUNK
        R = t // 8 // J
        QB = min(512, 8 * R)
        dma = pltpu.SemaphoreType.DMA
        vm = pl.BlockSpec(memory_space=pltpu.VMEM)
        big = lambda *sh: jax.ShapeDtypeStruct(sh, BF)
        y, k, v, *_ = pl.pallas_call(
            functools.partial(_big_kernel, J, R, QB),
            in_specs=[ANY, vm] + [ANY] * 9,
            out_specs=[ANY] * 7,
            out_shape=[big(t, d), big(t, HEAD), big(t, HEAD), big(8, J, R, hq), big(t, d), big(J, 4 * R, d),
                       big(8 * hq, d)],
            scratch_shapes=[pltpu.VMEM((d, ff), BF), pltpu.VMEM((d, ff), BF), pltpu.VMEM((ff, d), BF),
                            pltpu.VMEM((J, 2, R, d // 2), BF), pltpu.VMEM((J, 2, R, d // 2), BF),
                            pltpu.VMEM((J, R, d // 2), BF), pltpu.VMEM((J, R, d // 2), BF),
                            pltpu.VMEM((J * R, d), BF), pltpu.VMEM((J * R, d), BF), pltpu.VMEM((J, 8, R, hq), BF),
                            dma((2, 8)), dma((2, 8)), dma((J, 9)), dma((J, 9)), dma((J, 9)), dma((J, 9)),
                            dma((J, 7)), dma((J, 7)), dma((19,)), dma((19,)), dma((2, J)), dma((3,))],
            compiler_params=pltpu.CompilerParams(collective_id=0, has_side_effects=True,
                                                 vmem_limit_bytes=67043328),
            cost_estimate=pl.CostEstimate(flops=2 * t * d * ff * 4, bytes_accessed=2 * t * d * 6, transcendentals=0),
            name="layer",
        )(x, jnp.stack([g1, g2]).astype(F32), cs, sn, wq, wk, wv, wo, wg, wu, wd)
        nt = 16
        y, k, v = pl.pallas_call(
            functools.partial(_copy_kernel, nt), in_specs=[ANY] * 3, out_specs=[ANY] * 3,
            out_shape=[big(t, d), big(t, HEAD), big(t, HEAD)],
            scratch_shapes=[pltpu.VMEM((t, d), BF), pltpu.VMEM((t, HEAD), BF), pltpu.VMEM((t, HEAD), BF),
                            dma((nt + 2,)), dma((nt + 2,))],
            compiler_params=pltpu.CompilerParams(vmem_limit_bytes=67043328), name="out")(y, k, v)
        return y, k.reshape(t, 1, HEAD), v.reshape(t, 1, HEAD)

    return jax.shard_map(
        local,
        mesh=mesh,
        in_specs=(P("dp", None), P("dp"), P(), P(), P(None, "tp"), P(), P(), P("tp", None),
                  P(None, "tp"), P(None, "tp"), P("tp", None)),
        out_specs=(P("dp", None), P("dp", "tp", None), P("dp", "tp", None)),
        check_vma=False,
    )
```
